32 devices in a mesh: gx: 4 (over x, core), gy: 2 (over y), gz: 4 (over z).
Axes of the slice: x: 2, y: 2, z: 4, core: 2. Of those that a mesh axis runs over, the one named last changes fastest.
Arguments:
- fields: float32 [5, 64, 16, 512], P(None, 'gz', 'gy', 'gx'), may hold values from -4 to 4
- radius: float32 [8, 64, 16, 512], P(None, 'gz', 'gy', 'gx'), may hold values from 0.4 to 1.5
- weight: float32 [8, 64, 16, 512], P(None, 'gz', 'gy', 'gx'), may hold values from 0.05 to 0.5
- column: int32 [8, 64, 16, 512], P(None, 'gz', 'gy', 'gx'), may hold values from 0 to 127
- counts: int32 [64, 16, 512], P('gz', 'gy', 'gx'), may hold values from 1 to 8
- fall_depth: int32 [8, 64, 16, 4], P(None, 'gz', 'gy', 'gx'), may hold values from 0 to 8, as said below
Outputs:
- new_fields: float32 [5, 64, 16, 512], P(None, 'gz', 'gy', 'gx')
- moments: float32 [3, 64, 16, 512], P(None, 'gz', 'gy', 'gx')
The draws below stay inside these ranges and needn't reach their ends.
Inputs may be any that keep to these rules, and one draw needn't show every extreme that they name: The droplet in slot s of cell (k, j, i) sits in x cell (i // 128) * 128 + column[s, k, j, i]. Slots s < counts[k, j, i] hold live droplets. The droplets of slot s in cells (k, j, b * 128) to (k, j, (b + 1) * 128 - 1) fall together by fall_depth[s, k, j, b] levels, never below the lowest level: fall_depth[s, k, j, b] <= k; 8 is reached in every draw.
All inputs are finite; a program needn't handle non-finite values. Where the reference program divides by a largest or mean magnitude, that divisor is 1e-20 or more.
Results may differ from the reference program's by a relative error of at most 0.00021.
Values sent between devices are 32-bit elements; how exact they have to be, the bound alone decides.
A program may use at most 64 MiB of HBM per device.

```python
import math
import jax
import jax.numpy as jnp
from jax import lax

CX = 128
SLOTS = 8
NS = 4
FMAX = 8
NX = 512
NY = 16
NZ = 64
XBLOCKS = 4


def draw_fall_depth(key, part):
    drawn = jax.random.randint(key, (SLOTS, NZ, NY, XBLOCKS), 0, FMAX + 1, dtype=jnp.int32)
    drawn = drawn.at[0, NZ - 1, 0, 0].set(FMAX)
    levels = jnp.arange(NZ, dtype=jnp.int32)[None, :, None, None]
    return jnp.minimum(drawn, levels).astype(jnp.int32)


def set_ends(values, own_key, least, largest):
    shape = values.shape
    index_at = [jax.random.randint(jax.random.fold_in(own_key, axis), (), 0, shape[axis]) for axis in range(len(shape))]
    values = values.at[tuple(index_at)].set(least)
    longest = shape.index(max(shape))
    index_at[longest] = (index_at[longest] + 1) % shape[longest]
    return values.at[tuple(index_at)].set(largest)


def shard_levels(key, shape, cuts, smallest, high):
    loudness = 1.0
    for position, shards_of in cuts:
        steps = jax.random.uniform(jax.random.fold_in(jax.random.fold_in(key, 6), position), (shards_of,), jnp.float32, smallest / len(cuts), high / len(cuts))
        loudness = loudness * jnp.repeat(jnp.exp(steps), shape[position] // shards_of).reshape((-1,) + (1,) * (len(shape) - 1 - position))
    return loudness


def centred(rng, dims, spread, reach, cuts=(), held_as=jnp.bfloat16):
    entries = spread * jax.random.normal(rng, dims, jnp.float32)
    if cuts:
        entries = entries * shard_levels(rng, dims, cuts, -0.22, 0.18)
    return jnp.clip(entries, -reach, reach).astype(held_as)


def setup_inputs(seed: int = 0) -> dict:
    splits = jax.random.split(jax.random.key(seed), 7)
    fields = centred(splits[0], (5, NZ, NY, NX), 0.5, 4.0, ((1, 4), (2, 2), (3, 4)), jnp.float32)
    radius = jnp.clip(jnp.exp(math.log(1.5) - 1.3217558 * jax.random.uniform(splits[1], (SLOTS, NZ, NY, NX), jnp.float32) ** shard_levels(splits[1], (SLOTS, NZ, NY, NX), ((1, 4), (2, 2), (3, 4)), -0.2, 0.2)), 0.4, 1.5)
    weight = jnp.clip(jnp.exp(math.log(0.5) - 2.3025851 * jax.random.uniform(splits[2], (SLOTS, NZ, NY, NX), jnp.float32) ** shard_levels(splits[2], (SLOTS, NZ, NY, NX), ((1, 4), (2, 2), (3, 4)), -0.2, 0.2)), 0.05, 0.5)
    column = set_ends(jax.random.randint(splits[3], (SLOTS, NZ, NY, NX), 0, CX), jax.random.fold_in(splits[3], 1), 0, CX - 1).astype(jnp.int32)
    counts = set_ends(jax.random.randint(splits[4], (NZ, NY, NX), 1, SLOTS + 1), jax.random.fold_in(splits[4], 1), 1, SLOTS).astype(jnp.int32)
    fall_depth = draw_fall_depth(jax.random.fold_in(splits[6], 71), 0)
    return dict(fields=fields, radius=radius, weight=weight, column=column, counts=counts, fall_depth=fall_depth)


sound_speed = 10.0
buoyancy = 0.5
courant_goal = 0.6
growth = 0.3

def window(padded, margin, direction, offset, length):
    cut = []
    for dimension in range(3):
        if dimension == direction:
            cut.append(slice(margin + offset, margin + offset + length))
        else:
            cut.append(slice(margin, padded.shape[dimension] - margin))
    return padded[tuple(cut)]

def advect(quantity, margin, wind_pad, wind_margin):
    tendency = jnp.zeros(tuple((quantity.shape[dimension] - 2 * margin for dimension in range(3))), jnp.float32)
    for direction in range(3):
        cells_along = quantity.shape[direction] - 2 * margin
        stencil = [window(quantity, margin, direction, offset - 1, cells_along + 1) for offset in range(-2, 4)]
        face_wind = window(wind_pad[2 - direction], wind_margin, direction, -1, cells_along + 1)
        central = 37.0 * (stencil[2] + stencil[3]) - 8.0 * (stencil[1] + stencil[4]) + (stencil[0] + stencil[5])
        upwind = 10.0 * (stencil[3] - stencil[2]) - 5.0 * (stencil[4] - stencil[1]) + (stencil[5] - stencil[0])
        face_flux = (face_wind * central - jnp.abs(face_wind) * upwind) / 60.0
        upper_flux = lax.slice_in_dim(face_flux, 1, cells_along + 1, axis=direction)
        lower_flux = lax.slice_in_dim(face_flux, 0, cells_along, axis=direction)
        tendency = tendency - (upper_flux - lower_flux)
    return tendency

def extend(fields, margin):
    fields = jnp.pad(fields, ((0, 0), (margin, margin), (0, 0), (0, 0)))
    return jnp.pad(fields, ((0, 0), (0, 0), (margin, margin), (margin, margin)), mode='wrap')

def acoustic(fast_fields, lift_term, pressure_rate, sub_step, lid_mask):
    grid_levels, grid_rows, grid_cols = (fast_fields.shape[1], fast_fields.shape[2], fast_fields.shape[3])
    pressure_pad = extend(fast_fields[0:1], 1)[0]
    pressure = fast_fields[0]
    east_wind = fast_fields[1] - sub_step * sound_speed * (window(pressure_pad, 1, 2, 1, grid_cols) - pressure)
    north_wind = fast_fields[2] - sub_step * sound_speed * (window(pressure_pad, 1, 1, 1, grid_rows) - pressure)
    vertical_wind = (fast_fields[3] + sub_step * (lift_term - sound_speed * (window(pressure_pad, 1, 0, 1, grid_levels) - pressure))) * lid_mask
    wind_halo = extend(jnp.stack([east_wind, north_wind, vertical_wind]), 1)
    divergence = east_wind - window(wind_halo[0], 1, 2, -1, grid_cols) + (north_wind - window(wind_halo[1], 1, 1, -1, grid_rows)) + (vertical_wind - window(wind_halo[2], 1, 0, -1, grid_levels))
    pressure = pressure + sub_step * (pressure_rate - sound_speed * divergence)
    return jnp.stack([pressure, east_wind, north_wind, vertical_wind])

def reference(fields, radius, weight, column, counts, fall_depth):
    grid_levels, grid_rows, grid_cols = (fields.shape[1], fields.shape[2], fields.shape[3])
    lid_mask = (jnp.arange(grid_levels, dtype=jnp.int32) < grid_levels - 1).astype(jnp.float32)[:, None, None]
    initial = jnp.concatenate([fields[0:4], (fields[4] * lid_mask)[None]])
    top_speed = jnp.max(jnp.abs(initial[2]) + jnp.abs(initial[3]) + jnp.abs(initial[4]))
    time_step = courant_goal / (1.0 + top_speed)
    current = initial
    for fraction, substeps in ((1.0 / 3.0, 1), (0.5, NS // 2), (1.0, NS)):
        padded = extend(current, 3)
        tracer_rate = advect(padded[0], 3, padded[2:5], 3)
        pressure_rate = advect(padded[1], 3, padded[2:5], 3)
        lift_term = buoyancy * 0.5 * (window(padded[0], 3, 0, 0, grid_levels) + window(padded[0], 3, 0, 1, grid_levels)) * lid_mask
        sub_step = fraction * time_step / substeps
        fast_fields = initial[1:5]
        for repeat in range(substeps):
            fast_fields = acoustic(fast_fields, lift_term, pressure_rate, sub_step, lid_mask)
        tracer = initial[0] + fraction * time_step * tracer_rate
        current = jnp.concatenate([tracer[None], fast_fields])
    tracer = current[0]
    block_start = jnp.arange(grid_cols, dtype=jnp.int32) // CX * CX
    levels = jnp.arange(grid_levels, dtype=jnp.int32)[:, None, None]
    row_index = jnp.arange(grid_rows, dtype=jnp.int32)[None, :, None]
    moments = jnp.zeros((3, grid_levels * grid_rows * grid_cols), jnp.float32)
    for slot_index in range(SLOTS):
        cell_column = (block_start[None, None, :] + column[slot_index]).astype(jnp.int32)
        near_tracer = jnp.take_along_axis(tracer, cell_column, axis=2)
        squared = radius[slot_index] * radius[slot_index] * jnp.exp(growth * near_tracer)
        number = weight[slot_index] * (slot_index < counts).astype(jnp.float32)
        area_term = number * squared
        mass_term = area_term * jnp.sqrt(squared)
        fall_cells = jnp.repeat(fall_depth[slot_index], CX, axis=2).astype(jnp.int32)
        flat_index = (((levels - fall_cells) * grid_rows + row_index) * grid_cols + cell_column).astype(jnp.int32)
        moments = moments.at[:, flat_index.reshape(-1)].add(jnp.stack([number, area_term, mass_term]).reshape(3, -1))
    return (current, moments.reshape(3, grid_levels, grid_rows, grid_cols))
```

```python
import functools
import itertools
import jax
import jax.numpy as jnp
from jax import lax
from jax.experimental import pallas as pl
from jax.experimental.pallas import tpu as pltpu
from jax.sharding import PartitionSpec as P

NS = 4
FMAX = 8
CELLS = 8
SLOT = 8
EDGE = 3
CHUNKS = (24, 24, 16, 24, 8, 16, 16)
ONE_SHOT = 32

sound_speed = 10.0
buoyancy = 0.5
courant_goal = 0.6
growth = 0.3

MESH = pl.DeviceIdType.MESH
AXES = ("gy", "gx", "gz")
FULL = {"0": 0, "1": 1, "2": 2}
THIN = {"a": 0, "b": 1, "c": 2, "d": 3}


def flux(wind, a, b, c, d, e, f):
    central = 37.0 * (c + d) - 8.0 * (b + e) + (a + f)
    upwind = 10.0 * (d - c) - 5.0 * (e - b) + (f - a)
    return wind * central - jnp.abs(wind) * upwind


def max_groups(count):
    total = 1
    for a in AXES:
        total *= count[a]
    return (AXES,) if total <= ONE_SHOT else tuple((a,) for a in AXES)


def shifts_of(group, count):
    return [s for s in itertools.product(*(range(count[a]) for a in group)) if any(s)]


def kernel(
    sizes, depth_hbm, fields_hbm, radius_hbm, weight_hbm, column_hbm, counts_hbm,
    out_fields, moments, *scratch
):
    names, levels, rows, cols, slots = sizes
    refs = dict(zip(names, scratch))
    radius, weight, column, counts = (refs[n] for n in ("radius", "weight", "column", "counts"))
    depth = refs["depth"]
    vals, fallen = refs["vals"], refs["fallen"]
    local_sem = refs["local_sem"]
    shape = (rows, cols)
    lane = lax.broadcasted_iota(jnp.int32, shape, 1)
    row = lax.broadcasted_iota(jnp.int32, shape, 0)
    slot_lane = lane % SLOT
    place = {a: lax.axis_index(a) for a in AXES}
    count = {a: lax.axis_size(a) for a in AXES}
    groups = max_groups(count)
    has_low = place["gz"] > 0
    has_high = place["gz"] < count["gz"] - 1
    zero = jnp.zeros(shape, jnp.float32)

    def lanes_by(x, shift):
        return pltpu.roll(x, shift % cols, 1)

    def rows_by(x, shift):
        return pltpu.roll(x, shift % rows, 0)

    def loop(n, body, carry, unroll=True):
        return lax.fori_loop(0, n, body, carry, unroll=unroll)

    first_copies = []
    for n, dst in enumerate(
        (refs["C0"].at[pl.ds(3, levels)], refs["P0"].at[pl.ds(3, levels)],
         refs["U0"], refs["V0"], refs["W0"].at[pl.ds(1, levels)])
    ):
        first_copies.append(pltpu.make_async_copy(fields_hbm.at[n], dst, local_sem.at[n]))
    later_copies = []
    for n, (src, dst) in enumerate(
        ((counts_hbm, counts), (weight_hbm, weight), (radius_hbm, radius),
         (column_hbm, column), (depth_hbm, depth))
    ):
        later_copies.append(pltpu.make_async_copy(src, dst, local_sem.at[5 + n]))
    for copy in first_copies + later_copies:
        copy.start()

    def away(group, shift):
        return {a: lax.rem(place[a] + s, count[a]) for a, s in zip(group, shift) if s}

    barrier = pltpu.get_barrier_semaphore()
    peers = 0
    for group in groups:
        for shift in shifts_of(group, count):
            pl.semaphore_signal(barrier, inc=1, device_id=away(group, shift), device_id_type=MESH)
            peers += 1

    for copy in first_copies:
        copy.wait()

    @pl.when(jnp.logical_not(has_high))
    def _():
        refs["W0"][levels] = zero
        for tag in ("0", "1", "2"):
            for t in range(EDGE):
                refs["C" + tag][3 + levels + t] = zero
        for tag in "012abcd":
            for t in range(EDGE if tag in FULL else 1):
                refs["P" + tag][3 + levels + t] = zero

    @pl.when(jnp.logical_not(has_low))
    def _():
        refs["W0"][0] = zero
        for tag in ("0", "1", "2"):
            for t in range(EDGE):
                refs["C" + tag][t] = zero
        for tag in "012abcd":
            for t in range(3 - (EDGE if tag in FULL else 1), 3):
                refs["P" + tag][t] = zero

    def fastest(k, top):
        speed = jnp.abs(refs["U0"][k]) + jnp.abs(refs["V0"][k]) + jnp.abs(refs["W0"][k + 1])
        return jnp.maximum(top, speed)

    top = loop(levels, fastest, zero)
    top = jnp.max(top, axis=0, keepdims=True)
    pl.semaphore_wait(barrier, peers)

    def max_start(g, value):
        refs["max_send"][g] = value
        copies = []
        for n, shift in enumerate(shifts_of(groups[g], count)):
            copy = pltpu.make_async_remote_copy(
                src_ref=refs["max_send"].at[g],
                dst_ref=refs["max_recv"].at[g, n],
                send_sem=refs["max_ss"].at[g, n],
                recv_sem=refs["max_rs"].at[g, n],
                device_id=away(groups[g], shift), device_id_type=MESH,
            )
            copy.start()
            copies.append(copy)
        return copies

    def max_end(g, value, copies):
        for copy in copies:
            copy.wait()
        for n in range(len(copies)):
            value = jnp.maximum(value, refs["max_recv"][g, n])
        return value

    def neighbour(a, step):
        return {a: lax.rem(place[a] + count[a] + step, count[a])}

    def remote(src, dst, sems, n, a, step):
        return pltpu.make_async_remote_copy(
            src_ref=src, dst_ref=dst, send_sem=refs[sems + "_ss"].at[n],
            recv_sem=refs[sems + "_rs"].at[n],
            device_id=neighbour(a, step), device_id_type=MESH,
        )

    def y_copies(name, tag, sems, at):
        source = refs[name + tag]
        if tag in FULL:
            w, low, high, dst = EDGE, rows - EDGE, 0, refs["HY" + name + tag]
        else:
            w, low, high, dst = 1, 0, rows - 1, refs["HYT" + tag]
        own = pl.ds(3, levels)
        return (
            remote(source.at[own, pl.ds(rows - w, w), :], dst.at[:, pl.ds(low, w), :],
                   sems, at, "gy", 1),
            remote(source.at[own, pl.ds(0, w), :], dst.at[:, pl.ds(high, w), :],
                   sems, at + 1, "gy", -1),
        )

    def z_copies(name, tag, sems, at):
        w = EDGE if tag in FULL else 1
        q = refs[name + tag]
        return (
            remote(q.at[pl.ds(3 + levels - w, w)], q.at[pl.ds(3 - w, w)], sems, at, "gz", 1),
            remote(q.at[pl.ds(3, w)], q.at[pl.ds(3 + levels, w)], sems, at + 1, "gz", -1),
        )

    def x_copies(tag, sems, at):
        kind, e = ("fx", FULL[tag]) if tag in FULL else ("tx", THIN[tag])
        return (
            remote(refs[kind + "_s"].at[e], refs[kind + "_lo"].at[e], sems, at, "gx", 1),
            remote(refs[kind + "_s"].at[e], refs[kind + "_hi"].at[e], sems, at + 1, "gx", -1),
        )

    def z_start(pair):
        @pl.when(has_high)
        def _():
            pair[0].start()

        @pl.when(has_low)
        def _():
            pair[1].start()

    def z_wait(pair):
        @pl.when(has_high)
        def _():
            pair[0].wait_send()
            pair[1].wait_recv()

        @pl.when(has_low)
        def _():
            pair[1].wait_send()
            pair[0].wait_recv()

    def wind_copies():
        own = refs["V0"].at[:, pl.ds(rows - 1, 1), :]
        return (
            remote(own, refs["HYV0"].at[:, pl.ds(0, 1), :], "f0", 10, "gy", 1),
            remote(refs["W0"].at[levels], refs["W0"].at[0], "f0", 11, "gz", 1),
        )

    def pack(names_at, tag):
        def body(k, packed):
            out = []
            for name, got in zip(names_at, packed):
                edge = lanes_by(refs[name + tag][k + 3], SLOT * k + (EDGE if tag in FULL else 1))
                if tag == "0" and name == "P":
                    edge = jnp.where(
                        slot_lane == 6, lanes_by(refs["U0"][k], SLOT * k + 7), edge
                    )
                out.append(jnp.where(lane // SLOT == k, edge, got))
            return tuple(out)

        packed = (zero,) * len(names_at)
        for k in range(levels):
            packed = body(k, packed)
        return packed

    def send_full(tag):
        sems, e = "f" + tag, FULL[tag]
        x = x_copies(tag, sems, 0)
        for n, part in enumerate(pack("PC", tag)):
            refs["fx_s"][e, n] = part
        for copy in y_copies("P", tag, sems, 2):
            copy.start()
        if tag == "0":
            wind_copies()[0].start()
        for name, at in (("P", 4), ("C", 6)):
            z_start(z_copies(name, tag, sems, at))
        if tag == "0":
            @pl.when(has_high)
            def _():
                wind_copies()[1].start()
        for copy in x:
            copy.start()
        for copy in y_copies("C", tag, sems, 8):
            copy.start()

    def receive_xz(tag):
        sems, e = "f" + tag, FULL[tag]
        for copy in x_copies(tag, sems, 0):
            copy.wait()
        for n, name in enumerate("PC"):
            low, high = refs["fx_lo"][e, n], refs["fx_hi"][e, n]
            both = jnp.where(slot_lane < EDGE, low, high)
            for k in range(levels):
                refs["HX" + name + tag][k] = lanes_by(both, -(SLOT * k + EDGE))
            if tag == "0" and name == "P":
                for k in range(levels):
                    refs["HXU0"][k] = lanes_by(low, -(SLOT * k + 6))
        for name, at in (("P", 4), ("C", 6)):
            z_wait(z_copies(name, tag, sems, at))
        if tag == "0":
            @pl.when(has_high)
            def _():
                wind_copies()[1].wait_send()

            @pl.when(has_low)
            def _():
                wind_copies()[1].wait_recv()

    def receive_y(name, tag):
        for copy in y_copies(name, tag, "f" + tag, 2 if name == "P" else 8):
            copy.wait()
        if tag == "0" and name == "P":
            wind_copies()[0].wait()

    def first_edges():
        for k in range(levels):
            x, y = refs["HXP0"][k], refs["HYP0"][k]
            refs["HXT0"][k] = jnp.where(lane == 0, lanes_by(x, 1), lanes_by(x, -1))
            refs["HYT0"][k] = jnp.where(row == 0, rows_by(y, 1), rows_by(y, -1))

    def send_thin(tag):
        sems = "t" + tag
        refs["tx_s"][THIN[tag]] = pack("P", tag)[0]
        for copy in y_copies("P", tag, sems, 2):
            copy.start()
        z_start(z_copies("P", tag, sems, 4))
        for copy in x_copies(tag, sems, 0):
            copy.start()

    def receive_thin(tag):
        sems, e = "t" + tag, THIN[tag]
        for copy in x_copies(tag, sems, 0):
            copy.wait()
        low, high = refs["tx_lo"][e], refs["tx_hi"][e]
        both = jnp.where(slot_lane == 1, lanes_by(low, 1), lanes_by(high, -1))
        for k in range(levels):
            refs["HXT" + tag][k] = lanes_by(both, -(SLOT * k + 1))
        z_wait(z_copies("P", tag, sems, 4))
        for copy in y_copies("P", tag, sems, 2):
            copy.wait()

    def sides(q, halo, by, index, extent):
        low = [by(jnp.where(index >= extent - n, halo, q), n) for n in (3, 2, 1)]
        high = [by(jnp.where(index < n, halo, q), -n) for n in (1, 2, 3)]
        return (*low, q, *high)

    def advect_xz(name, tag, rate):
        Q, HX = refs[name + tag], refs["HX" + name + tag]

        def level(k, below):
            u = refs["U" + tag][k]
            u_low = jnp.where(lane == 0, refs["HXU" + tag][k], lanes_by(u, 1))
            xs = sides(Q[k + 3], HX[k], lanes_by, lane, cols)
            above = flux(refs["W" + tag][k + 1], *(Q[k + n] for n in range(1, 7)))
            total = flux(u, *xs[1:]) - flux(u_low, *xs[:6])
            refs[rate][k] = total + (above - below)
            return above

        loop(levels, level, flux(refs["W" + tag][0], *(Q[n] for n in range(6))))

    def advect_y(name, tag, rate):
        Q, HY = refs[name + tag], refs["HY" + name + tag]

        def level(k, carry):
            v = refs["V" + tag][k]
            v_low = jnp.where(row == 0, refs["HYV" + tag][k], rows_by(v, 1))
            ys = sides(Q[k + 3], HY[k], rows_by, row, rows)
            total = refs[rate][k] + (flux(v, *ys[1:]) - flux(v_low, *ys[:6]))
            refs[rate][k] = total * (-1.0 / 60.0)
            return carry

        loop(levels, level, 0)

    def lift_of(tag):
        C = refs["C" + tag]
        lid_low = jnp.where(has_low, 1.0, 0.0)
        lid_high = jnp.where(has_high, 1.0, 0.0)
        for k in range(levels + 1):
            lift = (buoyancy * 0.5) * (C[k + 2] + C[k + 3])
            if k == 0:
                lift = lift * lid_low
            if k == levels:
                lift = lift * lid_high
            refs["lift"][k] = lift

    def substep(sp, sw, dp, dw, sub_step):
        SP, HXT, HYT = refs["P" + sp], refs["HXT" + sp], refs["HYT" + sp]
        SU, SV, SW, HXU, HYV = (refs[n + sw] for n in ("U", "V", "W", "HXU", "HYV"))
        push = sub_step * sound_speed
        lid_low = jnp.where(has_low, 1.0, 0.0)
        lid_high = jnp.where(has_high, 1.0, 0.0)
        last = dp is None

        def vertical(k):
            return SW[k] + sub_step * (
                refs["lift"][k] - sound_speed * (SP[k + 3] - SP[k + 2])
            )

        w_low = vertical(0) * lid_low
        if not last:
            refs["W" + dw][0] = w_low
        for k in range(levels):
            p, u, v = SP[k + 3], SU[k], SV[k]
            hx, hy = HXT[k], HYT[k]
            w = vertical(k + 1)
            if k == levels - 1:
                w = w * lid_high
            u_new = u - push * (jnp.where(lane == cols - 1, hx, lanes_by(p, -1)) - p)
            v_new = v - push * (jnp.where(row == rows - 1, hy, rows_by(p, -1)) - p)
            u_halo = HXU[k] - push * (p - hx)
            v_halo = HYV[k] - push * (p - hy)
            u_low = jnp.where(lane == 0, u_halo, lanes_by(u_new, 1))
            v_low = jnp.where(row == 0, v_halo, rows_by(v_new, 1))
            div = (u_new - u_low) + (v_new - v_low) + (w - w_low)
            p_new = p + sub_step * (refs["rate_p"][k] - sound_speed * div)
            w_low = w
            if last:
                for n, part in enumerate((p_new, u_new, v_new, w)):
                    out_fields[n + 1, k] = part
            else:
                refs["U" + dw][k] = u_new
                refs["V" + dw][k] = v_new
                refs["W" + dw][k + 1] = w
                refs["HXU" + dw][k] = u_halo
                refs["HYV" + dw][k] = v_halo
                refs["P" + dp][k + 3] = p_new

    def tracer(tag, scale):
        for k in range(levels):
            value = refs["C0"][k + 3] + scale * refs["rate_c"][k]
            if tag is None:
                out_fields[0, k] = value
                swell = jnp.exp(growth * value)
                refs["swell"][0, k] = swell
                refs["swell"][1, k] = swell * jnp.sqrt(swell)
            else:
                refs["C" + tag][k + 3] = value

    def droplet_terms():
        for copy in later_copies:
            copy.wait()

        def cell(k, carry):
            live = counts[k]
            for s in range(slots):
                r = jnp.abs(radius[s, k])
                number = jnp.where(live > s, weight[s, k], 0.0)
                area = number * (r * r)
                mass = area * r
                for m, term in enumerate((number, area, mass)):
                    high = term.astype(jnp.bfloat16).astype(jnp.float32)
                    vals[s, k, m * rows:(m + 1) * rows, :] = high
                    vals[s, k, (m + 3) * rows:(m + 4) * rows, :] = term - high
                vals[s, k, 6 * rows:, :] = jnp.zeros((2 * rows, cols), jnp.float32)
            return carry

        loop(levels, cell, 0, 2)

    def deposit(begin, cells):
        ids = lax.broadcasted_iota(jnp.int32, (cols, cols), 0).astype(jnp.float32).astype(jnp.bfloat16)
        one = jnp.ones((cols, cols), jnp.bfloat16)
        none = jnp.zeros((cols, cols), jnp.bfloat16)
        blank = jnp.zeros((8, cols), jnp.float32)

        def cell(n, carry):
            k, j = (begin + n) // rows, (begin + n) % rows
            by_depth = [None] * (FMAX + 1)
            for s in range(0, slots, 4):
                left, hots = [], []
                for t in range(4):
                    v = vals[s + t, k, pl.ds(j, 8, stride=rows), :]
                    left.append(jnp.concatenate([v, blank] if t % 2 == 0 else [blank, v], axis=1))
                    c = column[s + t, k, pl.ds(j, 1), :].astype(jnp.float32).astype(jnp.bfloat16)
                    hots.append(jnp.where(ids == jnp.broadcast_to(c, (cols, cols)), one, none))
                lhs = jnp.concatenate(left, axis=0).astype(jnp.bfloat16)
                rhs = jnp.concatenate(
                    [jnp.concatenate(hots[:2], axis=1), jnp.concatenate(hots[2:], axis=1)], axis=0
                )
                got = lax.dot_general(
                    lhs, rhs, (((1,), (1,)), ((), ())), preferred_element_type=jnp.float32
                )
                for t in range(4):
                    half = t // 2
                    part = got[8 * t:8 * (t + 1), half * cols:(half + 1) * cols]
                    fall = depth[s + t, j, 0, k]
                    for d in range(FMAX + 1):
                        term = jnp.where(fall == d, part, 0.0)
                        by_depth[d] = term if by_depth[d] is None else by_depth[d] + term
            at = pl.ds(pl.multiple_of(j * 8, 8), 8)
            for d in range(FMAX + 1):
                fallen[k, d, at, :] = by_depth[d]
            return carry

        lax.fori_loop(0, cells, cell, 0, unroll=min(CELLS, cells))

    def landed(m, l):
        total = None
        for d in range(FMAX + 1):
            k = l + d
            if not 0 <= k < levels:
                continue
            part = (
                fallen[k, d, pl.ds(m, rows, stride=8), :]
                + fallen[k, d, pl.ds(m + 3, rows, stride=8), :]
            )
            if m:
                part = part * refs["swell"][m - 1, k]
            total = part if total is None else total + part
        return total

    def fall_copy(m):
        return remote(refs["fall_s"].at[m], refs["fall_r"].at[m], "fall", m, "gz", -1)

    def fall_send(m):
        for l in range(FMAX):
            refs["fall_s"][m, l] = landed(m, l - FMAX)

        @pl.when(has_low)
        def _():
            fall_copy(m).start()

    def fall_home(m):
        for l in range(levels):
            moments[m, l] = landed(m, l)

    begins = [sum(CHUNKS[:n]) for n in range(len(CHUNKS))]
    cells = levels * rows

    def chunk(n):
        begin = min(begins[n], cells)
        end = cells if n == len(CHUNKS) - 1 else min(begins[n] + CHUNKS[n], cells)
        if end > begin:
            deposit(begin, end - begin)

    copies = max_start(0, top)
    send_full("0")
    droplet_terms()
    receive_xz("0")
    receive_y("P", "0")
    receive_y("C", "0")
    first_edges()
    lift_of("0")
    for name, rate in (("P", "rate_p"), ("C", "rate_c")):
        advect_xz(name, "0", rate)
        advect_y(name, "0", rate)
    for g in range(1, len(groups)):
        top = max_end(g - 1, top, copies)
        copies = max_start(g, top)
    chunk(0)
    top = max_end(len(groups) - 1, top, copies)
    time_step = courant_goal / (1.0 + jnp.max(top, axis=(0, 1), keepdims=True))
    time_step = jnp.broadcast_to(time_step, shape)

    def section(tag, part, after):
        receive_xz(tag)
        lift_of(tag)
        advect_xz("P", tag, "rate_p")
        receive_y("P", tag)
        advect_y("P", tag, "rate_p")
        substep("0", "0", after, after, part)
        send_thin(after)
        receive_y("C", tag)
        advect_xz("C", tag, "rate_c")
        advect_y("C", tag, "rate_c")

    third = time_step * (1.0 / 3.0)
    tracer("1", third)
    substep("0", "0", "1", "1", third)
    send_full("1")
    chunk(1)
    half = time_step * 0.5
    part = half / (NS // 2)
    section("1", part, "a")
    tracer("2", half)
    chunk(2)
    receive_thin("a")
    substep("a", "a", "2", "2", part)
    send_full("2")
    chunk(3)
    fall_send(0)
    part = time_step / NS
    section("2", part, "b")
    tracer(None, time_step)
    fall_send(1)
    fall_send(2)
    chunk(4)
    receive_thin("b")
    substep("b", "b", "c", "b", part)
    send_thin("c")
    chunk(5)
    receive_thin("c")
    substep("c", "b", "d", "b", part)
    send_thin("d")
    chunk(6)
    for m in range(3):
        fall_home(m)
    receive_thin("d")
    substep("d", "b", None, None, part)

    @pl.when(has_low)
    def _():
        for m in range(3):
            fall_copy(m).wait_send()

    @pl.when(has_high)
    def _():
        for m in range(3):
            fall_copy(m).wait_recv()
            for l in range(FMAX):
                at = levels - FMAX + l
                moments[m, at] = moments[m, at] + refs["fall_r"][m, l]


def per_device(fields, radius, weight, column, counts, fall_depth):
    levels, rows, cols = fields.shape[1:]
    slots = radius.shape[0]
    assert slots % 4 == 0 and levels * SLOT <= cols and rows == 8 and FMAX <= levels
    f32 = jnp.float32
    cell = (rows, cols)
    count = {a: lax.axis_size(a) for a in AXES}
    groups = max_groups(count)
    widest = max(len(shifts_of(g, count)) for g in groups)
    spaces = {}

    def add(name, *shape, dtype=f32):
        spaces[name] = pltpu.VMEM(shape, dtype)

    add("radius", *radius.shape)
    add("weight", *weight.shape)
    add("column", *column.shape, dtype=jnp.int32)
    add("counts", *counts.shape, dtype=jnp.int32)
    spaces["depth"] = pltpu.SMEM((slots, rows, 1, levels), jnp.int32)
    for tag in "012":
        add("C" + tag, levels + 6, *cell)
        for name in ("HXC", "HXP", "HYC", "HYP"):
            add(name + tag, levels, *cell)
    for tag in "012abcd":
        add("P" + tag, levels + 6, *cell)
    for tag in "0abcd":
        add("HXT" + tag, levels, *cell)
        add("HYT" + tag, levels, *cell)
    for tag in "012ab":
        for name in ("U", "V", "HXU", "HYV"):
            add(name + tag, levels, *cell)
        add("W" + tag, levels + 1, *cell)
    add("rate_c", levels, *cell)
    add("rate_p", levels, *cell)
    add("lift", levels + 1, *cell)
    add("swell", 2, levels, *cell)
    add("max_send", len(groups), 1, cols)
    add("max_recv", len(groups), widest, 1, cols)
    for end in ("_s", "_lo", "_hi"):
        add("fx" + end, len(FULL), 2, *cell)
        add("tx" + end, len(THIN), *cell)
    add("vals", slots, levels, 8 * rows, cols)
    add("fallen", levels, FMAX + 1, 8 * rows, cols)
    add("fall_s", 3, FMAX, *cell)
    add("fall_r", 3, FMAX, *cell)
    for end in ("_ss", "_rs"):
        for tag in FULL:
            spaces["f" + tag + end] = pltpu.SemaphoreType.DMA((12,))
        for tag in THIN:
            spaces["t" + tag + end] = pltpu.SemaphoreType.DMA((6,))
        spaces["fall" + end] = pltpu.SemaphoreType.DMA((3,))
        spaces["max" + end] = pltpu.SemaphoreType.DMA((len(groups), widest))
    spaces["local_sem"] = pltpu.SemaphoreType.DMA((10,))
    vmem = pl.BlockSpec(memory_space=pltpu.VMEM)
    anywhere = pl.BlockSpec(memory_space=pltpu.HBM)
    return pl.pallas_call(
        functools.partial(kernel, (tuple(spaces), levels, rows, cols, slots)),
        out_shape=(
            jax.ShapeDtypeStruct(fields.shape, f32),
            jax.ShapeDtypeStruct((3, levels, rows, cols), f32),
        ),
        in_specs=[anywhere] * 6,
        out_specs=(vmem, vmem),
        scratch_shapes=list(spaces.values()),
        compiler_params=pltpu.CompilerParams(
            collective_id=0, has_side_effects=True, vmem_limit_bytes=67043328
        ),
        name="slab_step",
    )(fall_depth.transpose(0, 2, 3, 1), fields, radius, weight, column, counts)


def solution(mesh):
    in_specs = (
        P(None, "gz", "gy", "gx"),
        P(None, "gz", "gy", "gx"),
        P(None, "gz", "gy", "gx"),
        P(None, "gz", "gy", "gx"),
        P("gz", "gy", "gx"),
        P(None, "gz", "gy", "gx"),
    )
    out_specs = (P(None, "gz", "gy", "gx"), P(None, "gz", "gy", "gx"))
    return jax.shard_map(
        per_device, mesh=mesh, in_specs=in_specs, out_specs=out_specs, check_vma=False
    )
```

```python
import functools
import itertools
import jax
import jax.numpy as jnp
from jax import lax
from jax.experimental import pallas as pl
from jax.experimental.pallas import tpu as pltpu
from jax.sharding import PartitionSpec as P

NS = 4
FMAX = 8
CELLS = 8
SLOT = 8
EDGE = 3
CHUNKS = (24, 24, 16, 24, 8, 16, 16)
ONE_SHOT = 32
KERNEL_BYTES = 40 * 1024 * 1024

sound_speed = 10.0
buoyancy = 0.5
courant_goal = 0.6
growth = 0.3

MESH = pl.DeviceIdType.MESH
AXES = ("gy", "gx", "gz")
FULL = {"0": 0, "1": 1, "2": 2}
THIN = {"a": 0, "b": 1, "c": 2, "d": 3}


def flux(wind, a, b, c, d, e, f):
    central = 37.0 * (c + d) - 8.0 * (b + e) + (a + f)
    upwind = 10.0 * (d - c) - 5.0 * (e - b) + (f - a)
    return wind * central - jnp.abs(wind) * upwind


def max_groups(count):
    total = 1
    for a in AXES:
        total *= count[a]
    return (AXES,) if total <= ONE_SHOT else tuple((a,) for a in AXES)


def shifts_of(group, count):
    return [s for s in itertools.product(*(range(count[a]) for a in group)) if any(s)]


def kernel(
    sizes, depth_hbm, fields_hbm, radius_hbm, weight_hbm, column_hbm, counts_hbm,
    out_fields, moments, *scratch
):
    names, levels, rows, cols, slots = sizes
    refs = dict(zip(names, scratch))
    radius, weight, column, counts = (refs[n] for n in ("radius", "weight", "column", "counts"))
    depth = refs["depth"]
    vals, fallen = refs["vals"], refs["fallen"]
    local_sem = refs["local_sem"]
    shape = (rows, cols)
    lane = lax.broadcasted_iota(jnp.int32, shape, 1)
    row = lax.broadcasted_iota(jnp.int32, shape, 0)
    slot_lane = lane % SLOT
    place = {a: lax.axis_index(a) for a in AXES}
    count = {a: lax.axis_size(a) for a in AXES}
    groups = max_groups(count)
    has_low = place["gz"] > 0
    has_high = place["gz"] < count["gz"] - 1
    zero = jnp.zeros(shape, jnp.float32)

    def lanes_by(x, shift):
        return pltpu.roll(x, shift % cols, 1)

    def rows_by(x, shift):
        return pltpu.roll(x, shift % rows, 0)

    def loop(n, body, carry, unroll=True):
        return lax.fori_loop(0, n, body, carry, unroll=unroll)

    first_copies = []
    for n, dst in enumerate(
        (refs["C0"].at[pl.ds(3, levels)], refs["P0"].at[pl.ds(3, levels)],
         refs["U0"], refs["V0"], refs["W0"].at[pl.ds(1, levels)])
    ):
        first_copies.append(pltpu.make_async_copy(fields_hbm.at[n], dst, local_sem.at[n]))
    later_copies = []
    for n, (src, dst) in enumerate(
        ((counts_hbm, counts), (weight_hbm, weight), (radius_hbm, radius),
         (column_hbm, column), (depth_hbm, depth))
    ):
        later_copies.append(pltpu.make_async_copy(src, dst, local_sem.at[5 + n]))
    for copy in first_copies + later_copies:
        copy.start()

    def away(group, shift):
        return {a: lax.rem(place[a] + s, count[a]) for a, s in zip(group, shift) if s}

    barrier = pltpu.get_barrier_semaphore()
    peers = 0
    for group in groups:
        for shift in shifts_of(group, count):
            pl.semaphore_signal(barrier, inc=1, device_id=away(group, shift), device_id_type=MESH)
            peers += 1

    for copy in first_copies:
        copy.wait()

    @pl.when(jnp.logical_not(has_high))
    def _():
        refs["W0"][levels] = zero
        for tag in ("0", "1", "2"):
            for t in range(EDGE):
                refs["C" + tag][3 + levels + t] = zero
        for tag in "012abcd":
            for t in range(EDGE if tag in FULL else 1):
                refs["P" + tag][3 + levels + t] = zero

    @pl.when(jnp.logical_not(has_low))
    def _():
        refs["W0"][0] = zero
        for tag in ("0", "1", "2"):
            for t in range(EDGE):
                refs["C" + tag][t] = zero
        for tag in "012abcd":
            for t in range(3 - (EDGE if tag in FULL else 1), 3):
                refs["P" + tag][t] = zero

    def fastest(k, top):
        speed = jnp.abs(refs["U0"][k]) + jnp.abs(refs["V0"][k]) + jnp.abs(refs["W0"][k + 1])
        return jnp.maximum(top, speed)

    top = loop(levels, fastest, zero)
    top = jnp.max(top, axis=0, keepdims=True)
    pl.semaphore_wait(barrier, peers)

    def max_start(g, value):
        refs["max_send"][g] = value
        copies = []
        for n, shift in enumerate(shifts_of(groups[g], count)):
            copy = pltpu.make_async_remote_copy(
                src_ref=refs["max_send"].at[g],
                dst_ref=refs["max_recv"].at[g, n],
                send_sem=refs["max_ss"].at[g, n],
                recv_sem=refs["max_rs"].at[g, n],
                device_id=away(groups[g], shift), device_id_type=MESH,
            )
            copy.start()
            copies.append(copy)
        return copies

    def max_end(g, value, copies):
        for copy in copies:
            copy.wait()
        for n in range(len(copies)):
            value = jnp.maximum(value, refs["max_recv"][g, n])
        return value

    def neighbour(a, step):
        return {a: lax.rem(place[a] + count[a] + step, count[a])}

    def remote(src, dst, sems, n, a, step):
        return pltpu.make_async_remote_copy(
            src_ref=src, dst_ref=dst, send_sem=refs[sems + "_ss"].at[n],
            recv_sem=refs[sems + "_rs"].at[n],
            device_id=neighbour(a, step), device_id_type=MESH,
        )

    def y_copies(name, tag, sems, at):
        source = refs[name + tag]
        if tag in FULL:
            w, low, high, dst = EDGE, rows - EDGE, 0, refs["HY" + name + tag]
        else:
            w, low, high, dst = 1, 0, rows - 1, refs["HYT" + tag]
        own = pl.ds(3, levels)
        return (
            remote(source.at[own, pl.ds(rows - w, w), :], dst.at[:, pl.ds(low, w), :],
                   sems, at, "gy", 1),
            remote(source.at[own, pl.ds(0, w), :], dst.at[:, pl.ds(high, w), :],
                   sems, at + 1, "gy", -1),
        )

    def z_copies(name, tag, sems, at):
        w = EDGE if tag in FULL else 1
        q = refs[name + tag]
        return (
            remote(q.at[pl.ds(3 + levels - w, w)], q.at[pl.ds(3 - w, w)], sems, at, "gz", 1),
            remote(q.at[pl.ds(3, w)], q.at[pl.ds(3 + levels, w)], sems, at + 1, "gz", -1),
        )

    def x_copies(tag, sems, at):
        kind, e = ("fx", FULL[tag]) if tag in FULL else ("tx", THIN[tag])
        return (
            remote(refs[kind + "_s"].at[e], refs[kind + "_lo"].at[e], sems, at, "gx", 1),
            remote(refs[kind + "_s"].at[e], refs[kind + "_hi"].at[e], sems, at + 1, "gx", -1),
        )

    def z_start(pair):
        @pl.when(has_high)
        def _():
            pair[0].start()

        @pl.when(has_low)
        def _():
            pair[1].start()

    def z_wait(pair):
        @pl.when(has_high)
        def _():
            pair[0].wait_send()
            pair[1].wait_recv()

        @pl.when(has_low)
        def _():
            pair[1].wait_send()
            pair[0].wait_recv()

    def wind_copies():
        own = refs["V0"].at[:, pl.ds(rows - 1, 1), :]
        return (
            remote(own, refs["HYV0"].at[:, pl.ds(0, 1), :], "f0", 10, "gy", 1),
            remote(refs["W0"].at[levels], refs["W0"].at[0], "f0", 11, "gz", 1),
        )

    def pack(names_at, tag):
        def body(k, packed):
            out = []
            for name, got in zip(names_at, packed):
                edge = lanes_by(refs[name + tag][k + 3], SLOT * k + (EDGE if tag in FULL else 1))
                if tag == "0" and name == "P":
                    edge = jnp.where(
                        slot_lane == 6, lanes_by(refs["U0"][k], SLOT * k + 7), edge
                    )
                out.append(jnp.where(lane // SLOT == k, edge, got))
            return tuple(out)

        packed = (zero,) * len(names_at)
        for k in range(levels):
            packed = body(k, packed)
        return packed

    def send_full(tag):
        sems, e = "f" + tag, FULL[tag]
        x = x_copies(tag, sems, 0)
        for n, part in enumerate(pack("PC", tag)):
            refs["fx_s"][e, n] = part
        for copy in y_copies("P", tag, sems, 2):
            copy.start()
        if tag == "0":
            wind_copies()[0].start()
        for name, at in (("P", 4), ("C", 6)):
            z_start(z_copies(name, tag, sems, at))
        if tag == "0":
            @pl.when(has_high)
            def _():
                wind_copies()[1].start()
        for copy in x:
            copy.start()
        for copy in y_copies("C", tag, sems, 8):
            copy.start()

    def receive_xz(tag):
        sems, e = "f" + tag, FULL[tag]
        for copy in x_copies(tag, sems, 0):
            copy.wait()
        for n, name in enumerate("PC"):
            low, high = refs["fx_lo"][e, n], refs["fx_hi"][e, n]
            both = jnp.where(slot_lane < EDGE, low, high)
            for k in range(levels):
                refs["HX" + name + tag][k] = lanes_by(both, -(SLOT * k + EDGE))
            if tag == "0" and name == "P":
                for k in range(levels):
                    refs["HXU0"][k] = lanes_by(low, -(SLOT * k + 6))
        for name, at in (("P", 4), ("C", 6)):
            z_wait(z_copies(name, tag, sems, at))
        if tag == "0":
            @pl.when(has_high)
            def _():
                wind_copies()[1].wait_send()

            @pl.when(has_low)
            def _():
                wind_copies()[1].wait_recv()

    def receive_y(name, tag):
        for copy in y_copies(name, tag, "f" + tag, 2 if name == "P" else 8):
            copy.wait()
        if tag == "0" and name == "P":
            wind_copies()[0].wait()

    def first_edges():
        for k in range(levels):
            x, y = refs["HXP0"][k], refs["HYP0"][k]
            refs["HXT0"][k] = jnp.where(lane == 0, lanes_by(x, 1), lanes_by(x, -1))
            refs["HYT0"][k] = jnp.where(row == 0, rows_by(y, 1), rows_by(y, -1))

    def send_thin(tag):
        sems = "t" + tag
        refs["tx_s"][THIN[tag]] = pack("P", tag)[0]
        for copy in y_copies("P", tag, sems, 2):
            copy.start()
        z_start(z_copies("P", tag, sems, 4))
        for copy in x_copies(tag, sems, 0):
            copy.start()

    def receive_thin(tag):
        sems, e = "t" + tag, THIN[tag]
        for copy in x_copies(tag, sems, 0):
            copy.wait()
        low, high = refs["tx_lo"][e], refs["tx_hi"][e]
        both = jnp.where(slot_lane == 1, lanes_by(low, 1), lanes_by(high, -1))
        for k in range(levels):
            refs["HXT" + tag][k] = lanes_by(both, -(SLOT * k + 1))
        z_wait(z_copies("P", tag, sems, 4))
        for copy in y_copies("P", tag, sems, 2):
            copy.wait()

    def sides(q, halo, by, index, extent):
        low = [by(jnp.where(index >= extent - n, halo, q), n) for n in (3, 2, 1)]
        high = [by(jnp.where(index < n, halo, q), -n) for n in (1, 2, 3)]
        return (*low, q, *high)

    def advect_xz(name, tag, rate):
        Q, HX = refs[name + tag], refs["HX" + name + tag]

        def level(k, below):
            u = refs["U" + tag][k]
            u_low = jnp.where(lane == 0, refs["HXU" + tag][k], lanes_by(u, 1))
            xs = sides(Q[k + 3], HX[k], lanes_by, lane, cols)
            above = flux(refs["W" + tag][k + 1], *(Q[k + n] for n in range(1, 7)))
            total = flux(u, *xs[1:]) - flux(u_low, *xs[:6])
            refs[rate][k] = total + (above - below)
            return above

        loop(levels, level, flux(refs["W" + tag][0], *(Q[n] for n in range(6))))

    def advect_y(name, tag, rate):
        Q, HY = refs[name + tag], refs["HY" + name + tag]

        def level(k, carry):
            v = refs["V" + tag][k]
            v_low = jnp.where(row == 0, refs["HYV" + tag][k], rows_by(v, 1))
            ys = sides(Q[k + 3], HY[k], rows_by, row, rows)
            total = refs[rate][k] + (flux(v, *ys[1:]) - flux(v_low, *ys[:6]))
            refs[rate][k] = total * (-1.0 / 60.0)
            return carry

        loop(levels, level, 0)

    def lift_of(tag):
        C = refs["C" + tag]
        lid_low = jnp.where(has_low, 1.0, 0.0)
        lid_high = jnp.where(has_high, 1.0, 0.0)
        for k in range(levels + 1):
            lift = (buoyancy * 0.5) * (C[k + 2] + C[k + 3])
            if k == 0:
                lift = lift * lid_low
            if k == levels:
                lift = lift * lid_high
            refs["lift"][k] = lift

    def substep(sp, sw, dp, dw, sub_step):
        SP, HXT, HYT = refs["P" + sp], refs["HXT" + sp], refs["HYT" + sp]
        SU, SV, SW, HXU, HYV = (refs[n + sw] for n in ("U", "V", "W", "HXU", "HYV"))
        push = sub_step * sound_speed
        lid_low = jnp.where(has_low, 1.0, 0.0)
        lid_high = jnp.where(has_high, 1.0, 0.0)
        last = dp is None

        def vertical(k):
            return SW[k] + sub_step * (
                refs["lift"][k] - sound_speed * (SP[k + 3] - SP[k + 2])
            )

        w_low = vertical(0) * lid_low
        if not last:
            refs["W" + dw][0] = w_low
        for k in range(levels):
            p, u, v = SP[k + 3], SU[k], SV[k]
            hx, hy = HXT[k], HYT[k]
            w = vertical(k + 1)
            if k == levels - 1:
                w = w * lid_high
            u_new = u - push * (jnp.where(lane == cols - 1, hx, lanes_by(p, -1)) - p)
            v_new = v - push * (jnp.where(row == rows - 1, hy, rows_by(p, -1)) - p)
            u_halo = HXU[k] - push * (p - hx)
            v_halo = HYV[k] - push * (p - hy)
            u_low = jnp.where(lane == 0, u_halo, lanes_by(u_new, 1))
            v_low = jnp.where(row == 0, v_halo, rows_by(v_new, 1))
            div = (u_new - u_low) + (v_new - v_low) + (w - w_low)
            p_new = p + sub_step * (refs["rate_p"][k] - sound_speed * div)
            w_low = w
            if last:
                for n, part in enumerate((p_new, u_new, v_new, w)):
                    out_fields[n + 1, k] = part
            else:
                refs["U" + dw][k] = u_new
                refs["V" + dw][k] = v_new
                refs["W" + dw][k + 1] = w
                refs["HXU" + dw][k] = u_halo
                refs["HYV" + dw][k] = v_halo
                refs["P" + dp][k + 3] = p_new

    def tracer(tag, scale):
        for k in range(levels):
            value = refs["C0"][k + 3] + scale * refs["rate_c"][k]
            if tag is None:
                out_fields[0, k] = value
                swell = jnp.exp(growth * value)
                refs["swell"][0, k] = swell
                refs["swell"][1, k] = swell * jnp.sqrt(swell)
            else:
                refs["C" + tag][k + 3] = value

    def droplet_terms():
        for copy in later_copies:
            copy.wait()

        def cell(k, carry):
            live = counts[k]
            for s in range(slots):
                r = jnp.abs(radius[s, k])
                number = jnp.where(live > s, weight[s, k], 0.0)
                area = number * (r * r)
                mass = area * r
                for m, term in enumerate((number, area, mass)):
                    high = term.astype(jnp.bfloat16).astype(jnp.float32)
                    vals[s, k, m * rows:(m + 1) * rows, :] = high
                    vals[s, k, (m + 3) * rows:(m + 4) * rows, :] = term - high
                vals[s, k, 6 * rows:, :] = jnp.zeros((2 * rows, cols), jnp.float32)
            return carry

        loop(levels, cell, 0, 2)

    def deposit(begin, cells):
        ids = lax.broadcasted_iota(jnp.int32, (cols, cols), 0).astype(jnp.float32).astype(jnp.bfloat16)
        one = jnp.ones((cols, cols), jnp.bfloat16)
        none = jnp.zeros((cols, cols), jnp.bfloat16)
        blank = jnp.zeros((8, cols), jnp.float32)

        def cell(n, carry):
            k, j = (begin + n) // rows, (begin + n) % rows
            by_depth = [None] * (FMAX + 1)
            for s in range(0, slots, 4):
                left, hots = [], []
                for t in range(4):
                    v = vals[s + t, k, pl.ds(j, 8, stride=rows), :]
                    left.append(jnp.concatenate([v, blank] if t % 2 == 0 else [blank, v], axis=1))
                    c = column[s + t, k, pl.ds(j, 1), :].astype(jnp.float32).astype(jnp.bfloat16)
                    hots.append(jnp.where(ids == jnp.broadcast_to(c, (cols, cols)), one, none))
                lhs = jnp.concatenate(left, axis=0).astype(jnp.bfloat16)
                rhs = jnp.concatenate(
                    [jnp.concatenate(hots[:2], axis=1), jnp.concatenate(hots[2:], axis=1)], axis=0
                )
                got = lax.dot_general(
                    lhs, rhs, (((1,), (1,)), ((), ())), preferred_element_type=jnp.float32
                )
                for t in range(4):
                    half = t // 2
                    part = got[8 * t:8 * (t + 1), half * cols:(half + 1) * cols]
                    fall = depth[s + t, j, 0, k]
                    for d in range(FMAX + 1):
                        term = jnp.where(fall == d, part, 0.0)
                        by_depth[d] = term if by_depth[d] is None else by_depth[d] + term
            at = pl.ds(pl.multiple_of(j * 8, 8), 8)
            for d in range(FMAX + 1):
                fallen[k, d, at, :] = by_depth[d]
            return carry

        lax.fori_loop(0, cells, cell, 0, unroll=min(CELLS, cells))

    def landed(m, l):
        total = None
        for d in range(FMAX + 1):
            k = l + d
            if not 0 <= k < levels:
                continue
            part = (
                fallen[k, d, pl.ds(m, rows, stride=8), :]
                + fallen[k, d, pl.ds(m + 3, rows, stride=8), :]
            )
            if m:
                part = part * refs["swell"][m - 1, k]
            total = part if total is None else total + part
        return total

    def fall_copy(m):
        return remote(refs["fall_s"].at[m], refs["fall_r"].at[m], "fall", m, "gz", -1)

    def fall_send(m):
        for l in range(FMAX):
            refs["fall_s"][m, l] = landed(m, l - FMAX)

        @pl.when(has_low)
        def _():
            fall_copy(m).start()

    def fall_home(m):
        for l in range(levels):
            moments[m, l] = landed(m, l)

    begins = [sum(CHUNKS[:n]) for n in range(len(CHUNKS))]
    cells = levels * rows

    def chunk(n):
        begin = min(begins[n], cells)
        end = cells if n == len(CHUNKS) - 1 else min(begins[n] + CHUNKS[n], cells)
        if end > begin:
            deposit(begin, end - begin)

    copies = max_start(0, top)
    send_full("0")
    droplet_terms()
    if len(groups) > 1:
        chunk(0)
        top = max_end(0, top, copies)
        copies = max_start(1, top)
        for g in range(2, len(groups)):
            top = max_end(g - 1, top, copies)
            copies = max_start(g, top)
    else:
        chunk(0)
    receive_xz("0")
    receive_y("P", "0")
    receive_y("C", "0")
    first_edges()
    lift_of("0")
    for name, rate in (("P", "rate_p"), ("C", "rate_c")):
        advect_xz(name, "0", rate)
        advect_y(name, "0", rate)
    top = max_end(len(groups) - 1, top, copies)
    time_step = courant_goal / (1.0 + jnp.max(top, axis=(0, 1), keepdims=True))
    time_step = jnp.broadcast_to(time_step, shape)

    def section(tag, part, after):
        receive_xz(tag)
        lift_of(tag)
        advect_xz("P", tag, "rate_p")
        receive_y("P", tag)
        advect_y("P", tag, "rate_p")
        substep("0", "0", after, after, part)
        send_thin(after)
        receive_y("C", tag)
        advect_xz("C", tag, "rate_c")
        advect_y("C", tag, "rate_c")

    third = time_step * (1.0 / 3.0)
    tracer("1", third)
    substep("0", "0", "1", "1", third)
    send_full("1")
    chunk(1)
    half = time_step * 0.5
    part = half / (NS // 2)
    section("1", part, "a")
    tracer("2", half)
    chunk(2)
    receive_thin("a")
    substep("a", "a", "2", "2", part)
    send_full("2")
    chunk(3)
    fall_send(0)
    part = time_step / NS
    section("2", part, "b")
    tracer(None, time_step)
    fall_send(1)
    fall_send(2)
    chunk(4)
    receive_thin("b")
    substep("b", "b", "c", "b", part)
    send_thin("c")
    chunk(5)
    receive_thin("c")
    substep("c", "b", "d", "b", part)
    send_thin("d")
    chunk(6)
    for m in range(3):
        fall_home(m)
    receive_thin("d")
    substep("d", "b", None, None, part)

    @pl.when(has_low)
    def _():
        for m in range(3):
            fall_copy(m).wait_send()

    @pl.when(has_high)
    def _():
        for m in range(3):
            fall_copy(m).wait_recv()
            for l in range(FMAX):
                at = levels - FMAX + l
                moments[m, at] = moments[m, at] + refs["fall_r"][m, l]


def write_out(fields, moments, out_fields, out_moments, sem):
    copies = [
        pltpu.make_async_copy(fields, out_fields, sem.at[0]),
        pltpu.make_async_copy(moments, out_moments, sem.at[1]),
    ]
    for copy in copies:
        copy.start()
    for copy in copies:
        copy.wait()


def per_device(fields, radius, weight, column, counts, fall_depth):
    levels, rows, cols = fields.shape[1:]
    slots = radius.shape[0]
    assert slots % 4 == 0 and levels * SLOT <= cols and rows == 8 and FMAX <= levels
    f32 = jnp.float32
    cell = (rows, cols)
    count = {a: lax.axis_size(a) for a in AXES}
    groups = max_groups(count)
    widest = max(len(shifts_of(g, count)) for g in groups)
    spaces = {}

    def add(name, *shape, dtype=f32):
        spaces[name] = pltpu.VMEM(shape, dtype)

    add("radius", *radius.shape)
    add("weight", *weight.shape)
    add("column", *column.shape, dtype=jnp.int32)
    add("counts", *counts.shape, dtype=jnp.int32)
    spaces["depth"] = pltpu.SMEM((slots, rows, 1, levels), jnp.int32)
    for tag in "012":
        add("C" + tag, levels + 6, *cell)
        for name in ("HXC", "HXP", "HYC", "HYP"):
            add(name + tag, levels, *cell)
    for tag in "012abcd":
        add("P" + tag, levels + 6, *cell)
    for tag in "0abcd":
        add("HXT" + tag, levels, *cell)
        add("HYT" + tag, levels, *cell)
    for tag in "012ab":
        for name in ("U", "V", "HXU", "HYV"):
            add(name + tag, levels, *cell)
        add("W" + tag, levels + 1, *cell)
    add("rate_c", levels, *cell)
    add("rate_p", levels, *cell)
    add("lift", levels + 1, *cell)
    add("swell", 2, levels, *cell)
    add("max_send", len(groups), 1, cols)
    add("max_recv", len(groups), widest, 1, cols)
    for end in ("_s", "_lo", "_hi"):
        add("fx" + end, len(FULL), 2, *cell)
        add("tx" + end, len(THIN), *cell)
    add("vals", slots, levels, 8 * rows, cols)
    add("fallen", levels, FMAX + 1, 8 * rows, cols)
    add("fall_s", 3, FMAX, *cell)
    add("fall_r", 3, FMAX, *cell)
    for end in ("_ss", "_rs"):
        for tag in FULL:
            spaces["f" + tag + end] = pltpu.SemaphoreType.DMA((12,))
        for tag in THIN:
            spaces["t" + tag + end] = pltpu.SemaphoreType.DMA((6,))
        spaces["fall" + end] = pltpu.SemaphoreType.DMA((3,))
        spaces["max" + end] = pltpu.SemaphoreType.DMA((len(groups), widest))
    spaces["local_sem"] = pltpu.SemaphoreType.DMA((10,))
    vmem = pl.BlockSpec(memory_space=pltpu.VMEM)
    anywhere = pl.BlockSpec(memory_space=pltpu.HBM)
    results = pl.pallas_call(
        functools.partial(kernel, (tuple(spaces), levels, rows, cols, slots)),
        out_shape=(
            jax.ShapeDtypeStruct(fields.shape, f32),
            jax.ShapeDtypeStruct((3, levels, rows, cols), f32),
        ),
        in_specs=[anywhere] * 6,
        out_specs=(vmem, vmem),
        scratch_shapes=list(spaces.values()),
        compiler_params=pltpu.CompilerParams(
            collective_id=0, has_side_effects=True,
            vmem_limit_bytes=KERNEL_BYTES,
        ),
        name="slab_step",
    )(*(
        pltpu.with_memory_space_constraint(x, pltpu.HBM)
        for x in (fall_depth.transpose(0, 2, 3, 1), fields, radius, weight, column, counts)
    ))
    return pl.pallas_call(
        write_out,
        out_shape=tuple(jax.ShapeDtypeStruct(r.shape, f32) for r in results),
        in_specs=[vmem] * 2,
        out_specs=(anywhere,) * 2,
        scratch_shapes=[pltpu.SemaphoreType.DMA((2,))],
        compiler_params=pltpu.CompilerParams(vmem_limit_bytes=1024 * 1024),
        name="write_out",
    )(*results)


def solution(mesh):
    in_specs = (
        P(None, "gz", "gy", "gx"),
        P(None, "gz", "gy", "gx"),
        P(None, "gz", "gy", "gx"),
        P(None, "gz", "gy", "gx"),
        P("gz", "gy", "gx"),
        P(None, "gz", "gy", "gx"),
    )
    out_specs = (P(None, "gz", "gy", "gx"), P(None, "gz", "gy", "gx"))
    return jax.shard_map(
        per_device, mesh=mesh, in_specs=in_specs, out_specs=out_specs, check_vma=False
    )
```

```python
import functools
import itertools
import jax
import jax.numpy as jnp
from jax import lax
from jax.experimental import pallas as pl
from jax.experimental.pallas import tpu as pltpu
from jax.sharding import PartitionSpec as P

NS = 4
FMAX = 8
CELLS = 8
SLOT = 8
EDGE = 3
CHUNKS = (32, 24, 28, 24, 20)
ONE_SHOT = 32
KERNEL_BYTES = 40 * 1024 * 1024

sound_speed = 10.0
buoyancy = 0.5
courant_goal = 0.6
growth = 0.3

MESH = pl.DeviceIdType.MESH
AXES = ("gy", "gx", "gz")
FULL = {"0": 0, "1": 1, "2": 2}
THIN = {"c": 0, "d": 1}
DELTA = {"a": 0, "b": 1}


def flux(wind, a, b, c, d, e, f):
    central = 37.0 * (c + d) - 8.0 * (b + e) + (a + f)
    upwind = 10.0 * (d - c) - 5.0 * (e - b) + (f - a)
    return wind * central - jnp.abs(wind) * upwind


def max_groups(count):
    total = 1
    for a in AXES:
        total *= count[a]
    return (AXES,) if total <= ONE_SHOT else tuple((a,) for a in AXES)


def shifts_of(group, count):
    return [s for s in itertools.product(*(range(count[a]) for a in group)) if any(s)]


def greeted(groups, count):
    found = {}
    diagonals = [
        (pair, steps)
        for pair in itertools.combinations(AXES, 2)
        for steps in itertools.product((1, -1), repeat=2)
    ]
    for group, shift in [(g, s) for g in groups for s in shifts_of(g, count)] + diagonals:
        step = {a: s % count[a] for a, s in zip(group, shift) if s % count[a]}
        if step:
            found[tuple(sorted(step.items()))] = step
    return list(found.values())


def kernel(
    sizes, depth_hbm, fields_hbm, radius_hbm, weight_hbm, column_hbm, counts_hbm,
    out_fields, moments, *scratch
):
    names, levels, rows, cols, slots = sizes
    refs = dict(zip(names, scratch))
    radius, weight, column, counts = (refs[n] for n in ("radius", "weight", "column", "counts"))
    depth = refs["depth"]
    vals, fallen = refs["vals"], refs["fallen"]
    local_sem = refs["local_sem"]
    shape = (rows, cols)
    lane = lax.broadcasted_iota(jnp.int32, shape, 1)
    row = lax.broadcasted_iota(jnp.int32, shape, 0)
    slot_lane = lane % SLOT
    place = {a: lax.axis_index(a) for a in AXES}
    count = {a: lax.axis_size(a) for a in AXES}
    groups = max_groups(count)
    has_low = place["gz"] > 0
    has_high = place["gz"] < count["gz"] - 1
    zero = jnp.zeros(shape, jnp.float32)

    def lanes_by(x, shift):
        return pltpu.roll(x, shift % cols, 1)

    def rows_by(x, shift):
        return pltpu.roll(x, shift % rows, 0)

    def loop(n, body, carry, unroll=True):
        return lax.fori_loop(0, n, body, carry, unroll=unroll)

    first_copies = []
    for n, dst in enumerate(
        (refs["C0"].at[pl.ds(3, levels)], refs["P0"].at[pl.ds(3, levels)],
         refs["U0"], refs["V0"], refs["W0"].at[pl.ds(1, levels)])
    ):
        first_copies.append(pltpu.make_async_copy(fields_hbm.at[n], dst, local_sem.at[n]))
    later_copies = []
    for n, (src, dst) in enumerate(
        ((counts_hbm, counts), (weight_hbm, weight), (radius_hbm, radius),
         (column_hbm, column), (depth_hbm, depth))
    ):
        later_copies.append(pltpu.make_async_copy(src, dst, local_sem.at[5 + n]))
    for copy in first_copies + later_copies:
        copy.start()

    def away(group, shift):
        return {a: lax.rem(place[a] + s, count[a]) for a, s in zip(group, shift) if s}

    barrier = pltpu.get_barrier_semaphore()
    peers = 0
    for step in greeted(groups, count):
        pl.semaphore_signal(
            barrier, inc=1, device_id=away(tuple(step), tuple(step.values())),
            device_id_type=MESH,
        )
        peers += 1

    for copy in first_copies:
        copy.wait()

    @pl.when(jnp.logical_not(has_high))
    def _():
        refs["W0"][levels] = zero
        for tag in ("0", "1", "2"):
            for t in range(EDGE):
                refs["C" + tag][3 + levels + t] = zero
        for tag in "012abcd":
            for t in range(EDGE if tag in FULL else 1):
                refs["P" + tag][3 + levels + t] = zero

    @pl.when(jnp.logical_not(has_low))
    def _():
        refs["W0"][0] = zero
        for tag in ("0", "1", "2"):
            for t in range(EDGE):
                refs["C" + tag][t] = zero
        for tag in "012abcd":
            for t in range(3 - (EDGE if tag in FULL else 1), 3):
                refs["P" + tag][t] = zero

    def fastest(k, top):
        speed = jnp.abs(refs["U0"][k]) + jnp.abs(refs["V0"][k]) + jnp.abs(refs["W0"][k + 1])
        return jnp.maximum(top, speed)

    top = loop(levels, fastest, zero)
    top = jnp.max(top, axis=0, keepdims=True)
    pl.semaphore_wait(barrier, peers)

    def max_start(g, value):
        refs["max_send"][g] = value
        copies = []
        for n, shift in enumerate(shifts_of(groups[g], count)):
            copy = pltpu.make_async_remote_copy(
                src_ref=refs["max_send"].at[g],
                dst_ref=refs["max_recv"].at[g, n],
                send_sem=refs["max_ss"].at[g, n],
                recv_sem=refs["max_rs"].at[g, n],
                device_id=away(groups[g], shift), device_id_type=MESH,
            )
            copy.start()
            copies.append(copy)
        return copies

    def max_end(g, value, copies):
        for copy in copies:
            copy.wait()
        for n in range(len(copies)):
            value = jnp.maximum(value, refs["max_recv"][g, n])
        return value

    def neighbour(*steps):
        return {
            a: lax.rem(place[a] + count[a] + step, count[a])
            for a, step in zip(steps[::2], steps[1::2])
        }

    def remote(src, dst, sems, n, *steps):
        return pltpu.make_async_remote_copy(
            src_ref=src, dst_ref=dst, send_sem=refs[sems + "_ss"].at[n],
            recv_sem=refs[sems + "_rs"].at[n],
            device_id=neighbour(*steps), device_id_type=MESH,
        )

    def y_copies(name, tag, sems, at):
        source = refs[name + tag]
        if tag in FULL:
            w, low, high, dst = EDGE, rows - EDGE, 0, refs["HY" + name + tag]
        else:
            w, low, high, dst = 1, 0, rows - 1, refs["HYT" + tag]
        own = pl.ds(3, levels)
        return (
            remote(source.at[own, pl.ds(rows - w, w), :], dst.at[:, pl.ds(low, w), :],
                   sems, at, "gy", 1),
            remote(source.at[own, pl.ds(0, w), :], dst.at[:, pl.ds(high, w), :],
                   sems, at + 1, "gy", -1),
        )

    def z_copies(name, tag, sems, at):
        w = EDGE if tag in FULL else 1
        q = refs[name + tag]
        return (
            remote(q.at[pl.ds(3 + levels - w, w)], q.at[pl.ds(3 - w, w)], sems, at, "gz", 1),
            remote(q.at[pl.ds(3, w)], q.at[pl.ds(3 + levels, w)], sems, at + 1, "gz", -1),
        )

    def x_copies(kind, e, sems, at):
        return (
            remote(refs[kind + "_s"].at[e], refs[kind + "_lo"].at[e], sems, at, "gx", 1),
            remote(refs[kind + "_s"].at[e], refs[kind + "_hi"].at[e], sems, at + 1, "gx", -1),
        )

    def start(copies):
        for copy in copies:
            copy.start()

    def wait(copies):
        for copy in copies:
            copy.wait()

    def z_start(up, down):
        @pl.when(has_high)
        def _():
            start(up)

        @pl.when(has_low)
        def _():
            start(down)

    def z_wait(up, down):
        @pl.when(has_high)
        def _():
            for copy in up:
                copy.wait_send()
            for copy in down:
                copy.wait_recv()

        @pl.when(has_low)
        def _():
            for copy in down:
                copy.wait_send()
            for copy in up:
                copy.wait_recv()

    def wind_copies():
        own = refs["V0"].at[:, pl.ds(rows - 1, 1), :]
        return (
            remote(own, refs["HYV0"].at[:, pl.ds(0, 1), :], "f0", 12, "gy", 1),
            remote(refs["W0"].at[levels], refs["W0"].at[0], "f0", 13, "gz", 1),
        )

    def pack(value, packed=None):
        for k in range(levels):
            edge = lanes_by(value(k), SLOT * k + EDGE)
            packed = edge if packed is None else jnp.where(lane // SLOT == k, edge, packed)
        return packed

    def pairs(low, high):
        return jnp.where(slot_lane == EDGE, lanes_by(low, 1), lanes_by(high, -1))

    def to_level(packed, k):
        return lanes_by(packed, -(SLOT * k + EDGE))

    def send_full(name, tag):
        sems, e = "f" + tag, FULL[tag]
        at = 0 if name == "P" else 6
        packed = pack(lambda k: refs[name + tag][k + 3])
        z = z_copies(name, tag, sems, at + 4)
        if tag == "0" and name == "P":
            for k in range(levels):
                wind = lanes_by(refs["U0"][k], SLOT * k + 7)
                packed = jnp.where((lane // SLOT == k) & (slot_lane == 6), wind, packed)
        refs["x" + name + "_s"][e] = packed
        if name == "P":
            start(y_copies(name, tag, sems, at + 2))
            if tag == "0":
                start(wind_copies()[:1])
                z_start((z[0], wind_copies()[1]), (z[1],))
            else:
                z_start((z[0],), (z[1],))
            start(x_copies("x" + name, e, sems, at))
        else:
            z_start((z[0],), (z[1],))
            start(x_copies("x" + name, e, sems, at))
            start(y_copies(name, tag, sems, at + 2))

    def receive_x(name, tag, fix=None):
        sems, e = "f" + tag, FULL[tag]
        wait(x_copies("x" + name, e, sems, 0 if name == "P" else 6))
        low, high = refs["x" + name + "_lo"][e], refs["x" + name + "_hi"][e]
        both = jnp.where(slot_lane < EDGE, low, high)
        if fix is not None:
            both = both + fix
        for k in range(levels):
            refs["HX" + name + tag][k] = to_level(both, k)
        if tag == "0" and name == "P":
            for k in range(levels):
                refs["HXU0"][k] = lanes_by(low, -(SLOT * k + 6))

    def receive_z(name, tag):
        z = z_copies(name, tag, "f" + tag, 4 if name == "P" else 10)
        if tag == "0" and name == "P":
            z_wait((z[0], wind_copies()[1]), (z[1],))
        else:
            z_wait((z[0],), (z[1],))

    def receive_y(name, tag):
        wait(y_copies(name, tag, "f" + tag, 2 if name == "P" else 8))
        if tag == "0" and name == "P":
            wait(wind_copies()[:1])

    def first_edges():
        for k in range(levels):
            x, y = refs["HXP0"][k], refs["HYP0"][k]
            refs["HXT0"][k] = jnp.where(lane == 0, lanes_by(x, 1), lanes_by(x, -1))
            refs["HYT0"][k] = jnp.where(row == 0, rows_by(y, 1), rows_by(y, -1))

    def send_thin(tag):
        sems, e = "t" + tag, THIN[tag]
        z = z_copies("P", tag, sems, 4)
        refs["tx_s"][e] = pack(lambda k: refs["P" + tag][k + 3])
        start(y_copies("P", tag, sems, 2))
        z_start((z[0],), (z[1],))
        start(x_copies("tx", e, sems, 0))

    def receive_thin(tag, fix=None):
        sems, e = "t" + tag, THIN[tag]
        z = z_copies("P", tag, sems, 4)
        wait(x_copies("tx", e, sems, 0))
        low, high = refs["tx_lo"][e], refs["tx_hi"][e]
        if fix is not None:
            low, high = low + fix, high + fix
        both = pairs(low, high)
        for k in range(levels):
            refs["HXT" + tag][k] = to_level(both, k)
        z_wait((z[0],), (z[1],))
        wait(y_copies("P", tag, sems, 2))

    def change(tag, k):
        return refs["P" + tag][k + 3] - refs["P0"][k + 3]

    top_rows, low_rows = pl.ds(rows - EDGE, EDGE), pl.ds(0, EDGE)
    top_levels, low_levels = pl.ds(EDGE, EDGE), pl.ds(0, EDGE)

    def delta_copies(tag):
        e, sems = DELTA[tag], "d" + tag
        s, dz = refs["d_s"].at[e], refs["dz_s"].at[e]
        flat = list(x_copies("d", e, sems, 0)) + list(y_copies("P", tag, sems, 2))
        for n, (end, sx) in enumerate((("lo", 1), ("hi", -1))):
            dst = refs["dxy_" + end].at[e]
            for m, (part, sy) in enumerate(((top_rows, 1), (low_rows, -1))):
                flat.append(remote(s.at[part, :], dst.at[part, :], sems, 6 + 2 * n + m,
                                   "gx", sx, "gy", sy))
        z = z_copies("P", tag, sems, 4)
        ups, downs = [z[0]], [z[1]]
        for t, (found, sz, part) in enumerate(((ups, 1, top_levels), (downs, -1, low_levels))):
            for n, (end, sx) in enumerate((("lo", 1), ("hi", -1))):
                found.append(remote(s, refs["dxz_" + end].at[e, t], sems, 10 + 2 * t + n,
                                    "gx", sx, "gz", sz))
            for n, (part_y, sy) in enumerate(((top_rows, 1), (low_rows, -1))):
                found.append(remote(dz.at[part, part_y, :], refs["dyz"].at[e, t, :, part_y, :],
                                    sems, 14 + 2 * t + n, "gy", sy, "gz", sz))
        return flat, ups, downs

    def send_delta(tag):
        e = DELTA[tag]
        for t in range(EDGE):
            refs["dz_s"][e, t] = change(tag, t)
            refs["dz_s"][e, EDGE + t] = change(tag, levels - EDGE + t)
        refs["d_s"][e] = pack(lambda k: change(tag, k))
        flat, ups, downs = delta_copies(tag)
        z_start(ups, downs)
        start(flat)

    def receive_delta(tag):
        flat, ups, downs = delta_copies(tag)
        wait(flat)
        z_wait(ups, downs)

    edge_lane = (lane == 0) | (lane == cols - 1)
    edge_row = (row == 0) | (row == rows - 1)

    def nearer(x):
        return jnp.where(row == 0, rows_by(x, 1), rows_by(x, -1))

    def packed_fix(tag):
        e = DELTA[tag]
        d = refs["d_s"][e]
        across = jnp.where(slot_lane < EDGE, refs["dxy_lo"][e], refs["dxy_hi"][e])
        below = jnp.where(slot_lane < EDGE, refs["dxz_lo"][e, 0], refs["dxz_hi"][e, 0])
        above = jnp.where(slot_lane < EDGE, refs["dxz_lo"][e, 1], refs["dxz_hi"][e, 1])
        last = SLOT * (levels - 1)
        fix = jnp.where(
            slot_lane == EDGE - 1, lanes_by(d, -1),
            jnp.where(slot_lane == EDGE, lanes_by(d, 1), 0.0),
        )
        fix = fix + jnp.where(edge_row, nearer(across), 0.0)
        fix = fix + jnp.where((lane < SLOT) & has_low, lanes_by(below, -last), 0.0)
        return fix + jnp.where((lane // SLOT == levels - 1) & has_high, lanes_by(above, last), 0.0)

    def mend(tag, p_tag, w_tag, push):
        e, gain = DELTA[tag], push * push
        P, U, V, W, HXU, HYV = (refs[n] for n in (
            "P" + p_tag, "U" + w_tag, "V" + w_tag, "W" + w_tag, "HXU" + w_tag, "HYV" + w_tag,
        ))
        full = p_tag in FULL
        face = pairs(refs["d_lo"][e], refs["d_hi"][e])
        corner = pairs(refs["dxy_lo"][e], refs["dxy_hi"][e])
        low = refs["P" + tag][2] - refs["P0"][2]
        high = refs["P" + tag][3 + levels] - refs["P0"][3 + levels]
        W[0] = W[0] + push * low
        W[levels] = W[levels] - push * high
        for k in range(levels):
            own = change(tag, k)
            dx = jnp.where(edge_lane, to_level(face, k), 0.0)
            dy = jnp.where(edge_row, refs["HYT" + tag][k] - refs["HYT0"][k], 0.0)
            total = dx + dy
            if k == 0:
                total = total + low
            if k == levels - 1:
                total = total + high
            P[k + 3] = P[k + 3] + gain * total
            U[k] = U[k] - push * jnp.where(lane == cols - 1, dx, 0.0)
            V[k] = V[k] - push * jnp.where(row == rows - 1, dy, 0.0)
            HXU[k] = HXU[k] + push * dx
            HYV[k] = HYV[k] + push * dy
            beside = jnp.where(edge_row, jnp.where(row == 0, rows_by(own, 1), rows_by(own, -1)), 0.0)
            beside = beside + jnp.where(edge_lane, to_level(corner, k), 0.0)
            if k == 0:
                beside = beside + jnp.where(has_low, refs["dyz"][e, 0, EDGE - 1], 0.0)
            if k == levels - 1:
                beside = beside + jnp.where(has_high, refs["dyz"][e, 1, 0], 0.0)
            if full:
                refs["HYP" + p_tag][k] = refs["HYP" + p_tag][k] + gain * beside
            else:
                refs["HYT" + p_tag][k] = refs["HYT" + p_tag][k] + gain * nearer(beside)

        def layers(t, wanted, nearest, source, level, at):
            sides_of = pairs(refs["dxz_lo"][e, t], refs["dxz_hi"][e, t])
            for n in wanted:
                part = jnp.where(edge_lane, to_level(sides_of, level + n), 0.0)
                part = part + jnp.where(edge_row, nearer(refs["dyz"][e, t, n]), 0.0)
                if n == nearest:
                    part = part + change(tag, source)
                P[at + n] = P[at + n] + gain * part

        @pl.when(has_low)
        def _():
            layers(0, range(EDGE) if full else (EDGE - 1,), EDGE - 1, 0, levels - EDGE, 0)

        @pl.when(has_high)
        def _():
            layers(1, range(EDGE) if full else (0,), 0, levels - 1, 0, 3 + levels)

    def sides(q, halo, by, index, extent):
        low = [by(jnp.where(index >= extent - n, halo, q), n) for n in (3, 2, 1)]
        high = [by(jnp.where(index < n, halo, q), -n) for n in (1, 2, 3)]
        return (*low, q, *high)

    def advect_xz(name, tag, rate):
        Q, HX = refs[name + tag], refs["HX" + name + tag]

        def level(k, below):
            u = refs["U" + tag][k]
            u_low = jnp.where(lane == 0, refs["HXU" + tag][k], lanes_by(u, 1))
            xs = sides(Q[k + 3], HX[k], lanes_by, lane, cols)
            above = flux(refs["W" + tag][k + 1], *(Q[k + n] for n in range(1, 7)))
            total = flux(u, *xs[1:]) - flux(u_low, *xs[:6])
            refs[rate][k] = total + (above - below)
            return above

        loop(levels, level, flux(refs["W" + tag][0], *(Q[n] for n in range(6))))

    def advect_y(name, tag, rate):
        Q, HY = refs[name + tag], refs["HY" + name + tag]

        def level(k, carry):
            v = refs["V" + tag][k]
            v_low = jnp.where(row == 0, refs["HYV" + tag][k], rows_by(v, 1))
            ys = sides(Q[k + 3], HY[k], rows_by, row, rows)
            total = refs[rate][k] + (flux(v, *ys[1:]) - flux(v_low, *ys[:6]))
            refs[rate][k] = total * (-1.0 / 60.0)
            return carry

        loop(levels, level, 0)

    def lift_of(tag):
        C = refs["C" + tag]
        lid_low = jnp.where(has_low, 1.0, 0.0)
        lid_high = jnp.where(has_high, 1.0, 0.0)
        for k in range(levels + 1):
            lift = (buoyancy * 0.5) * (C[k + 2] + C[k + 3])
            if k == 0:
                lift = lift * lid_low
            if k == levels:
                lift = lift * lid_high
            refs["lift"][k] = lift

    def substep(sp, hp, sw, dp, dw, sub_step):
        SP, HP, HXT, HYT = refs["P" + sp], refs["P" + hp], refs["HXT" + hp], refs["HYT" + hp]
        SU, SV, SW, HXU, HYV = (refs[n + sw] for n in ("U", "V", "W", "HXU", "HYV"))
        push = sub_step * sound_speed
        lid_low = jnp.where(has_low, 1.0, 0.0)
        lid_high = jnp.where(has_high, 1.0, 0.0)
        last = dp is None

        def vertical(k):
            above = (HP if k == levels else SP)[k + 3]
            below = (HP if k == 0 else SP)[k + 2]
            return SW[k] + sub_step * (refs["lift"][k] - sound_speed * (above - below))

        w_low = vertical(0) * lid_low
        if not last:
            refs["W" + dw][0] = w_low
        for k in range(levels):
            p, u, v = SP[k + 3], SU[k], SV[k]
            hx, hy = HXT[k], HYT[k]
            w = vertical(k + 1)
            if k == levels - 1:
                w = w * lid_high
            u_new = u - push * (jnp.where(lane == cols - 1, hx, lanes_by(p, -1)) - p)
            v_new = v - push * (jnp.where(row == rows - 1, hy, rows_by(p, -1)) - p)
            u_halo = HXU[k] - push * (p - hx)
            v_halo = HYV[k] - push * (p - hy)
            u_low = jnp.where(lane == 0, u_halo, lanes_by(u_new, 1))
            v_low = jnp.where(row == 0, v_halo, rows_by(v_new, 1))
            div = (u_new - u_low) + (v_new - v_low) + (w - w_low)
            p_new = p + sub_step * (refs["rate_p"][k] - sound_speed * div)
            w_low = w
            if last:
                for n, part in enumerate((p_new, u_new, v_new, w)):
                    out_fields[n + 1, k] = part
            else:
                refs["U" + dw][k] = u_new
                refs["V" + dw][k] = v_new
                refs["W" + dw][k + 1] = w
                refs["HXU" + dw][k] = u_halo
                refs["HYV" + dw][k] = v_halo
                refs["P" + dp][k + 3] = p_new

    def tracer(tag, scale):
        for k in range(levels):
            value = refs["C0"][k + 3] + scale * refs["rate_c"][k]
            if tag is None:
                out_fields[0, k] = value
                swell = jnp.exp(growth * value)
                refs["swell"][0, k] = swell
                refs["swell"][1, k] = swell * jnp.sqrt(swell)
            else:
                refs["C" + tag][k + 3] = value

    def droplet_terms():
        for copy in later_copies:
            copy.wait()

        def cell(k, carry):
            live = counts[k]
            for s in range(slots):
                r = jnp.abs(radius[s, k])
                number = jnp.where(live > s, weight[s, k], 0.0)
                area = number * (r * r)
                mass = area * r
                for m, term in enumerate((number, area, mass)):
                    high = term.astype(jnp.bfloat16).astype(jnp.float32)
                    vals[s, k, m * rows:(m + 1) * rows, :] = high
                    vals[s, k, (m + 3) * rows:(m + 4) * rows, :] = term - high
                vals[s, k, 6 * rows:, :] = jnp.zeros((2 * rows, cols), jnp.float32)
            return carry

        loop(levels, cell, 0, 2)

    def deposit(begin, cells):
        ids = lax.broadcasted_iota(jnp.int32, (cols, cols), 0).astype(jnp.float32).astype(jnp.bfloat16)
        one = jnp.ones((cols, cols), jnp.bfloat16)
        none = jnp.zeros((cols, cols), jnp.bfloat16)
        blank = jnp.zeros((8, cols), jnp.float32)

        def cell(n, carry):
            k, j = (begin + n) // rows, (begin + n) % rows
            by_depth = [None] * (FMAX + 1)
            for s in range(0, slots, 4):
                left, hots = [], []
                for t in range(4):
                    v = vals[s + t, k, pl.ds(j, 8, stride=rows), :]
                    left.append(jnp.concatenate([v, blank] if t % 2 == 0 else [blank, v], axis=1))
                    c = column[s + t, k, pl.ds(j, 1), :].astype(jnp.float32).astype(jnp.bfloat16)
                    hots.append(jnp.where(ids == jnp.broadcast_to(c, (cols, cols)), one, none))
                lhs = jnp.concatenate(left, axis=0).astype(jnp.bfloat16)
                rhs = jnp.concatenate(
                    [jnp.concatenate(hots[:2], axis=1), jnp.concatenate(hots[2:], axis=1)], axis=0
                )
                got = lax.dot_general(
                    lhs, rhs, (((1,), (1,)), ((), ())), preferred_element_type=jnp.float32
                )
                for t in range(4):
                    half = t // 2
                    part = got[8 * t:8 * (t + 1), half * cols:(half + 1) * cols]
                    fall = depth[s + t, j, 0, k]
                    for d in range(FMAX + 1):
                        term = jnp.where(fall == d, part, 0.0)
                        by_depth[d] = term if by_depth[d] is None else by_depth[d] + term
            at = pl.ds(pl.multiple_of(j * 8, 8), 8)
            for d in range(FMAX + 1):
                fallen[k, d, at, :] = by_depth[d]
            return carry

        lax.fori_loop(0, cells, cell, 0, unroll=min(CELLS, cells))

    def landed(m, l):
        total = None
        for d in range(FMAX + 1):
            k = l + d
            if not 0 <= k < levels:
                continue
            part = (
                fallen[k, d, pl.ds(m, rows, stride=8), :]
                + fallen[k, d, pl.ds(m + 3, rows, stride=8), :]
            )
            if m:
                part = part * refs["swell"][m - 1, k]
            total = part if total is None else total + part
        return total

    def fall_copy(m):
        return remote(refs["fall_s"].at[m], refs["fall_r"].at[m], "fall", m, "gz", -1)

    def fall_send(m):
        for l in range(FMAX):
            refs["fall_s"][m, l] = landed(m, l - FMAX)

        @pl.when(has_low)
        def _():
            fall_copy(m).start()

    def fall_home(m):
        for l in range(levels):
            moments[m, l] = landed(m, l)

    begins = [sum(CHUNKS[:n]) for n in range(len(CHUNKS))]
    cells = levels * rows

    def chunk(n):
        begin = min(begins[n], cells)
        end = cells if n == len(CHUNKS) - 1 else min(begins[n] + CHUNKS[n], cells)
        if end > begin:
            deposit(begin, end - begin)

    def advect(name, tag, rate):
        advect_xz(name, tag, rate)
        receive_y(name, tag)
        advect_y(name, tag, rate)

    def tracer_section(tag):
        receive_x("C", tag)
        advect("C", tag, "rate_c")

    copies = max_start(0, top)
    send_full("P", "0")
    send_full("C", "0")
    droplet_terms()
    chunk(0)
    for g in range(1, len(groups)):
        top = max_end(g - 1, top, copies)
        copies = max_start(g, top)
    receive_x("P", "0")
    receive_z("P", "0")
    advect("P", "0", "rate_p")
    first_edges()
    receive_z("C", "0")
    lift_of("0")
    top = max_end(len(groups) - 1, top, copies)
    time_step = courant_goal / (1.0 + jnp.max(top, axis=(0, 1), keepdims=True))
    time_step = jnp.broadcast_to(time_step, shape)

    third = time_step * (1.0 / 3.0)
    substep("0", "0", "0", "1", "1", third)
    send_full("P", "1")
    tracer_section("0")
    tracer("1", third)
    send_full("C", "1")
    chunk(1)

    receive_x("P", "1")
    receive_z("P", "1")
    advect("P", "1", "rate_p")
    receive_z("C", "1")
    lift_of("1")
    half = time_step * 0.5
    part = half / (NS // 2)
    substep("0", "0", "0", "a", "a", part)
    send_delta("a")
    substep("a", "0", "a", "2", "2", part)
    send_full("P", "2")
    tracer_section("1")
    tracer("2", half)
    send_full("C", "2")
    chunk(2)
    fall_send(0)

    receive_delta("a")
    push = part * sound_speed
    receive_x("P", "2", push * push * packed_fix("a"))
    receive_z("P", "2")
    receive_y("P", "2")
    mend("a", "2", "2", push)
    advect_xz("P", "2", "rate_p")
    advect_y("P", "2", "rate_p")
    receive_z("C", "2")
    lift_of("2")
    part = time_step / NS
    substep("0", "0", "0", "b", "b", part)
    send_delta("b")
    substep("b", "0", "b", "c", "c", part)
    send_thin("c")
    tracer_section("2")
    tracer(None, time_step)
    fall_send(1)
    fall_send(2)
    chunk(3)

    receive_delta("b")
    push = part * sound_speed
    receive_thin("c", push * push * packed_fix("b"))
    mend("b", "c", "c", push)
    substep("c", "c", "c", "d", "c", part)
    send_thin("d")
    chunk(4)
    for m in range(3):
        fall_home(m)
    receive_thin("d")
    substep("d", "d", "c", None, None, part)

    @pl.when(has_low)
    def _():
        for m in range(3):
            fall_copy(m).wait_send()

    @pl.when(has_high)
    def _():
        for m in range(3):
            fall_copy(m).wait_recv()
            for l in range(FMAX):
                at = levels - FMAX + l
                moments[m, at] = moments[m, at] + refs["fall_r"][m, l]


def write_out(fields, moments, out_fields, out_moments, sem):
    copies = [
        pltpu.make_async_copy(fields, out_fields, sem.at[0]),
        pltpu.make_async_copy(moments, out_moments, sem.at[1]),
    ]
    for copy in copies:
        copy.start()
    for copy in copies:
        copy.wait()


def per_device(fields, radius, weight, column, counts, fall_depth):
    levels, rows, cols = fields.shape[1:]
    slots = radius.shape[0]
    assert slots % 4 == 0 and levels * SLOT <= cols and rows == 8 and max(FMAX, 2 * EDGE) <= levels
    f32 = jnp.float32
    cell = (rows, cols)
    count = {a: lax.axis_size(a) for a in AXES}
    groups = max_groups(count)
    widest = max(len(shifts_of(g, count)) for g in groups)
    spaces = {}

    def add(name, *shape, dtype=f32):
        spaces[name] = pltpu.VMEM(shape, dtype)

    add("radius", *radius.shape)
    add("weight", *weight.shape)
    add("column", *column.shape, dtype=jnp.int32)
    add("counts", *counts.shape, dtype=jnp.int32)
    spaces["depth"] = pltpu.SMEM((slots, rows, 1, levels), jnp.int32)
    for tag in "012":
        add("C" + tag, levels + 6, *cell)
        for name in ("HXC", "HXP", "HYC", "HYP"):
            add(name + tag, levels, *cell)
    for tag in "012abcd":
        add("P" + tag, levels + 6, *cell)
    for tag in "0cd":
        add("HXT" + tag, levels, *cell)
    for tag in "0abcd":
        add("HYT" + tag, levels, *cell)
    for tag in "012abc":
        for name in ("U", "V", "HXU", "HYV"):
            add(name + tag, levels, *cell)
        add("W" + tag, levels + 1, *cell)
    add("rate_c", levels, *cell)
    add("rate_p", levels, *cell)
    add("lift", levels + 1, *cell)
    add("swell", 2, levels, *cell)
    add("max_send", len(groups), 1, cols)
    add("max_recv", len(groups), widest, 1, cols)
    for end in ("_s", "_lo", "_hi"):
        add("xP" + end, len(FULL), *cell)
        add("xC" + end, len(FULL), *cell)
        add("tx" + end, len(THIN), *cell)
        add("d" + end, len(DELTA), *cell)
    for end in ("_lo", "_hi"):
        add("dxy" + end, len(DELTA), *cell)
        add("dxz" + end, len(DELTA), 2, *cell)
    add("dz_s", len(DELTA), 2 * EDGE, *cell)
    add("dyz", len(DELTA), 2, EDGE, *cell)
    add("vals", slots, levels, 8 * rows, cols)
    add("fallen", levels, FMAX + 1, 8 * rows, cols)
    add("fall_s", 3, FMAX, *cell)
    add("fall_r", 3, FMAX, *cell)
    for end in ("_ss", "_rs"):
        for tag in FULL:
            spaces["f" + tag + end] = pltpu.SemaphoreType.DMA((14,))
        for tag in THIN:
            spaces["t" + tag + end] = pltpu.SemaphoreType.DMA((6,))
        for tag in DELTA:
            spaces["d" + tag + end] = pltpu.SemaphoreType.DMA((18,))
        spaces["fall" + end] = pltpu.SemaphoreType.DMA((3,))
        spaces["max" + end] = pltpu.SemaphoreType.DMA((len(groups), widest))
    spaces["local_sem"] = pltpu.SemaphoreType.DMA((10,))
    vmem = pl.BlockSpec(memory_space=pltpu.VMEM)
    anywhere = pl.BlockSpec(memory_space=pltpu.HBM)
    results = pl.pallas_call(
        functools.partial(kernel, (tuple(spaces), levels, rows, cols, slots)),
        out_shape=(
            jax.ShapeDtypeStruct(fields.shape, f32),
            jax.ShapeDtypeStruct((3, levels, rows, cols), f32),
        ),
        in_specs=[anywhere] * 6,
        out_specs=(vmem, vmem),
        scratch_shapes=list(spaces.values()),
        compiler_params=pltpu.CompilerParams(
            collective_id=0, has_side_effects=True,
            vmem_limit_bytes=KERNEL_BYTES,
        ),
        name="slab_step",
    )(*(
        pltpu.with_memory_space_constraint(x, pltpu.HBM)
        for x in (fall_depth.transpose(0, 2, 3, 1), fields, radius, weight, column, counts)
    ))
    return pl.pallas_call(
        write_out,
        out_shape=tuple(jax.ShapeDtypeStruct(r.shape, f32) for r in results),
        in_specs=[vmem] * 2,
        out_specs=(anywhere,) * 2,
        scratch_shapes=[pltpu.SemaphoreType.DMA((2,))],
        compiler_params=pltpu.CompilerParams(vmem_limit_bytes=1024 * 1024),
        name="write_out",
    )(*results)


def solution(mesh):
    in_specs = (
        P(None, "gz", "gy", "gx"),
        P(None, "gz", "gy", "gx"),
        P(None, "gz", "gy", "gx"),
        P(None, "gz", "gy", "gx"),
        P("gz", "gy", "gx"),
        P(None, "gz", "gy", "gx"),
    )
    out_specs = (P(None, "gz", "gy", "gx"), P(None, "gz", "gy", "gx"))
    return jax.shard_map(
        per_device, mesh=mesh, in_specs=in_specs, out_specs=out_specs, check_vma=False
    )
```

```python
import functools
import itertools
import jax
import jax.numpy as jnp
from jax import lax
from jax.experimental import pallas as pl
from jax.experimental.pallas import tpu as pltpu
from jax.sharding import PartitionSpec as P

NS = 4
FMAX = 8
CELLS = 4
SLOT = 8
EDGE = 3
CHUNKS = (32, 24, 28, 24, 20)
ONE_SHOT = 32
KERNEL_BYTES = 40 * 1024 * 1024

sound_speed = 10.0
buoyancy = 0.5
courant_goal = 0.6
growth = 0.3

MESH = pl.DeviceIdType.MESH
AXES = ("gy", "gx", "gz")
FULL = {"0": 0, "1": 1, "2": 2}
THIN = {"c": 0, "d": 1}
DELTA = {"a": 0, "b": 1}


def flux(wind, a, b, c, d, e, f):
    central = 37.0 * (c + d) - 8.0 * (b + e) + (a + f)
    upwind = 10.0 * (d - c) - 5.0 * (e - b) + (f - a)
    return wind * central - jnp.abs(wind) * upwind


def max_groups(count):
    total = 1
    for a in AXES:
        total *= count[a]
    return (AXES,) if total <= ONE_SHOT else tuple((a,) for a in AXES)


def shifts_of(group, count):
    return [s for s in itertools.product(*(range(count[a]) for a in group)) if any(s)]


def greeted(groups, count):
    found = {}
    diagonals = [
        (pair, steps)
        for pair in itertools.combinations(AXES, 2)
        for steps in itertools.product((1, -1), repeat=2)
    ]
    for group, shift in [(g, s) for g in groups for s in shifts_of(g, count)] + diagonals:
        step = {a: s % count[a] for a, s in zip(group, shift) if s % count[a]}
        if step:
            found[tuple(sorted(step.items()))] = step
    return list(found.values())


def kernel(
    sizes, depth_hbm, fields_hbm, radius_hbm, weight_hbm, column_hbm, counts_hbm,
    out_fields, moments, *scratch
):
    names, levels, rows, cols, slots = sizes
    refs = dict(zip(names, scratch))
    radius, weight, column, counts = (refs[n] for n in ("radius", "weight", "column", "counts"))
    depth = refs["depth"]
    vals, fallen = refs["vals"], refs["fallen"]
    local_sem = refs["local_sem"]
    shape = (rows, cols)
    lane = lax.broadcasted_iota(jnp.int32, shape, 1)
    row = lax.broadcasted_iota(jnp.int32, shape, 0)
    slot_lane = lane % SLOT
    place = {a: lax.axis_index(a) for a in AXES}
    count = {a: lax.axis_size(a) for a in AXES}
    groups = max_groups(count)
    has_low = place["gz"] > 0
    has_high = place["gz"] < count["gz"] - 1
    zero = jnp.zeros(shape, jnp.float32)

    def lanes_by(x, shift):
        return pltpu.roll(x, shift % cols, 1)

    def rows_by(x, shift):
        return pltpu.roll(x, shift % rows, 0)

    def loop(n, body, carry, unroll=True):
        return lax.fori_loop(0, n, body, carry, unroll=unroll)

    first_copies = []
    for n, dst in enumerate(
        (refs["C0"].at[pl.ds(3, levels)], refs["P0"].at[pl.ds(3, levels)],
         refs["U0"], refs["V0"], refs["W0"].at[pl.ds(1, levels)])
    ):
        first_copies.append(pltpu.make_async_copy(fields_hbm.at[n], dst, local_sem.at[n]))
    later_copies = []
    for n, (src, dst) in enumerate(
        ((counts_hbm, counts), (weight_hbm, weight), (radius_hbm, radius),
         (column_hbm, column), (depth_hbm, depth))
    ):
        later_copies.append(pltpu.make_async_copy(src, dst, local_sem.at[5 + n]))
    for copy in first_copies + later_copies:
        copy.start()

    def away(group, shift):
        return {a: lax.rem(place[a] + s, count[a]) for a, s in zip(group, shift) if s}

    barrier = pltpu.get_barrier_semaphore()
    peers = 0
    for step in greeted(groups, count):
        pl.semaphore_signal(
            barrier, inc=1, device_id=away(tuple(step), tuple(step.values())),
            device_id_type=MESH,
        )
        peers += 1

    for copy in first_copies:
        copy.wait()

    @pl.when(jnp.logical_not(has_high))
    def _():
        refs["W0"][levels] = zero
        for tag in ("0", "1", "2"):
            for t in range(EDGE):
                refs["C" + tag][3 + levels + t] = zero
        for tag in "012abcd":
            for t in range(EDGE if tag in FULL else 1):
                refs["P" + tag][3 + levels + t] = zero

    @pl.when(jnp.logical_not(has_low))
    def _():
        refs["W0"][0] = zero
        for tag in ("0", "1", "2"):
            for t in range(EDGE):
                refs["C" + tag][t] = zero
        for tag in "012abcd":
            for t in range(3 - (EDGE if tag in FULL else 1), 3):
                refs["P" + tag][t] = zero

    def fastest(k, top):
        speed = jnp.abs(refs["U0"][k]) + jnp.abs(refs["V0"][k]) + jnp.abs(refs["W0"][k + 1])
        return jnp.maximum(top, speed)

    top = loop(levels, fastest, zero)
    top = jnp.max(top, axis=0, keepdims=True)
    pl.semaphore_wait(barrier, peers)

    def max_start(g, value):
        refs["max_send"][g] = value
        copies = []
        for n, shift in enumerate(shifts_of(groups[g], count)):
            copy = pltpu.make_async_remote_copy(
                src_ref=refs["max_send"].at[g],
                dst_ref=refs["max_recv"].at[g, n],
                send_sem=refs["max_ss"].at[g, n],
                recv_sem=refs["max_rs"].at[g, n],
                device_id=away(groups[g], shift), device_id_type=MESH,
            )
            copy.start()
            copies.append(copy)
        return copies

    def max_end(g, value, copies):
        for copy in copies:
            copy.wait()
        for n in range(len(copies)):
            value = jnp.maximum(value, refs["max_recv"][g, n])
        return value

    def neighbour(*steps):
        return {
            a: lax.rem(place[a] + count[a] + step, count[a])
            for a, step in zip(steps[::2], steps[1::2])
        }

    def remote(src, dst, sems, n, *steps):
        return pltpu.make_async_remote_copy(
            src_ref=src, dst_ref=dst, send_sem=refs[sems + "_ss"].at[n],
            recv_sem=refs[sems + "_rs"].at[n],
            device_id=neighbour(*steps), device_id_type=MESH,
        )

    def y_copies(name, tag, sems, at):
        source = refs[name + tag]
        if tag in FULL:
            w, low, high, dst = EDGE, rows - EDGE, 0, refs["HY" + name + tag]
        else:
            w, low, high, dst = 1, 0, rows - 1, refs["HYT" + tag]
        own = pl.ds(3, levels)
        return (
            remote(source.at[own, pl.ds(rows - w, w), :], dst.at[:, pl.ds(low, w), :],
                   sems, at, "gy", 1),
            remote(source.at[own, pl.ds(0, w), :], dst.at[:, pl.ds(high, w), :],
                   sems, at + 1, "gy", -1),
        )

    def z_copies(name, tag, sems, at):
        w = EDGE if tag in FULL else 1
        q = refs[name + tag]
        return (
            remote(q.at[pl.ds(3 + levels - w, w)], q.at[pl.ds(3 - w, w)], sems, at, "gz", 1),
            remote(q.at[pl.ds(3, w)], q.at[pl.ds(3 + levels, w)], sems, at + 1, "gz", -1),
        )

    def x_copies(kind, e, sems, at):
        return (
            remote(refs[kind + "_s"].at[e], refs[kind + "_lo"].at[e], sems, at, "gx", 1),
            remote(refs[kind + "_s"].at[e], refs[kind + "_hi"].at[e], sems, at + 1, "gx", -1),
        )

    def start(copies):
        for copy in copies:
            copy.start()

    def wait(copies):
        for copy in copies:
            copy.wait()

    def z_start(up, down):
        @pl.when(has_high)
        def _():
            start(up)

        @pl.when(has_low)
        def _():
            start(down)

    def z_wait(up, down):
        @pl.when(has_high)
        def _():
            for copy in up:
                copy.wait_send()
            for copy in down:
                copy.wait_recv()

        @pl.when(has_low)
        def _():
            for copy in down:
                copy.wait_send()
            for copy in up:
                copy.wait_recv()

    def wind_copies():
        own = refs["V0"].at[:, pl.ds(rows - 1, 1), :]
        return (
            remote(own, refs["HYV0"].at[:, pl.ds(0, 1), :], "f0", 12, "gy", 1),
            remote(refs["W0"].at[levels], refs["W0"].at[0], "f0", 13, "gz", 1),
        )

    def pack(value, packed=None):
        for k in range(levels):
            edge = lanes_by(value(k), SLOT * k + EDGE)
            packed = edge if packed is None else jnp.where(lane // SLOT == k, edge, packed)
        return packed

    def pairs(low, high):
        return jnp.where(slot_lane == EDGE, lanes_by(low, 1), lanes_by(high, -1))

    def to_level(packed, k):
        return lanes_by(packed, -(SLOT * k + EDGE))

    def send_full(name, tag):
        sems, e = "f" + tag, FULL[tag]
        at = 0 if name == "P" else 6
        packed = pack(lambda k: refs[name + tag][k + 3])
        z = z_copies(name, tag, sems, at + 4)
        if tag == "0" and name == "P":
            for k in range(levels):
                wind = lanes_by(refs["U0"][k], SLOT * k + 7)
                packed = jnp.where((lane // SLOT == k) & (slot_lane == 6), wind, packed)
        refs["x" + name + "_s"][e] = packed
        if name == "P":
            start(y_copies(name, tag, sems, at + 2))
            if tag == "0":
                start(wind_copies()[:1])
                z_start((z[0], wind_copies()[1]), (z[1],))
            else:
                z_start((z[0],), (z[1],))
            start(x_copies("x" + name, e, sems, at))
        else:
            z_start((z[0],), (z[1],))
            start(x_copies("x" + name, e, sems, at))
            start(y_copies(name, tag, sems, at + 2))

    def receive_x(name, tag, fix=None):
        sems, e = "f" + tag, FULL[tag]
        wait(x_copies("x" + name, e, sems, 0 if name == "P" else 6))
        low, high = refs["x" + name + "_lo"][e], refs["x" + name + "_hi"][e]
        both = jnp.where(slot_lane < EDGE, low, high)
        if fix is not None:
            both = both + fix
        for k in range(levels):
            refs["HX" + name + tag][k] = to_level(both, k)
        if tag == "0" and name == "P":
            for k in range(levels):
                refs["HXU0"][k] = lanes_by(low, -(SLOT * k + 6))

    def receive_z(name, tag):
        z = z_copies(name, tag, "f" + tag, 4 if name == "P" else 10)
        if tag == "0" and name == "P":
            z_wait((z[0], wind_copies()[1]), (z[1],))
        else:
            z_wait((z[0],), (z[1],))

    def receive_y(name, tag):
        wait(y_copies(name, tag, "f" + tag, 2 if name == "P" else 8))
        if tag == "0" and name == "P":
            wait(wind_copies()[:1])

    def first_edges():
        for k in range(levels):
            x, y = refs["HXP0"][k], refs["HYP0"][k]
            refs["HXT0"][k] = jnp.where(lane == 0, lanes_by(x, 1), lanes_by(x, -1))
            refs["HYT0"][k] = jnp.where(row == 0, rows_by(y, 1), rows_by(y, -1))

    def send_thin(tag):
        sems, e = "t" + tag, THIN[tag]
        z = z_copies("P", tag, sems, 4)
        refs["tx_s"][e] = pack(lambda k: refs["P" + tag][k + 3])
        start(y_copies("P", tag, sems, 2))
        z_start((z[0],), (z[1],))
        start(x_copies("tx", e, sems, 0))

    def receive_thin(tag, fix=None):
        sems, e = "t" + tag, THIN[tag]
        z = z_copies("P", tag, sems, 4)
        wait(x_copies("tx", e, sems, 0))
        low, high = refs["tx_lo"][e], refs["tx_hi"][e]
        if fix is not None:
            low, high = low + fix, high + fix
        both = pairs(low, high)
        for k in range(levels):
            refs["HXT" + tag][k] = to_level(both, k)
        z_wait((z[0],), (z[1],))
        wait(y_copies("P", tag, sems, 2))

    def change(tag, k):
        return refs["P" + tag][k + 3] - refs["P0"][k + 3]

    top_rows, low_rows = pl.ds(rows - EDGE, EDGE), pl.ds(0, EDGE)
    top_levels, low_levels = pl.ds(EDGE, EDGE), pl.ds(0, EDGE)

    def delta_copies(tag):
        e, sems = DELTA[tag], "d" + tag
        s, dz = refs["d_s"].at[e], refs["dz_s"].at[e]
        flat = list(x_copies("d", e, sems, 0)) + list(y_copies("P", tag, sems, 2))
        for n, (end, sx) in enumerate((("lo", 1), ("hi", -1))):
            dst = refs["dxy_" + end].at[e]
            for m, (part, sy) in enumerate(((top_rows, 1), (low_rows, -1))):
                flat.append(remote(s.at[part, :], dst.at[part, :], sems, 6 + 2 * n + m,
                                   "gx", sx, "gy", sy))
        z = z_copies("P", tag, sems, 4)
        ups, downs = [z[0]], [z[1]]
        for t, (found, sz, part) in enumerate(((ups, 1, top_levels), (downs, -1, low_levels))):
            for n, (end, sx) in enumerate((("lo", 1), ("hi", -1))):
                found.append(remote(s, refs["dxz_" + end].at[e, t], sems, 10 + 2 * t + n,
                                    "gx", sx, "gz", sz))
            for n, (part_y, sy) in enumerate(((top_rows, 1), (low_rows, -1))):
                found.append(remote(dz.at[part, part_y, :], refs["dyz"].at[e, t, :, part_y, :],
                                    sems, 14 + 2 * t + n, "gy", sy, "gz", sz))
        return flat, ups, downs

    def send_delta(tag):
        e = DELTA[tag]
        for t in range(EDGE):
            refs["dz_s"][e, t] = change(tag, t)
            refs["dz_s"][e, EDGE + t] = change(tag, levels - EDGE + t)
        refs["d_s"][e] = pack(lambda k: change(tag, k))
        flat, ups, downs = delta_copies(tag)
        z_start(ups, downs)
        start(flat)

    def receive_delta(tag):
        flat, ups, downs = delta_copies(tag)
        wait(flat)
        z_wait(ups, downs)

    edge_lane = (lane == 0) | (lane == cols - 1)
    edge_row = (row == 0) | (row == rows - 1)

    def nearer(x):
        return jnp.where(row == 0, rows_by(x, 1), rows_by(x, -1))

    def packed_fix(tag):
        e = DELTA[tag]
        d = refs["d_s"][e]
        across = jnp.where(slot_lane < EDGE, refs["dxy_lo"][e], refs["dxy_hi"][e])
        below = jnp.where(slot_lane < EDGE, refs["dxz_lo"][e, 0], refs["dxz_hi"][e, 0])
        above = jnp.where(slot_lane < EDGE, refs["dxz_lo"][e, 1], refs["dxz_hi"][e, 1])
        last = SLOT * (levels - 1)
        fix = jnp.where(
            slot_lane == EDGE - 1, lanes_by(d, -1),
            jnp.where(slot_lane == EDGE, lanes_by(d, 1), 0.0),
        )
        fix = fix + jnp.where(edge_row, nearer(across), 0.0)
        fix = fix + jnp.where((lane < SLOT) & has_low, lanes_by(below, -last), 0.0)
        return fix + jnp.where((lane // SLOT == levels - 1) & has_high, lanes_by(above, last), 0.0)

    def mend(tag, p_tag, w_tag, push):
        e, gain = DELTA[tag], push * push
        P, U, V, W, HXU, HYV = (refs[n] for n in (
            "P" + p_tag, "U" + w_tag, "V" + w_tag, "W" + w_tag, "HXU" + w_tag, "HYV" + w_tag,
        ))
        full = p_tag in FULL
        face = pairs(refs["d_lo"][e], refs["d_hi"][e])
        corner = pairs(refs["dxy_lo"][e], refs["dxy_hi"][e])
        low = refs["P" + tag][2] - refs["P0"][2]
        high = refs["P" + tag][3 + levels] - refs["P0"][3 + levels]
        W[0] = W[0] + push * low
        W[levels] = W[levels] - push * high
        for k in range(levels):
            own = change(tag, k)
            dx = jnp.where(edge_lane, to_level(face, k), 0.0)
            dy = jnp.where(edge_row, refs["HYT" + tag][k] - refs["HYT0"][k], 0.0)
            total = dx + dy
            if k == 0:
                total = total + low
            if k == levels - 1:
                total = total + high
            P[k + 3] = P[k + 3] + gain * total
            U[k] = U[k] - push * jnp.where(lane == cols - 1, dx, 0.0)
            V[k] = V[k] - push * jnp.where(row == rows - 1, dy, 0.0)
            HXU[k] = HXU[k] + push * dx
            HYV[k] = HYV[k] + push * dy
            beside = jnp.where(edge_row, jnp.where(row == 0, rows_by(own, 1), rows_by(own, -1)), 0.0)
            beside = beside + jnp.where(edge_lane, to_level(corner, k), 0.0)
            if k == 0:
                beside = beside + jnp.where(has_low, refs["dyz"][e, 0, EDGE - 1], 0.0)
            if k == levels - 1:
                beside = beside + jnp.where(has_high, refs["dyz"][e, 1, 0], 0.0)
            if full:
                refs["HYP" + p_tag][k] = refs["HYP" + p_tag][k] + gain * beside
            else:
                refs["HYT" + p_tag][k] = refs["HYT" + p_tag][k] + gain * nearer(beside)

        def layers(t, wanted, nearest, source, level, at):
            sides_of = pairs(refs["dxz_lo"][e, t], refs["dxz_hi"][e, t])
            for n in wanted:
                part = jnp.where(edge_lane, to_level(sides_of, level + n), 0.0)
                part = part + jnp.where(edge_row, nearer(refs["dyz"][e, t, n]), 0.0)
                if n == nearest:
                    part = part + change(tag, source)
                P[at + n] = P[at + n] + gain * part

        @pl.when(has_low)
        def _():
            layers(0, range(EDGE) if full else (EDGE - 1,), EDGE - 1, 0, levels - EDGE, 0)

        @pl.when(has_high)
        def _():
            layers(1, range(EDGE) if full else (0,), 0, levels - 1, 0, 3 + levels)

    def sides(q, halo, by, index, extent):
        low = [by(jnp.where(index >= extent - n, halo, q), n) for n in (3, 2, 1)]
        high = [by(jnp.where(index < n, halo, q), -n) for n in (1, 2, 3)]
        return (*low, q, *high)

    def advect_xz(name, tag, rate):
        Q, HX = refs[name + tag], refs["HX" + name + tag]

        def level(k, below):
            u = refs["U" + tag][k]
            u_low = jnp.where(lane == 0, refs["HXU" + tag][k], lanes_by(u, 1))
            xs = sides(Q[k + 3], HX[k], lanes_by, lane, cols)
            above = flux(refs["W" + tag][k + 1], *(Q[k + n] for n in range(1, 7)))
            total = flux(u, *xs[1:]) - flux(u_low, *xs[:6])
            refs[rate][k] = total + (above - below)
            return above

        loop(levels, level, flux(refs["W" + tag][0], *(Q[n] for n in range(6))))

    def advect_y(name, tag, rate):
        Q, HY = refs[name + tag], refs["HY" + name + tag]

        def level(k, carry):
            v = refs["V" + tag][k]
            v_low = jnp.where(row == 0, refs["HYV" + tag][k], rows_by(v, 1))
            ys = sides(Q[k + 3], HY[k], rows_by, row, rows)
            total = refs[rate][k] + (flux(v, *ys[1:]) - flux(v_low, *ys[:6]))
            refs[rate][k] = total * (-1.0 / 60.0)
            return carry

        loop(levels, level, 0)

    def lift_of(tag):
        C = refs["C" + tag]
        lid_low = jnp.where(has_low, 1.0, 0.0)
        lid_high = jnp.where(has_high, 1.0, 0.0)
        for k in range(levels + 1):
            lift = (buoyancy * 0.5) * (C[k + 2] + C[k + 3])
            if k == 0:
                lift = lift * lid_low
            if k == levels:
                lift = lift * lid_high
            refs["lift"][k] = lift

    def substep(sp, hp, sw, dp, dw, sub_step):
        SP, HP, HXT, HYT = refs["P" + sp], refs["P" + hp], refs["HXT" + hp], refs["HYT" + hp]
        SU, SV, SW, HXU, HYV = (refs[n + sw] for n in ("U", "V", "W", "HXU", "HYV"))
        push = sub_step * sound_speed
        lid_low = jnp.where(has_low, 1.0, 0.0)
        lid_high = jnp.where(has_high, 1.0, 0.0)
        last = dp is None

        def vertical(k):
            above = (HP if k == levels else SP)[k + 3]
            below = (HP if k == 0 else SP)[k + 2]
            return SW[k] + sub_step * (refs["lift"][k] - sound_speed * (above - below))

        w_low = vertical(0) * lid_low
        if not last:
            refs["W" + dw][0] = w_low
        for k in range(levels):
            p, u, v = SP[k + 3], SU[k], SV[k]
            hx, hy = HXT[k], HYT[k]
            w = vertical(k + 1)
            if k == levels - 1:
                w = w * lid_high
            u_new = u - push * (jnp.where(lane == cols - 1, hx, lanes_by(p, -1)) - p)
            v_new = v - push * (jnp.where(row == rows - 1, hy, rows_by(p, -1)) - p)
            u_halo = HXU[k] - push * (p - hx)
            v_halo = HYV[k] - push * (p - hy)
            u_low = jnp.where(lane == 0, u_halo, lanes_by(u_new, 1))
            v_low = jnp.where(row == 0, v_halo, rows_by(v_new, 1))
            div = (u_new - u_low) + (v_new - v_low) + (w - w_low)
            p_new = p + sub_step * (refs["rate_p"][k] - sound_speed * div)
            w_low = w
            if last:
                for n, part in enumerate((p_new, u_new, v_new, w)):
                    out_fields[n + 1, k] = part
            else:
                refs["U" + dw][k] = u_new
                refs["V" + dw][k] = v_new
                refs["W" + dw][k + 1] = w
                refs["HXU" + dw][k] = u_halo
                refs["HYV" + dw][k] = v_halo
                refs["P" + dp][k + 3] = p_new

    def tracer(tag, scale):
        for k in range(levels):
            value = refs["C0"][k + 3] + scale * refs["rate_c"][k]
            if tag is None:
                out_fields[0, k] = value
                swell = jnp.exp(growth * value)
                refs["swell"][0, k] = swell
                refs["swell"][1, k] = swell * jnp.sqrt(swell)
            else:
                refs["C" + tag][k + 3] = value

    def droplet_terms():
        for copy in later_copies:
            copy.wait()

        def cell(k, carry):
            live = counts[k]
            for s in range(slots):
                r = jnp.abs(radius[s, k])
                number = jnp.where(live > s, weight[s, k], 0.0)
                area = number * (r * r)
                mass = area * r
                for m, term in enumerate((number, area, mass)):
                    high = term.astype(jnp.bfloat16).astype(jnp.float32)
                    vals[s, k, m * rows:(m + 1) * rows, :] = high
                    vals[s, k, (m + 3) * rows:(m + 4) * rows, :] = term - high
                vals[s, k, 6 * rows:, :] = jnp.zeros((2 * rows, cols), jnp.float32)
            return carry

        loop(levels, cell, 0, 2)

    def deposit(begin, cells):
        narrow, thin_type = jnp.bfloat16, jnp.float8_e4m3fn
        ids = lax.broadcasted_iota(jnp.int32, (cols, cols), 0).astype(jnp.float32).astype(narrow)
        one = jnp.ones((cols, cols), narrow)
        none = jnp.zeros((cols, cols), narrow)
        tile = (2 * rows, cols)
        blank = jnp.zeros(tile, narrow)
        half = (lax.broadcasted_iota(jnp.int32, tile, 0) // rows).astype(jnp.float32)
        stairs = [(half + 2.0 * q).astype(narrow) for q in range(FMAX // 2 + 1)]

        def cell(n, carry):
            k, j = (begin + n) // rows, (begin + n) % rows
            total = None
            for s in range(0, slots, 2):
                left, hots = [], []
                for t in (s, s + 1):
                    v = vals[t, k, pl.ds(j, 8, stride=rows), :]
                    base = jnp.concatenate([v, v], axis=0).astype(narrow)
                    fall = jnp.full(tile, depth[t, j, 0, k], jnp.int32)
                    fall = fall.astype(jnp.float32).astype(narrow)
                    left.append(jnp.concatenate(
                        [jnp.where(stair == fall, base, blank) for stair in stairs], axis=0
                    ))
                    c = column[t, k, pl.ds(j, 1), :].astype(jnp.float32).astype(narrow)
                    hot = jnp.where(ids == jnp.broadcast_to(c, (cols, cols)), one, none)
                    hots.append(hot.astype(thin_type))
                got = lax.dot_general(
                    jnp.concatenate(left, axis=1), jnp.concatenate(hots, axis=1),
                    (((1,), (1,)), ((), ())), preferred_element_type=jnp.float32,
                )
                total = got if total is None else total + got
            at = pl.ds(pl.multiple_of(j * 8, 8), 8)
            for d in range(FMAX + 1):
                fallen[k, d, at, :] = total[8 * d:8 * (d + 1)]
            return carry

        lax.fori_loop(0, cells, cell, 0, unroll=min(CELLS, cells))

    def landed(m, l):
        total = None
        for d in range(FMAX + 1):
            k = l + d
            if not 0 <= k < levels:
                continue
            part = (
                fallen[k, d, pl.ds(m, rows, stride=8), :]
                + fallen[k, d, pl.ds(m + 3, rows, stride=8), :]
            )
            if m:
                part = part * refs["swell"][m - 1, k]
            total = part if total is None else total + part
        return total

    def fall_copy(m):
        return remote(refs["fall_s"].at[m], refs["fall_r"].at[m], "fall", m, "gz", -1)

    def fall_send(m):
        for l in range(FMAX):
            refs["fall_s"][m, l] = landed(m, l - FMAX)

        @pl.when(has_low)
        def _():
            fall_copy(m).start()

    def fall_home(m):
        for l in range(levels):
            moments[m, l] = landed(m, l)

    begins = [sum(CHUNKS[:n]) for n in range(len(CHUNKS))]
    cells = levels * rows

    def chunk(n):
        begin = min(begins[n], cells)
        end = cells if n == len(CHUNKS) - 1 else min(begins[n] + CHUNKS[n], cells)
        if end > begin:
            deposit(begin, end - begin)

    def advect(name, tag, rate):
        advect_xz(name, tag, rate)
        receive_y(name, tag)
        advect_y(name, tag, rate)

    def tracer_section(tag):
        receive_x("C", tag)
        advect("C", tag, "rate_c")

    copies = max_start(0, top)
    send_full("P", "0")
    send_full("C", "0")
    droplet_terms()
    chunk(0)
    for g in range(1, len(groups)):
        top = max_end(g - 1, top, copies)
        copies = max_start(g, top)
    receive_x("P", "0")
    receive_z("P", "0")
    advect("P", "0", "rate_p")
    first_edges()
    receive_z("C", "0")
    lift_of("0")
    top = max_end(len(groups) - 1, top, copies)
    time_step = courant_goal / (1.0 + jnp.max(top, axis=(0, 1), keepdims=True))
    time_step = jnp.broadcast_to(time_step, shape)

    third = time_step * (1.0 / 3.0)
    substep("0", "0", "0", "1", "1", third)
    send_full("P", "1")
    tracer_section("0")
    tracer("1", third)
    send_full("C", "1")
    chunk(1)

    receive_x("P", "1")
    receive_z("P", "1")
    advect("P", "1", "rate_p")
    receive_z("C", "1")
    lift_of("1")
    half = time_step * 0.5
    part = half / (NS // 2)
    substep("0", "0", "0", "a", "a", part)
    send_delta("a")
    substep("a", "0", "a", "2", "2", part)
    send_full("P", "2")
    tracer_section("1")
    tracer("2", half)
    send_full("C", "2")
    chunk(2)
    fall_send(0)

    receive_delta("a")
    push = part * sound_speed
    receive_x("P", "2", push * push * packed_fix("a"))
    receive_z("P", "2")
    receive_y("P", "2")
    mend("a", "2", "2", push)
    advect_xz("P", "2", "rate_p")
    advect_y("P", "2", "rate_p")
    receive_z("C", "2")
    lift_of("2")
    part = time_step / NS
    substep("0", "0", "0", "b", "b", part)
    send_delta("b")
    substep("b", "0", "b", "c", "c", part)
    send_thin("c")
    tracer_section("2")
    tracer(None, time_step)
    fall_send(1)
    fall_send(2)
    chunk(3)

    receive_delta("b")
    push = part * sound_speed
    receive_thin("c", push * push * packed_fix("b"))
    mend("b", "c", "c", push)
    substep("c", "c", "c", "d", "c", part)
    send_thin("d")
    chunk(4)
    for m in range(3):
        fall_home(m)
    receive_thin("d")
    substep("d", "d", "c", None, None, part)

    @pl.when(has_low)
    def _():
        for m in range(3):
            fall_copy(m).wait_send()

    @pl.when(has_high)
    def _():
        for m in range(3):
            fall_copy(m).wait_recv()
            for l in range(FMAX):
                at = levels - FMAX + l
                moments[m, at] = moments[m, at] + refs["fall_r"][m, l]


def write_out(fields, moments, out_fields, out_moments, sem):
    copies = [
        pltpu.make_async_copy(fields, out_fields, sem.at[0]),
        pltpu.make_async_copy(moments, out_moments, sem.at[1]),
    ]
    for copy in copies:
        copy.start()
    for copy in copies:
        copy.wait()


def per_device(fields, radius, weight, column, counts, fall_depth):
    levels, rows, cols = fields.shape[1:]
    slots = radius.shape[0]
    assert slots % 4 == 0 and levels * SLOT <= cols and rows == 8 and max(FMAX, 2 * EDGE) <= levels
    f32 = jnp.float32
    cell = (rows, cols)
    count = {a: lax.axis_size(a) for a in AXES}
    groups = max_groups(count)
    widest = max(len(shifts_of(g, count)) for g in groups)
    spaces = {}

    def add(name, *shape, dtype=f32):
        spaces[name] = pltpu.VMEM(shape, dtype)

    add("radius", *radius.shape)
    add("weight", *weight.shape)
    add("column", *column.shape, dtype=jnp.int32)
    add("counts", *counts.shape, dtype=jnp.int32)
    spaces["depth"] = pltpu.SMEM((slots, rows, 1, levels), jnp.int32)
    for tag in "012":
        add("C" + tag, levels + 6, *cell)
        for name in ("HXC", "HXP", "HYC", "HYP"):
            add(name + tag, levels, *cell)
    for tag in "012abcd":
        add("P" + tag, levels + 6, *cell)
    for tag in "0cd":
        add("HXT" + tag, levels, *cell)
    for tag in "0abcd":
        add("HYT" + tag, levels, *cell)
    for tag in "012abc":
        for name in ("U", "V", "HXU", "HYV"):
            add(name + tag, levels, *cell)
        add("W" + tag, levels + 1, *cell)
    add("rate_c", levels, *cell)
    add("rate_p", levels, *cell)
    add("lift", levels + 1, *cell)
    add("swell", 2, levels, *cell)
    add("max_send", len(groups), 1, cols)
    add("max_recv", len(groups), widest, 1, cols)
    for end in ("_s", "_lo", "_hi"):
        add("xP" + end, len(FULL), *cell)
        add("xC" + end, len(FULL), *cell)
        add("tx" + end, len(THIN), *cell)
        add("d" + end, len(DELTA), *cell)
    for end in ("_lo", "_hi"):
        add("dxy" + end, len(DELTA), *cell)
        add("dxz" + end, len(DELTA), 2, *cell)
    add("dz_s", len(DELTA), 2 * EDGE, *cell)
    add("dyz", len(DELTA), 2, EDGE, *cell)
    add("vals", slots, levels, 8 * rows, cols)
    add("fallen", levels, FMAX + 1, 8 * rows, cols)
    add("fall_s", 3, FMAX, *cell)
    add("fall_r", 3, FMAX, *cell)
    for end in ("_ss", "_rs"):
        for tag in FULL:
            spaces["f" + tag + end] = pltpu.SemaphoreType.DMA((14,))
        for tag in THIN:
            spaces["t" + tag + end] = pltpu.SemaphoreType.DMA((6,))
        for tag in DELTA:
            spaces["d" + tag + end] = pltpu.SemaphoreType.DMA((18,))
        spaces["fall" + end] = pltpu.SemaphoreType.DMA((3,))
        spaces["max" + end] = pltpu.SemaphoreType.DMA((len(groups), widest))
    spaces["local_sem"] = pltpu.SemaphoreType.DMA((10,))
    vmem = pl.BlockSpec(memory_space=pltpu.VMEM)
    anywhere = pl.BlockSpec(memory_space=pltpu.HBM)
    results = pl.pallas_call(
        functools.partial(kernel, (tuple(spaces), levels, rows, cols, slots)),
        out_shape=(
            jax.ShapeDtypeStruct(fields.shape, f32),
            jax.ShapeDtypeStruct((3, levels, rows, cols), f32),
        ),
        in_specs=[anywhere] * 6,
        out_specs=(vmem, vmem),
        scratch_shapes=list(spaces.values()),
        compiler_params=pltpu.CompilerParams(
            collective_id=0, has_side_effects=True,
            vmem_limit_bytes=KERNEL_BYTES,
        ),
        name="slab_step",
    )(*(
        pltpu.with_memory_space_constraint(x, pltpu.HBM)
        for x in (fall_depth.transpose(0, 2, 3, 1), fields, radius, weight, column, counts)
    ))
    return pl.pallas_call(
        write_out,
        out_shape=tuple(jax.ShapeDtypeStruct(r.shape, f32) for r in results),
        in_specs=[vmem] * 2,
        out_specs=(anywhere,) * 2,
        scratch_shapes=[pltpu.SemaphoreType.DMA((2,))],
        compiler_params=pltpu.CompilerParams(vmem_limit_bytes=1024 * 1024),
        name="write_out",
    )(*results)


def solution(mesh):
    in_specs = (
        P(None, "gz", "gy", "gx"),
        P(None, "gz", "gy", "gx"),
        P(None, "gz", "gy", "gx"),
        P(None, "gz", "gy", "gx"),
        P("gz", "gy", "gx"),
        P(None, "gz", "gy", "gx"),
    )
    out_specs = (P(None, "gz", "gy", "gx"), P(None, "gz", "gy", "gx"))
    return jax.shard_map(
        per_device, mesh=mesh, in_specs=in_specs, out_specs=out_specs, check_vma=False
    )
```

```python
import functools
import itertools
import jax
import jax.numpy as jnp
from jax import lax
from jax.experimental import pallas as pl
from jax.experimental.pallas import tpu as pltpu
from jax.sharding import PartitionSpec as P

NS = 4
FMAX = 8
CELLS = 8
SLOT = 8
EDGE = 3
CHUNKS = (40, 24, 24, 24, 16)
ONE_SHOT = 32
KERNEL_BYTES = 40 * 1024 * 1024

sound_speed = 10.0
buoyancy = 0.5
courant_goal = 0.6
growth = 0.3

MESH = pl.DeviceIdType.MESH
AXES = ("gy", "gx", "gz")
FULL = {"0": 0, "1": 1, "2": 2}
THIN = {"c": 0, "d": 1}
DELTA = {"a": 0, "b": 1}


def flux(wind, a, b, c, d, e, f):
    central = 37.0 * (c + d) - 8.0 * (b + e) + (a + f)
    upwind = 10.0 * (d - c) - 5.0 * (e - b) + (f - a)
    return wind * central - jnp.abs(wind) * upwind


def max_groups(count):
    total = 1
    for a in AXES:
        total *= count[a]
    return (("gz", "gy", "gx"),) if total <= ONE_SHOT else tuple((a,) for a in AXES)


def shifts_of(group, count):
    return [s for s in itertools.product(*(range(count[a]) for a in group)) if any(s)]


def greeted(groups, count):
    found = {}
    diagonals = [
        (pair, steps)
        for pair in itertools.combinations(AXES, 2)
        for steps in itertools.product((1, -1), repeat=2)
    ]
    for group, shift in [(g, s) for g in groups for s in shifts_of(g, count)] + diagonals:
        step = {a: s % count[a] for a, s in zip(group, shift) if s % count[a]}
        if step:
            found[tuple(sorted(step.items()))] = step
    return list(found.values())


def kernel(
    sizes, depth_hbm, fields_hbm, radius_hbm, weight_hbm, column_hbm, counts_hbm,
    out_fields, moments, *scratch
):
    names, levels, rows, cols, slots = sizes
    refs = dict(zip(names, scratch))
    radius, weight, column, counts = (refs[n] for n in ("radius", "weight", "column", "counts"))
    depth = refs["depth"]
    vals, fallen = refs["vals"], refs["fallen"]
    local_sem = refs["local_sem"]
    shape = (rows, cols)
    lane = lax.broadcasted_iota(jnp.int32, shape, 1)
    row = lax.broadcasted_iota(jnp.int32, shape, 0)
    slot_lane = lane % SLOT
    place = {a: lax.axis_index(a) for a in AXES}
    count = {a: lax.axis_size(a) for a in AXES}
    groups = max_groups(count)
    has_low = place["gz"] > 0
    has_high = place["gz"] < count["gz"] - 1
    zero = jnp.zeros(shape, jnp.float32)

    def lanes_by(x, shift):
        return pltpu.roll(x, shift % cols, 1)

    def rows_by(x, shift):
        return pltpu.roll(x, shift % rows, 0)

    def loop(n, body, carry, unroll=True):
        return lax.fori_loop(0, n, body, carry, unroll=unroll)

    first_copies = []
    for n, dst in enumerate(
        (refs["C0"].at[pl.ds(3, levels)], refs["P0"].at[pl.ds(3, levels)],
         refs["U0"], refs["V0"], refs["W0"].at[pl.ds(1, levels)])
    ):
        first_copies.append(pltpu.make_async_copy(fields_hbm.at[n], dst, local_sem.at[n]))
    later_copies = []
    for n, (src, dst) in enumerate(
        ((counts_hbm, counts), (weight_hbm, weight), (radius_hbm, radius),
         (column_hbm, column), (depth_hbm, depth))
    ):
        later_copies.append(pltpu.make_async_copy(src, dst, local_sem.at[5 + n]))
    for copy in first_copies:
        copy.start()

    def away(group, shift):
        return {a: lax.rem(place[a] + s, count[a]) for a, s in zip(group, shift) if s}

    barrier = pltpu.get_barrier_semaphore()
    peers = 0
    for step in sorted(greeted(groups, count), key=lambda step: step.get("gz", count["gz"])):
        pl.semaphore_signal(
            barrier, inc=1, device_id=away(tuple(step), tuple(step.values())),
            device_id_type=MESH,
        )
        peers += 1

    for copy in later_copies:
        copy.start()
    for copy in first_copies:
        copy.wait()

    @pl.when(jnp.logical_not(has_high))
    def _():
        refs["W0"][levels] = zero
        for tag in ("0", "1", "2"):
            for t in range(EDGE):
                refs["C" + tag][3 + levels + t] = zero
        for tag in "012abcd":
            for t in range(EDGE if tag in FULL else 1):
                refs["P" + tag][3 + levels + t] = zero

    @pl.when(jnp.logical_not(has_low))
    def _():
        refs["W0"][0] = zero
        for tag in ("0", "1", "2"):
            for t in range(EDGE):
                refs["C" + tag][t] = zero
        for tag in "012abcd":
            for t in range(3 - (EDGE if tag in FULL else 1), 3):
                refs["P" + tag][t] = zero

    def fastest(k, top):
        speed = jnp.abs(refs["U0"][k]) + jnp.abs(refs["V0"][k]) + jnp.abs(refs["W0"][k + 1])
        return jnp.maximum(top, speed)

    top = loop(levels, fastest, zero)
    top = jnp.max(top, axis=0, keepdims=True)
    pl.semaphore_wait(barrier, peers)

    def max_start(g, value):
        refs["max_send"][g] = value
        copies = []
        for n, shift in reversed(list(enumerate(shifts_of(groups[g], count)))):
            copy = pltpu.make_async_remote_copy(
                src_ref=refs["max_send"].at[g],
                dst_ref=refs["max_recv"].at[g, n],
                send_sem=refs["max_ss"].at[g, n],
                recv_sem=refs["max_rs"].at[g, n],
                device_id=away(groups[g], shift), device_id_type=MESH,
            )
            copy.start()
            copies.append(copy)
        return copies

    def max_end(g, value, copies):
        wait(copies)
        for n in range(len(copies)):
            value = jnp.maximum(value, refs["max_recv"][g, n])
        return value

    def neighbour(*steps):
        return {
            a: lax.rem(place[a] + count[a] + step, count[a])
            for a, step in zip(steps[::2], steps[1::2])
        }

    def remote(src, dst, sems, n, *steps):
        return pltpu.make_async_remote_copy(
            src_ref=src, dst_ref=dst, send_sem=refs[sems + "_ss"].at[n],
            recv_sem=refs[sems + "_rs"].at[n],
            device_id=neighbour(*steps), device_id_type=MESH,
        )

    def y_copies(name, tag, sems, at):
        source = refs[name + tag]
        if tag in FULL:
            w, low, high, dst = EDGE, rows - EDGE, 0, refs["HY" + name + tag]
        else:
            w, low, high, dst = 1, 0, rows - 1, refs["HYT" + tag]
        own = pl.ds(3, levels)
        return (
            remote(source.at[own, pl.ds(rows - w, w), :], dst.at[:, pl.ds(low, w), :],
                   sems, at, "gy", 1),
            remote(source.at[own, pl.ds(0, w), :], dst.at[:, pl.ds(high, w), :],
                   sems, at + 1, "gy", -1),
        )

    def z_copies(name, tag, sems, at):
        w = EDGE if tag in FULL else 1
        q = refs[name + tag]
        return (
            remote(q.at[pl.ds(3 + levels - w, w)], q.at[pl.ds(3 - w, w)], sems, at, "gz", 1),
            remote(q.at[pl.ds(3, w)], q.at[pl.ds(3 + levels, w)], sems, at + 1, "gz", -1),
        )

    def x_copies(kind, e, sems, at):
        return (
            remote(refs[kind + "_s"].at[e], refs[kind + "_lo"].at[e], sems, at, "gx", 1),
            remote(refs[kind + "_s"].at[e], refs[kind + "_hi"].at[e], sems, at + 1, "gx", -1),
        )

    def start(copies):
        for copy in copies:
            copy.start()

    def wait(copies):
        for copy in copies:
            copy.wait()

    def z_start(up, down):
        @pl.when(has_high)
        def _():
            start(up)

        @pl.when(has_low)
        def _():
            start(down)

    def z_wait(up, down):
        @pl.when(has_high)
        def _():
            for copy in up:
                copy.wait_send()
            for copy in down:
                copy.wait_recv()

        @pl.when(has_low)
        def _():
            for copy in down:
                copy.wait_send()
            for copy in up:
                copy.wait_recv()

    def wind_copies():
        own = refs["V0"].at[:, pl.ds(rows - 1, 1), :]
        return (
            remote(own, refs["HYV0"].at[:, pl.ds(0, 1), :], "f0", 12, "gy", 1),
            remote(refs["W0"].at[levels], refs["W0"].at[0], "f0", 13, "gz", 1),
        )

    def pack(value, packed=None):
        for k in range(levels):
            edge = lanes_by(value(k), SLOT * k + EDGE)
            packed = edge if packed is None else jnp.where(lane // SLOT == k, edge, packed)
        return packed

    def pairs(low, high):
        return jnp.where(slot_lane == EDGE, lanes_by(low, 1), lanes_by(high, -1))

    def to_level(packed, k):
        return lanes_by(packed, -(SLOT * k + EDGE))

    def send_full(name, tag):
        sems, e = "f" + tag, FULL[tag]
        at = 0 if name == "P" else 6
        z = z_copies(name, tag, sems, at + 4)
        if name == "P":
            start(y_copies(name, tag, sems, at + 2))
            if tag == "0":
                start(wind_copies()[:1])
                z_start((z[0], wind_copies()[1]), (z[1],))
            else:
                z_start((z[0],), (z[1],))
        packed = pack(lambda k: refs[name + tag][k + 3])
        if tag == "0" and name == "P":
            for k in range(levels):
                wind = lanes_by(refs["U0"][k], SLOT * k + 7)
                packed = jnp.where((lane // SLOT == k) & (slot_lane == 6), wind, packed)
        refs["x" + name + "_s"][e] = packed
        if name == "P":
            start(x_copies("x" + name, e, sems, at))
        else:
            z_start((z[0],), (z[1],))
            start(x_copies("x" + name, e, sems, at))
            start(y_copies(name, tag, sems, at + 2))

    def receive_x(name, tag, fix=None):
        sems, e = "f" + tag, FULL[tag]
        wait(x_copies("x" + name, e, sems, 0 if name == "P" else 6))
        low, high = refs["x" + name + "_lo"][e], refs["x" + name + "_hi"][e]
        both = jnp.where(slot_lane < EDGE, low, high)
        if fix is not None:
            both = both + fix
        for k in range(levels):
            refs["HX" + name + tag][k] = to_level(both, k)
        if tag == "0" and name == "P":
            for k in range(levels):
                refs["HXU0"][k] = lanes_by(low, -(SLOT * k + 6))

    def receive_z(name, tag):
        z = z_copies(name, tag, "f" + tag, 4 if name == "P" else 10)
        if tag == "0" and name == "P":
            z_wait((z[0], wind_copies()[1]), (z[1],))
        else:
            z_wait((z[0],), (z[1],))

    def receive_y(name, tag):
        wait(y_copies(name, tag, "f" + tag, 2 if name == "P" else 8))
        if tag == "0" and name == "P":
            wait(wind_copies()[:1])

    def first_edges():
        for k in range(levels):
            x, y = refs["HXP0"][k], refs["HYP0"][k]
            refs["HXT0"][k] = jnp.where(lane == 0, lanes_by(x, 1), lanes_by(x, -1))
            refs["HYT0"][k] = jnp.where(row == 0, rows_by(y, 1), rows_by(y, -1))

    def send_thin(tag):
        sems, e = "t" + tag, THIN[tag]
        z = z_copies("P", tag, sems, 4)
        start(y_copies("P", tag, sems, 2))
        z_start((z[0],), (z[1],))
        refs["tx_s"][e] = pack(lambda k: refs["P" + tag][k + 3])
        start(x_copies("tx", e, sems, 0))

    def receive_thin(tag, fix=None):
        sems, e = "t" + tag, THIN[tag]
        z = z_copies("P", tag, sems, 4)
        wait(x_copies("tx", e, sems, 0))
        low, high = refs["tx_lo"][e], refs["tx_hi"][e]
        if fix is not None:
            low, high = low + fix, high + fix
        both = pairs(low, high)
        for k in range(levels):
            refs["HXT" + tag][k] = to_level(both, k)
        z_wait((z[0],), (z[1],))
        wait(y_copies("P", tag, sems, 2))

    def change(tag, k):
        return refs["P" + tag][k + 3] - refs["P0"][k + 3]

    top_rows, low_rows = pl.ds(rows - EDGE, EDGE), pl.ds(0, EDGE)
    top_levels, low_levels = pl.ds(EDGE, EDGE), pl.ds(0, EDGE)

    def delta_copies(tag):
        e, sems = DELTA[tag], "d" + tag
        s, dz = refs["d_s"].at[e], refs["dz_s"].at[e]
        flat = list(x_copies("d", e, sems, 0)) + list(y_copies("P", tag, sems, 2))
        for n, (end, sx) in enumerate((("lo", 1), ("hi", -1))):
            dst = refs["dxy_" + end].at[e]
            for m, (part, sy) in enumerate(((top_rows, 1), (low_rows, -1))):
                flat.append(remote(s.at[part, :], dst.at[part, :], sems, 6 + 2 * n + m,
                                   "gx", sx, "gy", sy))
        z = z_copies("P", tag, sems, 4)
        ups, downs = [z[0]], [z[1]]
        for t, (found, sz, part) in enumerate(((ups, 1, top_levels), (downs, -1, low_levels))):
            for n, (end, sx) in enumerate((("lo", 1), ("hi", -1))):
                found.append(remote(s, refs["dxz_" + end].at[e, t], sems, 10 + 2 * t + n,
                                    "gx", sx, "gz", sz))
            for n, (part_y, sy) in enumerate(((top_rows, 1), (low_rows, -1))):
                found.append(remote(dz.at[part, part_y, :], refs["dyz"].at[e, t, :, part_y, :],
                                    sems, 14 + 2 * t + n, "gy", sy, "gz", sz))
        return flat, ups, downs

    def send_delta(tag):
        e = DELTA[tag]
        for t in range(EDGE):
            refs["dz_s"][e, t] = change(tag, t)
            refs["dz_s"][e, EDGE + t] = change(tag, levels - EDGE + t)
        refs["d_s"][e] = pack(lambda k: change(tag, k))
        flat, ups, downs = delta_copies(tag)
        z_start(ups[1:] + ups[:1], downs[1:] + downs[:1])
        start(flat[4:] + flat[:4])

    def receive_delta(tag):
        flat, ups, downs = delta_copies(tag)
        wait(flat)
        z_wait(ups, downs)

    edge_lane = (lane == 0) | (lane == cols - 1)
    edge_row = (row == 0) | (row == rows - 1)

    def nearer(x):
        return jnp.where(row == 0, rows_by(x, 1), rows_by(x, -1))

    def packed_fix(tag):
        e = DELTA[tag]
        d = refs["d_s"][e]
        across = jnp.where(slot_lane < EDGE, refs["dxy_lo"][e], refs["dxy_hi"][e])
        below = jnp.where(slot_lane < EDGE, refs["dxz_lo"][e, 0], refs["dxz_hi"][e, 0])
        above = jnp.where(slot_lane < EDGE, refs["dxz_lo"][e, 1], refs["dxz_hi"][e, 1])
        last = SLOT * (levels - 1)
        fix = jnp.where(
            slot_lane == EDGE - 1, lanes_by(d, -1),
            jnp.where(slot_lane == EDGE, lanes_by(d, 1), 0.0),
        )
        fix = fix + jnp.where(edge_row, nearer(across), 0.0)
        fix = fix + jnp.where((lane < SLOT) & has_low, lanes_by(below, -last), 0.0)
        return fix + jnp.where((lane // SLOT == levels - 1) & has_high, lanes_by(above, last), 0.0)

    def mend(tag, p_tag, w_tag, push):
        e, gain = DELTA[tag], push * push
        P, U, V, W, HXU, HYV = (refs[n] for n in (
            "P" + p_tag, "U" + w_tag, "V" + w_tag, "W" + w_tag, "HXU" + w_tag, "HYV" + w_tag,
        ))
        full = p_tag in FULL
        face = pairs(refs["d_lo"][e], refs["d_hi"][e])
        corner = pairs(refs["dxy_lo"][e], refs["dxy_hi"][e])
        low = refs["P" + tag][2] - refs["P0"][2]
        high = refs["P" + tag][3 + levels] - refs["P0"][3 + levels]
        W[0] = W[0] + push * low
        W[levels] = W[levels] - push * high

        def layers(t, there, wanted, nearest, source, level, at):
            sides_of = pairs(refs["dxz_lo"][e, t], refs["dxz_hi"][e, t])
            for n in wanted:
                part = jnp.where(edge_lane, to_level(sides_of, level + n), 0.0)
                part = part + jnp.where(edge_row, nearer(refs["dyz"][e, t, n]), 0.0)
                if n == nearest:
                    part = part + change(tag, source)
                P[at + n] = P[at + n] + jnp.where(there, gain * part, 0.0)

        layers(0, has_low, range(EDGE) if full else (EDGE - 1,), EDGE - 1, 0, levels - EDGE, 0)
        layers(1, has_high, range(EDGE) if full else (0,), 0, levels - 1, 0, 3 + levels)
        for k in range(levels):
            own = change(tag, k)
            dx = jnp.where(edge_lane, to_level(face, k), 0.0)
            dy = jnp.where(edge_row, refs["HYT" + tag][k] - refs["HYT0"][k], 0.0)
            total = dx + dy
            if k == 0:
                total = total + low
            if k == levels - 1:
                total = total + high
            P[k + 3] = P[k + 3] + gain * total
            U[k] = U[k] - push * jnp.where(lane == cols - 1, dx, 0.0)
            V[k] = V[k] - push * jnp.where(row == rows - 1, dy, 0.0)
            HXU[k] = HXU[k] + push * dx
            HYV[k] = HYV[k] + push * dy
            beside = jnp.where(edge_row, jnp.where(row == 0, rows_by(own, 1), rows_by(own, -1)), 0.0)
            beside = beside + jnp.where(edge_lane, to_level(corner, k), 0.0)
            if k == 0:
                beside = beside + jnp.where(has_low, refs["dyz"][e, 0, EDGE - 1], 0.0)
            if k == levels - 1:
                beside = beside + jnp.where(has_high, refs["dyz"][e, 1, 0], 0.0)
            if full:
                refs["HYP" + p_tag][k] = refs["HYP" + p_tag][k] + gain * beside
            else:
                refs["HYT" + p_tag][k] = refs["HYT" + p_tag][k] + gain * nearer(beside)

    def sides(q, halo, by, index, extent):
        low = [by(jnp.where(index >= extent - n, halo, q), n) for n in (3, 2, 1)]
        high = [by(jnp.where(index < n, halo, q), -n) for n in (1, 2, 3)]
        return (*low, q, *high)

    def advect_xz(name, tag, rate):
        Q, HX = refs[name + tag], refs["HX" + name + tag]

        def level(k, below):
            u = refs["U" + tag][k]
            u_low = jnp.where(lane == 0, refs["HXU" + tag][k], lanes_by(u, 1))
            xs = sides(Q[k + 3], HX[k], lanes_by, lane, cols)
            above = flux(refs["W" + tag][k + 1], *(Q[k + n] for n in range(1, 7)))
            total = flux(u, *xs[1:]) - flux(u_low, *xs[:6])
            refs[rate][k] = total + (above - below)
            return above

        loop(levels, level, flux(refs["W" + tag][0], *(Q[n] for n in range(6))))

    def advect_y(name, tag, rate):
        Q, HY = refs[name + tag], refs["HY" + name + tag]

        def level(k, carry):
            v = refs["V" + tag][k]
            v_low = jnp.where(row == 0, refs["HYV" + tag][k], rows_by(v, 1))
            ys = sides(Q[k + 3], HY[k], rows_by, row, rows)
            total = refs[rate][k] + (flux(v, *ys[1:]) - flux(v_low, *ys[:6]))
            refs[rate][k] = total * (-1.0 / 60.0)
            return carry

        loop(levels, level, 0)

    def lift_of(tag):
        C = refs["C" + tag]
        lid_low = jnp.where(has_low, 1.0, 0.0)
        lid_high = jnp.where(has_high, 1.0, 0.0)
        for k in range(levels + 1):
            lift = (buoyancy * 0.5) * (C[k + 2] + C[k + 3])
            if k == 0:
                lift = lift * lid_low
            if k == levels:
                lift = lift * lid_high
            refs["lift"][k] = lift

    def substep(sp, hp, sw, dp, dw, sub_step):
        SP, HP, HXT, HYT = refs["P" + sp], refs["P" + hp], refs["HXT" + hp], refs["HYT" + hp]
        SU, SV, SW, HXU, HYV = (refs[n + sw] for n in ("U", "V", "W", "HXU", "HYV"))
        push = sub_step * sound_speed
        lid_low = jnp.where(has_low, 1.0, 0.0)
        lid_high = jnp.where(has_high, 1.0, 0.0)
        last = dp is None

        def vertical(k):
            above = (HP if k == levels else SP)[k + 3]
            below = (HP if k == 0 else SP)[k + 2]
            return SW[k] + sub_step * (refs["lift"][k] - sound_speed * (above - below))

        w_low = vertical(0) * lid_low
        if not last:
            refs["W" + dw][0] = w_low
        for k in range(levels):
            p, u, v = SP[k + 3], SU[k], SV[k]
            hx, hy = HXT[k], HYT[k]
            w = vertical(k + 1)
            if k == levels - 1:
                w = w * lid_high
            hu, hv = HXU[k], HYV[k]
            u_new = u - push * (jnp.where(lane == cols - 1, hx, lanes_by(p, -1)) - p)
            v_new = v - push * (jnp.where(row == rows - 1, hy, rows_by(p, -1)) - p)
            u_halo = u_low = jnp.where(lane == 0, hu, lanes_by(u, 1)) - push * (
                p - jnp.where(lane == 0, hx, lanes_by(p, 1))
            )
            v_halo = v_low = jnp.where(row == 0, hv, rows_by(v, 1)) - push * (
                p - jnp.where(row == 0, hy, rows_by(p, 1))
            )
            div = (u_new - u_low) + (v_new - v_low) + (w - w_low)
            p_new = p + sub_step * (refs["rate_p"][k] - sound_speed * div)
            w_low = w
            if last:
                for n, part in enumerate((p_new, u_new, v_new, w)):
                    out_fields[n + 1, k] = part
            else:
                refs["U" + dw][k] = u_new
                refs["V" + dw][k] = v_new
                refs["W" + dw][k + 1] = w
                refs["HXU" + dw][k] = u_halo
                refs["HYV" + dw][k] = v_halo
                refs["P" + dp][k + 3] = p_new

    def tracer(tag, scale):
        for k in range(levels):
            value = refs["C0"][k + 3] + scale * refs["rate_c"][k]
            if tag is None:
                out_fields[0, k] = value
                swell = jnp.exp(growth * value)
                refs["swell"][0, k] = swell
                refs["swell"][1, k] = swell * jnp.sqrt(swell)
            else:
                refs["C" + tag][k + 3] = value

    def droplet_terms():
        for copy in later_copies:
            copy.wait()

        def cell(k, carry):
            live = counts[k]
            for s in range(slots):
                r = jnp.abs(radius[s, k])
                number = jnp.where(live > s, weight[s, k], 0.0)
                area = number * (r * r)
                mass = area * r
                for m, term in enumerate((number, area, mass)):
                    high = term.astype(jnp.bfloat16).astype(jnp.float32)
                    vals[s, k, m * rows:(m + 1) * rows, :] = high
                    vals[s, k, (m + 3) * rows:(m + 4) * rows, :] = term - high
                vals[s, k, 6 * rows:, :] = jnp.zeros((2 * rows, cols), jnp.float32)
            return carry

        loop(levels, cell, 0, 2)

    def deposit(begin, cells):
        narrow, thin_type = jnp.bfloat16, jnp.float8_e4m3fn
        ids = lax.broadcasted_iota(jnp.int32, (cols, cols), 0).astype(jnp.float32).astype(narrow)
        one = jnp.ones((cols, cols), narrow)
        none = jnp.zeros((cols, cols), narrow)
        tile = (2 * rows, cols)
        blank = jnp.zeros(tile, narrow)
        half = (lax.broadcasted_iota(jnp.int32, tile, 0) // rows).astype(jnp.float32)
        stairs = [(half + 2.0 * q).astype(narrow) for q in range(FMAX // 2 + 1)]

        def cell(n, carry):
            k, j = (begin + n) // rows, (begin + n) % rows
            total = None
            for s in range(0, slots, 2):
                left, hots = [], []
                for t in (s, s + 1):
                    v = vals[t, k, pl.ds(j, 8, stride=rows), :]
                    base = jnp.concatenate([v, v], axis=0).astype(narrow)
                    fall = jnp.full(tile, depth[t, j, 0, k], jnp.int32)
                    fall = fall.astype(jnp.float32).astype(narrow)
                    left.append(jnp.concatenate(
                        [jnp.where(stair == fall, base, blank) for stair in stairs], axis=0
                    ))
                    c = column[t, k, pl.ds(j, 1), :].astype(jnp.float32).astype(narrow)
                    hot = jnp.where(ids == jnp.broadcast_to(c, (cols, cols)), one, none)
                    hots.append(hot.astype(thin_type))
                got = lax.dot_general(
                    jnp.concatenate(left, axis=1), jnp.concatenate(hots, axis=1),
                    (((1,), (1,)), ((), ())), preferred_element_type=jnp.float32,
                )
                total = got if total is None else total + got
            at = pl.ds(pl.multiple_of(j * 8, 8), 8)
            for d in range(FMAX + 1):
                fallen[k, d, at, :] = total[8 * d:8 * (d + 1)]
            return carry

        lax.fori_loop(0, cells, cell, 0, unroll=min(CELLS, cells))

    def landed(m, l):
        total = None
        for d in range(FMAX + 1):
            k = l + d
            if not 0 <= k < levels:
                continue
            part = (
                fallen[k, d, pl.ds(m, rows, stride=8), :]
                + fallen[k, d, pl.ds(m + 3, rows, stride=8), :]
            )
            if m:
                part = part * refs["swell"][m - 1, k]
            total = part if total is None else total + part
        return total

    def fall_copy(m):
        return remote(refs["fall_s"].at[m], refs["fall_r"].at[m], "fall", m, "gz", -1)

    def fall_send(m):
        for l in range(FMAX):
            refs["fall_s"][m, l] = landed(m, l - FMAX)

        @pl.when(has_low)
        def _():
            fall_copy(m).start()

    def fall_home(m):
        for l in range(levels):
            moments[m, l] = landed(m, l)

    begins = [sum(CHUNKS[:n]) for n in range(len(CHUNKS))]
    cells = levels * rows

    def chunk(n):
        begin = min(begins[n], cells)
        end = cells if n == len(CHUNKS) - 1 else min(begins[n] + CHUNKS[n], cells)
        if end > begin:
            deposit(begin, end - begin)

    def advect(name, tag, rate):
        advect_xz(name, tag, rate)
        receive_y(name, tag)
        advect_y(name, tag, rate)

    def tracer_section(tag):
        receive_x("C", tag)
        advect("C", tag, "rate_c")

    copies = max_start(0, top)
    send_full("P", "0")
    send_full("C", "0")
    droplet_terms()
    chunk(0)
    for g in range(1, len(groups)):
        top = max_end(g - 1, top, copies)
        copies = max_start(g, top)
    receive_x("P", "0")
    receive_z("P", "0")
    advect("P", "0", "rate_p")
    first_edges()
    receive_z("C", "0")
    lift_of("0")
    top = max_end(len(groups) - 1, top, copies)
    time_step = courant_goal / (1.0 + jnp.max(top, axis=(0, 1), keepdims=True))
    time_step = jnp.broadcast_to(time_step, shape)

    third = time_step * (1.0 / 3.0)
    substep("0", "0", "0", "1", "1", third)
    send_full("P", "1")
    tracer_section("0")
    tracer("1", third)
    send_full("C", "1")
    chunk(1)

    receive_x("P", "1")
    receive_z("P", "1")
    advect("P", "1", "rate_p")
    receive_z("C", "1")
    lift_of("1")
    half = time_step * 0.5
    part = half / (NS // 2)
    substep("0", "0", "0", "a", "a", part)
    send_delta("a")
    substep("a", "0", "a", "2", "2", part)
    send_full("P", "2")
    tracer_section("1")
    tracer("2", half)
    send_full("C", "2")
    chunk(2)
    fall_send(0)

    receive_delta("a")
    push = part * sound_speed
    receive_x("P", "2", push * push * packed_fix("a"))
    receive_z("P", "2")
    receive_y("P", "2")
    mend("a", "2", "2", push)
    advect_xz("P", "2", "rate_p")
    advect_y("P", "2", "rate_p")
    receive_z("C", "2")
    lift_of("2")
    part = time_step / NS
    substep("0", "0", "0", "b", "b", part)
    send_delta("b")
    substep("b", "0", "b", "c", "c", part)
    send_thin("c")
    tracer_section("2")
    tracer(None, time_step)
    fall_send(1)
    fall_send(2)
    chunk(3)

    receive_delta("b")
    push = part * sound_speed
    receive_thin("c", push * push * packed_fix("b"))
    mend("b", "c", "c", push)
    substep("c", "c", "c", "d", "c", part)
    send_thin("d")
    chunk(4)
    for m in range(3):
        fall_home(m)
    receive_thin("d")
    substep("d", "d", "c", None, None, part)

    @pl.when(has_low)
    def _():
        for m in range(3):
            fall_copy(m).wait_send()

    @pl.when(has_high)
    def _():
        for m in range(3):
            fall_copy(m).wait_recv()
            for l in range(FMAX):
                at = levels - FMAX + l
                moments[m, at] = moments[m, at] + refs["fall_r"][m, l]


def write_out(fields, moments, out_fields, out_moments, sem):
    copies = []
    for source, out in ((fields, out_fields), (moments, out_moments)):
        for n in range(source.shape[0]):
            copies.append(pltpu.make_async_copy(source.at[n], out.at[n], sem.at[len(copies)]))
    for copy in copies:
        copy.start()
    for copy in copies:
        copy.wait()


def per_device(fields, radius, weight, column, counts, fall_depth):
    levels, rows, cols = fields.shape[1:]
    slots = radius.shape[0]
    assert slots % 4 == 0 and levels * SLOT <= cols and rows == 8 and max(FMAX, 2 * EDGE) <= levels
    f32 = jnp.float32
    cell = (rows, cols)
    count = {a: lax.axis_size(a) for a in AXES}
    groups = max_groups(count)
    widest = max(len(shifts_of(g, count)) for g in groups)
    spaces = {}

    def add(name, *shape, dtype=f32):
        spaces[name] = pltpu.VMEM(shape, dtype)

    add("radius", *radius.shape)
    add("weight", *weight.shape)
    add("column", *column.shape, dtype=jnp.int32)
    add("counts", *counts.shape, dtype=jnp.int32)
    spaces["depth"] = pltpu.SMEM((slots, rows, 1, levels), jnp.int32)
    for tag in "012":
        add("C" + tag, levels + 6, *cell)
        for name in ("HXC", "HXP", "HYC", "HYP"):
            add(name + tag, levels, *cell)
    for tag in "012abcd":
        add("P" + tag, levels + 6, *cell)
    for tag in "0cd":
        add("HXT" + tag, levels, *cell)
    for tag in "0abcd":
        add("HYT" + tag, levels, *cell)
    for tag in "012abc":
        for name in ("U", "V", "HXU", "HYV"):
            add(name + tag, levels, *cell)
        add("W" + tag, levels + 1, *cell)
    add("rate_c", levels, *cell)
    add("rate_p", levels, *cell)
    add("lift", levels + 1, *cell)
    add("swell", 2, levels, *cell)
    add("max_send", len(groups), 1, cols)
    add("max_recv", len(groups), widest, 1, cols)
    for end in ("_s", "_lo", "_hi"):
        add("xP" + end, len(FULL), *cell)
        add("xC" + end, len(FULL), *cell)
        add("tx" + end, len(THIN), *cell)
        add("d" + end, len(DELTA), *cell)
    for end in ("_lo", "_hi"):
        add("dxy" + end, len(DELTA), *cell)
        add("dxz" + end, len(DELTA), 2, *cell)
    add("dz_s", len(DELTA), 2 * EDGE, *cell)
    add("dyz", len(DELTA), 2, EDGE, *cell)
    add("vals", slots, levels, 8 * rows, cols)
    add("fallen", levels, FMAX + 1, 8 * rows, cols)
    add("fall_s", 3, FMAX, *cell)
    add("fall_r", 3, FMAX, *cell)
    for end in ("_ss", "_rs"):
        for tag in FULL:
            spaces["f" + tag + end] = pltpu.SemaphoreType.DMA((14,))
        for tag in THIN:
            spaces["t" + tag + end] = pltpu.SemaphoreType.DMA((6,))
        for tag in DELTA:
            spaces["d" + tag + end] = pltpu.SemaphoreType.DMA((18,))
        spaces["fall" + end] = pltpu.SemaphoreType.DMA((3,))
        spaces["max" + end] = pltpu.SemaphoreType.DMA((len(groups), widest))
    spaces["local_sem"] = pltpu.SemaphoreType.DMA((10,))
    vmem = pl.BlockSpec(memory_space=pltpu.VMEM)
    anywhere = pl.BlockSpec(memory_space=pltpu.HBM)
    results = pl.pallas_call(
        functools.partial(kernel, (tuple(spaces), levels, rows, cols, slots)),
        out_shape=(
            jax.ShapeDtypeStruct(fields.shape, f32),
            jax.ShapeDtypeStruct((3, levels, rows, cols), f32),
        ),
        in_specs=[anywhere] * 6,
        out_specs=(vmem, vmem),
        scratch_shapes=list(spaces.values()),
        compiler_params=pltpu.CompilerParams(
            collective_id=0, has_side_effects=True,
            vmem_limit_bytes=KERNEL_BYTES,
        ),
        name="slab_step",
    )(*(
        pltpu.with_memory_space_constraint(x, pltpu.HBM)
        for x in (fall_depth.transpose(0, 2, 3, 1), fields, radius, weight, column, counts)
    ))
    return pl.pallas_call(
        write_out,
        out_shape=tuple(jax.ShapeDtypeStruct(r.shape, f32) for r in results),
        in_specs=[vmem] * 2,
        out_specs=(anywhere,) * 2,
        scratch_shapes=[pltpu.SemaphoreType.DMA((sum(r.shape[0] for r in results),))],
        compiler_params=pltpu.CompilerParams(vmem_limit_bytes=1024 * 1024),
        name="write_out",
    )(*results)


def solution(mesh):
    in_specs = (
        P(None, "gz", "gy", "gx"),
        P(None, "gz", "gy", "gx"),
        P(None, "gz", "gy", "gx"),
        P(None, "gz", "gy", "gx"),
        P("gz", "gy", "gx"),
        P(None, "gz", "gy", "gx"),
    )
    out_specs = (P(None, "gz", "gy", "gx"), P(None, "gz", "gy", "gx"))
    return jax.shard_map(
        per_device, mesh=mesh, in_specs=in_specs, out_specs=out_specs, check_vma=False
    )
```

```python
import functools
import itertools
import jax
import jax.numpy as jnp
from jax import lax
from jax.experimental import pallas as pl
from jax.experimental.pallas import tpu as pltpu
from jax.sharding import PartitionSpec as P

NS = 4
FMAX = 8
CELLS = 8
SLOT = 8
EDGE = 3
CHUNKS = (40, 24, 24, 24, 16)
ONE_SHOT = 32
KERNEL_BYTES = 40 * 1024 * 1024

sound_speed = 10.0
buoyancy = 0.5
courant_goal = 0.6
growth = 0.3

MESH = pl.DeviceIdType.MESH
AXES = ("gy", "gx", "gz")
FULL = {"0": 0, "1": 1, "2": 2}
THIN = {"c": 0, "d": 1}
DELTA = {"a": 0, "b": 1}


def flux(wind, a, b, c, d, e, f):
    central = 37.0 * (c + d) - 8.0 * (b + e) + (a + f)
    upwind = 10.0 * (d - c) - 5.0 * (e - b) + (f - a)
    return wind * central - jnp.abs(wind) * upwind


def max_groups(count):
    total = 1
    for a in AXES:
        total *= count[a]
    return (("gz", "gy", "gx"),) if total <= ONE_SHOT else tuple((a,) for a in AXES)


def shifts_of(group, count):
    return [s for s in itertools.product(*(range(count[a]) for a in group)) if any(s)]


def greeted(groups, count):
    found = {}
    diagonals = [
        (pair, steps)
        for pair in itertools.combinations(AXES, 2)
        for steps in itertools.product((1, -1), repeat=2)
    ]
    for group, shift in [(g, s) for g in groups for s in shifts_of(g, count)] + diagonals:
        step = {a: s % count[a] for a, s in zip(group, shift) if s % count[a]}
        if step:
            found[tuple(sorted(step.items()))] = step
    return list(found.values())


def kernel(
    sizes, depth_hbm, fields_hbm, radius_hbm, weight_hbm, column_hbm, counts_hbm,
    out_fields, moments, *scratch
):
    names, levels, rows, cols, slots = sizes
    refs = dict(zip(names, scratch))
    radius, weight, column, counts = (refs[n] for n in ("radius", "weight", "column", "counts"))
    depth = refs["depth"]
    vals, fallen = refs["vals"], refs["fallen"]
    local_sem = refs["local_sem"]
    shape = (rows, cols)
    lane = lax.broadcasted_iota(jnp.int32, shape, 1)
    row = lax.broadcasted_iota(jnp.int32, shape, 0)
    slot_lane = lane % SLOT
    place = {a: lax.axis_index(a) for a in AXES}
    count = {a: lax.axis_size(a) for a in AXES}
    groups = max_groups(count)
    has_low = place["gz"] > 0
    has_high = place["gz"] < count["gz"] - 1
    zero = jnp.zeros(shape, jnp.float32)

    def lanes_by(x, shift):
        return pltpu.roll(x, shift % cols, 1)

    def rows_by(x, shift):
        return pltpu.roll(x, shift % rows, 0)

    def loop(n, body, carry, unroll=True):
        return lax.fori_loop(0, n, body, carry, unroll=unroll)

    first_copies = []
    for n, dst in enumerate(
        (refs["C0"].at[pl.ds(3, levels)], refs["P0"].at[pl.ds(3, levels)],
         refs["U0"], refs["V0"], refs["W0"].at[pl.ds(1, levels)])
    ):
        first_copies.append(pltpu.make_async_copy(fields_hbm.at[n], dst, local_sem.at[n]))
    later_copies = []
    for n, (src, dst) in enumerate(
        ((counts_hbm, counts), (weight_hbm, weight), (radius_hbm, radius),
         (column_hbm, column), (depth_hbm, depth))
    ):
        later_copies.append(pltpu.make_async_copy(src, dst, local_sem.at[5 + n]))
    for copy in first_copies:
        copy.start()

    def away(group, shift):
        return {a: lax.rem(place[a] + s, count[a]) for a, s in zip(group, shift) if s}

    barrier = pltpu.get_barrier_semaphore()
    peers = 0
    for step in sorted(greeted(groups, count), key=lambda step: step.get("gz", count["gz"])):
        pl.semaphore_signal(
            barrier, inc=1, device_id=away(tuple(step), tuple(step.values())),
            device_id_type=MESH,
        )
        peers += 1

    for copy in later_copies:
        copy.start()
    for copy in first_copies:
        copy.wait()

    @pl.when(jnp.logical_not(has_high))
    def _():
        refs["W0"][levels] = zero
        for tag in ("0", "1", "2"):
            for t in range(EDGE):
                refs["C" + tag][3 + levels + t] = zero
        for tag in "012abcd":
            for t in range(EDGE if tag in FULL else 1):
                refs["P" + tag][3 + levels + t] = zero

    @pl.when(jnp.logical_not(has_low))
    def _():
        refs["W0"][0] = zero
        for tag in ("0", "1", "2"):
            for t in range(EDGE):
                refs["C" + tag][t] = zero
        for tag in "012abcd":
            for t in range(3 - (EDGE if tag in FULL else 1), 3):
                refs["P" + tag][t] = zero

    def fastest(k, top):
        speed = jnp.abs(refs["U0"][k]) + jnp.abs(refs["V0"][k]) + jnp.abs(refs["W0"][k + 1])
        return jnp.maximum(top, speed)

    top = loop(levels, fastest, zero)
    top = jnp.max(top, axis=(0, 1), keepdims=True)
    top = jnp.broadcast_to(top, (1, cols))
    pl.semaphore_wait(barrier, peers)

    def max_start(g, value):
        refs["max_send"][g] = value
        copies = []
        for n, shift in reversed(list(enumerate(shifts_of(groups[g], count)))):
            copy = pltpu.make_async_remote_copy(
                src_ref=refs["max_send"].at[g],
                dst_ref=refs["max_recv"].at[g, n],
                send_sem=refs["max_ss"].at[g, n],
                recv_sem=refs["max_rs"].at[g, n],
                device_id=away(groups[g], shift), device_id_type=MESH,
            )
            copy.start()
            copies.append(copy)
        return copies

    def max_end(g, value, copies):
        wait(copies)
        for n in range(len(copies)):
            value = jnp.maximum(value, refs["max_recv"][g, n])
        return value

    def neighbour(*steps):
        return {
            a: lax.rem(place[a] + count[a] + step, count[a])
            for a, step in zip(steps[::2], steps[1::2])
        }

    def remote(src, dst, sems, n, *steps):
        return pltpu.make_async_remote_copy(
            src_ref=src, dst_ref=dst, send_sem=refs[sems + "_ss"].at[n],
            recv_sem=refs[sems + "_rs"].at[n],
            device_id=neighbour(*steps), device_id_type=MESH,
        )

    def y_copies(name, tag, sems, at):
        source = refs[name + tag]
        if tag in FULL:
            w, low, high, dst = EDGE, rows - EDGE, 0, refs["HY" + name + tag]
        else:
            w, low, high, dst = 1, 0, rows - 1, refs["HYT" + tag]
        own = pl.ds(3, levels)
        return (
            remote(source.at[own, pl.ds(rows - w, w), :], dst.at[:, pl.ds(low, w), :],
                   sems, at, "gy", 1),
            remote(source.at[own, pl.ds(0, w), :], dst.at[:, pl.ds(high, w), :],
                   sems, at + 1, "gy", -1),
        )

    def z_copies(name, tag, sems, at):
        w = EDGE if tag in FULL else 1
        q = refs[name + tag]
        return (
            remote(q.at[pl.ds(3 + levels - w, w)], q.at[pl.ds(3 - w, w)], sems, at, "gz", 1),
            remote(q.at[pl.ds(3, w)], q.at[pl.ds(3 + levels, w)], sems, at + 1, "gz", -1),
        )

    def x_copies(kind, e, sems, at):
        return (
            remote(refs[kind + "_s"].at[e], refs[kind + "_lo"].at[e], sems, at, "gx", 1),
            remote(refs[kind + "_s"].at[e], refs[kind + "_hi"].at[e], sems, at + 1, "gx", -1),
        )

    def start(copies):
        for copy in copies:
            copy.start()

    def wait(copies):
        for copy in copies:
            copy.wait()

    def z_start(up, down):
        @pl.when(has_high)
        def _():
            start(up)

        @pl.when(has_low)
        def _():
            start(down)

    def z_wait(up, down):
        @pl.when(has_high)
        def _():
            for copy in up:
                copy.wait_send()
            for copy in down:
                copy.wait_recv()

        @pl.when(has_low)
        def _():
            for copy in down:
                copy.wait_send()
            for copy in up:
                copy.wait_recv()

    def wind_copies():
        own = refs["V0"].at[:, pl.ds(rows - 1, 1), :]
        return (
            remote(own, refs["HYV0"].at[:, pl.ds(0, 1), :], "f0", 12, "gy", 1),
            remote(refs["W0"].at[levels], refs["W0"].at[0], "f0", 13, "gz", 1),
        )

    def pack(value, packed=None):
        for k in range(levels):
            edge = lanes_by(value(k), SLOT * k + EDGE)
            packed = edge if packed is None else jnp.where(lane // SLOT == k, edge, packed)
        return packed

    def pairs(low, high):
        return jnp.where(slot_lane == EDGE, lanes_by(low, 1), lanes_by(high, -1))

    def to_level(packed, k):
        return lanes_by(packed, -(SLOT * k + EDGE))

    def send_full(name, tag):
        sems, e = "f" + tag, FULL[tag]
        at = 0 if name == "P" else 6
        z = z_copies(name, tag, sems, at + 4)
        if name == "P":
            start(y_copies(name, tag, sems, at + 2))
            if tag == "0":
                start(wind_copies()[:1])
                z_start((z[0], wind_copies()[1]), (z[1],))
            else:
                z_start((z[0],), (z[1],))
        packed = pack(lambda k: refs[name + tag][k + 3])
        if tag == "0" and name == "P":
            for k in range(levels):
                wind = lanes_by(refs["U0"][k], SLOT * k + 7)
                packed = jnp.where((lane // SLOT == k) & (slot_lane == 6), wind, packed)
        refs["x" + name + "_s"][e] = packed
        if name == "P":
            start(x_copies("x" + name, e, sems, at))
        else:
            z_start((z[0],), (z[1],))
            start(x_copies("x" + name, e, sems, at))
            start(y_copies(name, tag, sems, at + 2))

    def receive_x(name, tag, fix=None):
        sems, e = "f" + tag, FULL[tag]
        wait(x_copies("x" + name, e, sems, 0 if name == "P" else 6))
        if fix is not None:
            receive_z(name, tag)
            receive_y(name, tag)
            fix = fix()
        low, high = refs["x" + name + "_lo"][e], refs["x" + name + "_hi"][e]
        both = jnp.where(slot_lane < EDGE, low, high)
        if fix is not None:
            both = both + fix
        for k in range(levels):
            refs["HX" + name + tag][k] = to_level(both, k)
        if tag == "0" and name == "P":
            for k in range(levels):
                refs["HXU0"][k] = lanes_by(low, -(SLOT * k + 6))

    def receive_z(name, tag):
        z = z_copies(name, tag, "f" + tag, 4 if name == "P" else 10)
        if tag == "0" and name == "P":
            z_wait((z[0], wind_copies()[1]), (z[1],))
        else:
            z_wait((z[0],), (z[1],))

    def receive_y(name, tag):
        wait(y_copies(name, tag, "f" + tag, 2 if name == "P" else 8))
        if tag == "0" and name == "P":
            wait(wind_copies()[:1])

    def first_edges():
        for k in range(levels):
            x, y = refs["HXP0"][k], refs["HYP0"][k]
            refs["HXT0"][k] = jnp.where(lane == 0, lanes_by(x, 1), lanes_by(x, -1))
            refs["HYT0"][k] = jnp.where(row == 0, rows_by(y, 1), rows_by(y, -1))

    def send_thin(tag):
        sems, e = "t" + tag, THIN[tag]
        z = z_copies("P", tag, sems, 4)
        start(y_copies("P", tag, sems, 2))
        z_start((z[0],), (z[1],))
        refs["tx_s"][e] = pack(lambda k: refs["P" + tag][k + 3])
        start(x_copies("tx", e, sems, 0))

    def receive_thin(tag, fix=None):
        sems, e = "t" + tag, THIN[tag]
        z = z_copies("P", tag, sems, 4)
        wait(x_copies("tx", e, sems, 0))
        low, high = refs["tx_lo"][e], refs["tx_hi"][e]
        if fix is not None:
            z_wait((z[0],), (z[1],))
            wait(y_copies("P", tag, sems, 2))
            fix = fix()
            low, high = low + fix, high + fix
        both = pairs(low, high)
        for k in range(levels):
            refs["HXT" + tag][k] = to_level(both, k)
        if fix is None:
            z_wait((z[0],), (z[1],))
            wait(y_copies("P", tag, sems, 2))

    def change(tag, k):
        return refs["P" + tag][k + 3] - refs["P0"][k + 3]

    top_rows, low_rows = pl.ds(rows - EDGE, EDGE), pl.ds(0, EDGE)
    top_levels, low_levels = pl.ds(EDGE, EDGE), pl.ds(0, EDGE)

    def delta_copies(tag):
        e, sems = DELTA[tag], "d" + tag
        s, dz = refs["d_s"].at[e], refs["dz_s"].at[e]
        flat = list(x_copies("d", e, sems, 0)) + list(y_copies("P", tag, sems, 2))
        for n, (end, sx) in enumerate((("lo", 1), ("hi", -1))):
            dst = refs["dxy_" + end].at[e]
            for m, (part, sy) in enumerate(((top_rows, 1), (low_rows, -1))):
                flat.append(remote(s.at[part, :], dst.at[part, :], sems, 6 + 2 * n + m,
                                   "gx", sx, "gy", sy))
        z = z_copies("P", tag, sems, 4)
        ups, downs = [z[0]], [z[1]]
        for t, (found, sz, part) in enumerate(((ups, 1, top_levels), (downs, -1, low_levels))):
            for n, (end, sx) in enumerate((("lo", 1), ("hi", -1))):
                found.append(remote(s, refs["dxz_" + end].at[e, t], sems, 10 + 2 * t + n,
                                    "gx", sx, "gz", sz))
            for n, (part_y, sy) in enumerate(((top_rows, 1), (low_rows, -1))):
                found.append(remote(dz.at[part, part_y, :], refs["dyz"].at[e, t, :, part_y, :],
                                    sems, 14 + 2 * t + n, "gy", sy, "gz", sz))
        return flat, ups, downs

    def send_delta(tag):
        e = DELTA[tag]
        for t in range(EDGE):
            refs["dz_s"][e, t] = change(tag, t)
            refs["dz_s"][e, EDGE + t] = change(tag, levels - EDGE + t)
        refs["d_s"][e] = pack(lambda k: change(tag, k))
        flat, ups, downs = delta_copies(tag)
        z_start(ups[1:] + ups[:1], downs[1:] + downs[:1])
        start(flat[4:] + flat[:4])

    def receive_delta(tag):
        flat, ups, downs = delta_copies(tag)
        wait(flat)
        z_wait(ups, downs)

    edge_lane = (lane == 0) | (lane == cols - 1)
    edge_row = (row == 0) | (row == rows - 1)

    def nearer(x):
        return jnp.where(row == 0, rows_by(x, 1), rows_by(x, -1))

    def packed_fix(tag):
        e = DELTA[tag]
        d = refs["d_s"][e]
        across = jnp.where(slot_lane < EDGE, refs["dxy_lo"][e], refs["dxy_hi"][e])
        below = jnp.where(slot_lane < EDGE, refs["dxz_lo"][e, 0], refs["dxz_hi"][e, 0])
        above = jnp.where(slot_lane < EDGE, refs["dxz_lo"][e, 1], refs["dxz_hi"][e, 1])
        last = SLOT * (levels - 1)
        fix = jnp.where(
            slot_lane == EDGE - 1, lanes_by(d, -1),
            jnp.where(slot_lane == EDGE, lanes_by(d, 1), 0.0),
        )
        fix = fix + jnp.where(edge_row, nearer(across), 0.0)
        fix = fix + jnp.where((lane < SLOT) & has_low, lanes_by(below, -last), 0.0)
        return fix + jnp.where((lane // SLOT == levels - 1) & has_high, lanes_by(above, last), 0.0)

    def mend(tag, p_tag, w_tag, push):
        e, gain = DELTA[tag], push * push
        P, U, V, W, HXU, HYV = (refs[n] for n in (
            "P" + p_tag, "U" + w_tag, "V" + w_tag, "W" + w_tag, "HXU" + w_tag, "HYV" + w_tag,
        ))
        full = p_tag in FULL
        face = pairs(refs["d_lo"][e], refs["d_hi"][e])
        corner = pairs(refs["dxy_lo"][e], refs["dxy_hi"][e])
        low = refs["P" + tag][2] - refs["P0"][2]
        high = refs["P" + tag][3 + levels] - refs["P0"][3 + levels]
        W[0] = W[0] + push * low
        W[levels] = W[levels] - push * high

        def layers(t, there, wanted, nearest, source, level, at):
            sides_of = pairs(refs["dxz_lo"][e, t], refs["dxz_hi"][e, t])
            for n in wanted:
                part = jnp.where(edge_lane, to_level(sides_of, level + n), 0.0)
                part = part + jnp.where(edge_row, nearer(refs["dyz"][e, t, n]), 0.0)
                if n == nearest:
                    part = part + change(tag, source)
                P[at + n] = P[at + n] + jnp.where(there, gain * part, 0.0)

        layers(0, has_low, range(EDGE) if full else (EDGE - 1,), EDGE - 1, 0, levels - EDGE, 0)
        layers(1, has_high, range(EDGE) if full else (0,), 0, levels - 1, 0, 3 + levels)
        for k in range(levels):
            own = change(tag, k)
            dx = jnp.where(edge_lane, to_level(face, k), 0.0)
            dy = jnp.where(edge_row, refs["HYT" + tag][k] - refs["HYT0"][k], 0.0)
            total = dx + dy
            if k == 0:
                total = total + low
            if k == levels - 1:
                total = total + high
            P[k + 3] = P[k + 3] + gain * total
            U[k] = U[k] - push * jnp.where(lane == cols - 1, dx, 0.0)
            V[k] = V[k] - push * jnp.where(row == rows - 1, dy, 0.0)
            HXU[k] = HXU[k] + push * dx
            HYV[k] = HYV[k] + push * dy
            beside = jnp.where(edge_row, jnp.where(row == 0, rows_by(own, 1), rows_by(own, -1)), 0.0)
            beside = beside + jnp.where(edge_lane, to_level(corner, k), 0.0)
            if k == 0:
                beside = beside + jnp.where(has_low, refs["dyz"][e, 0, EDGE - 1], 0.0)
            if k == levels - 1:
                beside = beside + jnp.where(has_high, refs["dyz"][e, 1, 0], 0.0)
            if full:
                refs["HYP" + p_tag][k] = refs["HYP" + p_tag][k] + gain * beside
            else:
                refs["HYT" + p_tag][k] = refs["HYT" + p_tag][k] + gain * nearer(beside)

    def sides(q, halo, by, index, extent):
        low = [by(jnp.where(index >= extent - n, halo, q), n) for n in (3, 2, 1)]
        high = [by(jnp.where(index < n, halo, q), -n) for n in (1, 2, 3)]
        return (*low, q, *high)

    def advect_xz(name, tag, rate):
        Q, HX = refs[name + tag], refs["HX" + name + tag]

        def level(k, below):
            u = refs["U" + tag][k]
            u_low = jnp.where(lane == 0, refs["HXU" + tag][k], lanes_by(u, 1))
            xs = sides(Q[k + 3], HX[k], lanes_by, lane, cols)
            above = flux(refs["W" + tag][k + 1], *(Q[k + n] for n in range(1, 7)))
            total = flux(u, *xs[1:]) - flux(u_low, *xs[:6])
            refs[rate][k] = total + (above - below)
            return above

        loop(levels, level, flux(refs["W" + tag][0], *(Q[n] for n in range(6))))

    def advect_y(name, tag, rate):
        Q, HY = refs[name + tag], refs["HY" + name + tag]

        def level(k, carry):
            v = refs["V" + tag][k]
            v_low = jnp.where(row == 0, refs["HYV" + tag][k], rows_by(v, 1))
            ys = sides(Q[k + 3], HY[k], rows_by, row, rows)
            total = refs[rate][k] + (flux(v, *ys[1:]) - flux(v_low, *ys[:6]))
            refs[rate][k] = total * (-1.0 / 60.0)
            return carry

        loop(levels, level, 0)

    def lift_of(tag):
        C = refs["C" + tag]
        lid_low = jnp.where(has_low, 1.0, 0.0)
        lid_high = jnp.where(has_high, 1.0, 0.0)
        for k in range(levels + 1):
            lift = (buoyancy * 0.5) * (C[k + 2] + C[k + 3])
            if k == 0:
                lift = lift * lid_low
            if k == levels:
                lift = lift * lid_high
            refs["lift"][k] = lift

    def substep(sp, hp, sw, dp, dw, sub_step):
        SP, HP, HXT, HYT = refs["P" + sp], refs["P" + hp], refs["HXT" + hp], refs["HYT" + hp]
        SU, SV, SW, HXU, HYV = (refs[n + sw] for n in ("U", "V", "W", "HXU", "HYV"))
        push = sub_step * sound_speed
        lid_low = jnp.where(has_low, 1.0, 0.0)
        lid_high = jnp.where(has_high, 1.0, 0.0)
        last = dp is None

        def vertical(k):
            above = (HP if k == levels else SP)[k + 3]
            below = (HP if k == 0 else SP)[k + 2]
            return SW[k] + sub_step * (refs["lift"][k] - sound_speed * (above - below))

        w_low = vertical(0) * lid_low
        if not last:
            refs["W" + dw][0] = w_low
        for k in range(levels):
            p, u, v = SP[k + 3], SU[k], SV[k]
            hx, hy = HXT[k], HYT[k]
            w = vertical(k + 1)
            if k == levels - 1:
                w = w * lid_high
            hu, hv = HXU[k], HYV[k]
            u_new = u - push * (jnp.where(lane == cols - 1, hx, lanes_by(p, -1)) - p)
            v_new = v - push * (jnp.where(row == rows - 1, hy, rows_by(p, -1)) - p)
            u_halo = u_low = jnp.where(lane == 0, hu, lanes_by(u, 1)) - push * (
                p - jnp.where(lane == 0, hx, lanes_by(p, 1))
            )
            v_halo = v_low = jnp.where(row == 0, hv, rows_by(v, 1)) - push * (
                p - jnp.where(row == 0, hy, rows_by(p, 1))
            )
            if last:
                div = (u_new - u_low) + (v_new - v_low) + (w - w_low)
                p_new = p + sub_step * (refs["rate_p"][k] - sound_speed * div)
            w_low = w
            if last:
                for n, part in enumerate((p_new, u_new, v_new, w)):
                    out_fields[n + 1, k] = part
            else:
                refs["U" + dw][k] = u_new
                refs["V" + dw][k] = v_new
                refs["W" + dw][k + 1] = w
                refs["HXU" + dw][k] = u_halo
                refs["HYV" + dw][k] = v_halo

    def spread_of(p, hx, hy):
        east = jnp.where(lane == cols - 1, hx, lanes_by(p, -1))
        west = jnp.where(lane == 0, hx, lanes_by(p, 1))
        north = jnp.where(row == rows - 1, hy, rows_by(p, -1))
        south = jnp.where(row == 0, hy, rows_by(p, 1))
        return ((east - p) + (west - p)) + ((north - p) + (south - p))

    def lids():
        return jnp.where(has_low, 1.0, 0.0), jnp.where(has_high, 1.0, 0.0)

    def first_parts():
        P, U, V, W = (refs[n + "0"] for n in "PUVW")
        lid_low, lid_high = lids()
        low = (P[3] - P[2]) * lid_low
        for k in range(levels):
            p, u, v = P[k + 3], U[k], V[k]
            high = P[k + 4] - p
            if k == levels - 1:
                high = high * lid_high
            u_low = jnp.where(lane == 0, refs["HXU0"][k], lanes_by(u, 1))
            v_low = jnp.where(row == 0, refs["HYV0"][k], rows_by(v, 1))
            refs["div"][k] = (u - u_low) + (v - v_low) + (W[k + 1] - W[k])
            refs["bend"][k] = spread_of(p, refs["HXT0"][k], refs["HYT0"][k]) + (high - low)
            low = high

    def press_first(dp, sub_step):
        push = sub_step * sound_speed
        for k in range(levels):
            rate = refs["rate_p"][k] - sound_speed * refs["div"][k]
            lift = sound_speed * refs["bend"][k] - (refs["lift"][k + 1] - refs["lift"][k])
            refs["P" + dp][k + 3] = refs["P0"][k + 3] + sub_step * (rate + push * lift)

    def press(sp, hp, pp, dp, sub_step):
        SP, HP, PP, DP = (refs["P" + t] for t in (sp, hp, pp, dp))
        push = sub_step * sound_speed
        lid_low, lid_high = lids()

        def rise(k):
            above = (HP if k == levels else SP)[k + 3]
            below = (HP if k == 0 else SP)[k + 2]
            return refs["lift"][k] - sound_speed * (above - below)

        low = rise(0) * lid_low
        for k in range(levels):
            p = SP[k + 3]
            high = rise(k + 1)
            if k == levels - 1:
                high = high * lid_high
            spread = spread_of(p, refs["HXT" + hp][k], refs["HYT" + hp][k])
            gain = (push * sub_step) * (sound_speed * spread - (high - low))
            DP[k + 3] = (p + (p - PP[k + 3])) + gain
            low = high

    def winds(sp, hp, sw, dw, sub_step):
        substep(sp, hp, sw, "", dw, sub_step)

    def tracer(tag, scale):
        for k in range(levels):
            value = refs["C0"][k + 3] + scale * refs["rate_c"][k]
            if tag is None:
                out_fields[0, k] = value
                swell = jnp.exp(growth * value)
                refs["swell"][0, k] = swell
                refs["swell"][1, k] = swell * jnp.sqrt(swell)
            else:
                refs["C" + tag][k + 3] = value

    def droplet_terms():
        for copy in later_copies:
            copy.wait()

        def cell(k, carry):
            live = counts[k]
            for s in range(slots):
                r = jnp.abs(radius[s, k])
                number = jnp.where(live > s, weight[s, k], 0.0)
                area = number * (r * r)
                mass = area * r
                for m, term in enumerate((number, area, mass)):
                    high = term.astype(jnp.bfloat16).astype(jnp.float32)
                    vals[s, k, m * rows:(m + 1) * rows, :] = high
                    vals[s, k, (m + 3) * rows:(m + 4) * rows, :] = term - high
                vals[s, k, 6 * rows:, :] = jnp.zeros((2 * rows, cols), jnp.float32)
            return carry

        loop(levels, cell, 0, 2)

    def deposit(begin, cells):
        narrow, thin_type = jnp.bfloat16, jnp.float8_e4m3fn
        ids = lax.broadcasted_iota(jnp.int32, (cols, cols), 0).astype(jnp.float32).astype(narrow)
        one = jnp.ones((cols, cols), narrow)
        none = jnp.zeros((cols, cols), narrow)
        tile = (2 * rows, cols)
        blank = jnp.zeros(tile, narrow)
        half = (lax.broadcasted_iota(jnp.int32, tile, 0) // rows).astype(jnp.float32)
        stairs = [(half + 2.0 * q).astype(narrow) for q in range(FMAX // 2 + 1)]

        def cell(n, carry):
            k, j = (begin + n) // rows, (begin + n) % rows
            total = None
            for s in range(0, slots, 2):
                left, hots = [], []
                for t in (s, s + 1):
                    v = vals[t, k, pl.ds(j, 8, stride=rows), :]
                    base = jnp.concatenate([v, v], axis=0).astype(narrow)
                    fall = jnp.full(tile, depth[t, j, 0, k], jnp.int32)
                    fall = fall.astype(jnp.float32).astype(narrow)
                    left.append(jnp.concatenate(
                        [jnp.where(stair == fall, base, blank) for stair in stairs], axis=0
                    ))
                    c = column[t, k, pl.ds(j, 1), :].astype(jnp.float32).astype(narrow)
                    hot = jnp.where(ids == jnp.broadcast_to(c, (cols, cols)), one, none)
                    hots.append(hot.astype(thin_type))
                got = lax.dot_general(
                    jnp.concatenate(left, axis=1), jnp.concatenate(hots, axis=1),
                    (((1,), (1,)), ((), ())), preferred_element_type=jnp.float32,
                )
                total = got if total is None else total + got
            at = pl.ds(pl.multiple_of(j * 8, 8), 8)
            for d in range(FMAX + 1):
                fallen[k, d, at, :] = total[8 * d:8 * (d + 1)]
            return carry

        lax.fori_loop(0, cells, cell, 0, unroll=min(CELLS, cells))

    def landed(m, l):
        total = None
        for d in range(FMAX + 1):
            k = l + d
            if not 0 <= k < levels:
                continue
            part = (
                fallen[k, d, pl.ds(m, rows, stride=8), :]
                + fallen[k, d, pl.ds(m + 3, rows, stride=8), :]
            )
            if m:
                part = part * refs["swell"][m - 1, k]
            total = part if total is None else total + part
        return total

    def fall_copy(m):
        return remote(refs["fall_s"].at[m], refs["fall_r"].at[m], "fall", m, "gz", -1)

    def fall_send(m):
        for l in range(FMAX):
            refs["fall_s"][m, l] = landed(m, l - FMAX)

        @pl.when(has_low)
        def _():
            fall_copy(m).start()

    def fall_home(m):
        for l in range(levels):
            moments[m, l] = landed(m, l)

    begins = [sum(CHUNKS[:n]) for n in range(len(CHUNKS))]
    cells = levels * rows

    def chunk(n):
        begin = min(begins[n], cells)
        end = cells if n == len(CHUNKS) - 1 else min(begins[n] + CHUNKS[n], cells)
        if end > begin:
            deposit(begin, end - begin)

    def advect(name, tag, rate):
        advect_xz(name, tag, rate)
        receive_y(name, tag)
        advect_y(name, tag, rate)

    def tracer_section(tag):
        receive_x("C", tag)
        advect("C", tag, "rate_c")

    copies = max_start(0, top)
    send_full("P", "0")
    send_full("C", "0")
    droplet_terms()
    chunk(0)
    for g in range(1, len(groups)):
        top = max_end(g - 1, top, copies)
        copies = max_start(g, top)
    receive_x("P", "0")
    receive_z("P", "0")
    advect("P", "0", "rate_p")
    first_edges()
    first_parts()
    receive_z("C", "0")
    lift_of("0")
    top = max_end(len(groups) - 1, top, copies)
    time_step = jnp.broadcast_to(courant_goal / (1.0 + top), shape)

    third = time_step * (1.0 / 3.0)
    press_first("1", third)
    send_full("P", "1")
    winds("0", "0", "0", "1", third)
    tracer_section("0")
    tracer("1", third)
    send_full("C", "1")
    chunk(1)

    receive_x("P", "1")
    receive_z("P", "1")
    advect("P", "1", "rate_p")
    receive_z("C", "1")
    lift_of("1")
    half = time_step * 0.5
    part = half / (NS // 2)
    press_first("a", part)
    send_delta("a")
    press("a", "0", "0", "2", part)
    send_full("P", "2")
    winds("0", "0", "0", "a", part)
    winds("a", "0", "a", "2", part)
    tracer_section("1")
    tracer("2", half)
    send_full("C", "2")
    chunk(2)
    fall_send(0)

    push = part * sound_speed
    receive_delta("a")
    receive_x("P", "2", lambda: push * push * packed_fix("a"))
    mend("a", "2", "2", push)
    advect_xz("P", "2", "rate_p")
    advect_y("P", "2", "rate_p")
    receive_z("C", "2")
    lift_of("2")
    part = time_step / NS
    press_first("b", part)
    send_delta("b")
    press("b", "0", "0", "c", part)
    send_thin("c")
    winds("0", "0", "0", "b", part)
    winds("b", "0", "b", "c", part)
    tracer_section("2")
    tracer(None, time_step)
    fall_send(1)
    fall_send(2)
    chunk(3)

    receive_delta("b")
    push = part * sound_speed
    receive_thin("c", lambda: push * push * packed_fix("b"))
    mend("b", "c", "c", push)
    press("c", "c", "b", "d", part)
    send_thin("d")
    winds("c", "c", "c", "c", part)
    chunk(4)
    for m in range(3):
        fall_home(m)
    receive_thin("d")
    substep("d", "d", "c", None, None, part)

    @pl.when(has_low)
    def _():
        for m in range(3):
            fall_copy(m).wait_send()

    @pl.when(has_high)
    def _():
        for m in range(3):
            fall_copy(m).wait_recv()
            for l in range(FMAX):
                at = levels - FMAX + l
                moments[m, at] = moments[m, at] + refs["fall_r"][m, l]


def write_out(fields, moments, out_fields, out_moments, sem):
    copies = []
    for source, out in ((fields, out_fields), (moments, out_moments)):
        for n in range(source.shape[0]):
            copies.append(pltpu.make_async_copy(source.at[n], out.at[n], sem.at[len(copies)]))
    for copy in copies:
        copy.start()
    for copy in copies:
        copy.wait()


def per_device(fields, radius, weight, column, counts, fall_depth):
    levels, rows, cols = fields.shape[1:]
    slots = radius.shape[0]
    assert slots % 4 == 0 and levels * SLOT <= cols and rows == 8 and max(FMAX, 2 * EDGE) <= levels
    f32 = jnp.float32
    cell = (rows, cols)
    count = {a: lax.axis_size(a) for a in AXES}
    groups = max_groups(count)
    widest = max(len(shifts_of(g, count)) for g in groups)
    spaces = {}

    def add(name, *shape, dtype=f32):
        spaces[name] = pltpu.VMEM(shape, dtype)

    add("radius", *radius.shape)
    add("weight", *weight.shape)
    add("column", *column.shape, dtype=jnp.int32)
    add("counts", *counts.shape, dtype=jnp.int32)
    spaces["depth"] = pltpu.SMEM((slots, rows, 1, levels), jnp.int32)
    for tag in "012":
        add("C" + tag, levels + 6, *cell)
        for name in ("HXC", "HXP", "HYC", "HYP"):
            add(name + tag, levels, *cell)
    for tag in "012abcd":
        add("P" + tag, levels + 6, *cell)
    for tag in "0cd":
        add("HXT" + tag, levels, *cell)
    for tag in "0abcd":
        add("HYT" + tag, levels, *cell)
    for tag in "012abc":
        for name in ("U", "V", "HXU", "HYV"):
            add(name + tag, levels, *cell)
        add("W" + tag, levels + 1, *cell)
    add("rate_c", levels, *cell)
    add("rate_p", levels, *cell)
    add("lift", levels + 1, *cell)
    add("swell", 2, levels, *cell)
    add("div", levels, *cell)
    add("bend", levels, *cell)
    add("max_send", len(groups), 1, cols)
    add("max_recv", len(groups), widest, 1, cols)
    for end in ("_s", "_lo", "_hi"):
        add("xP" + end, len(FULL), *cell)
        add("xC" + end, len(FULL), *cell)
        add("tx" + end, len(THIN), *cell)
        add("d" + end, len(DELTA), *cell)
    for end in ("_lo", "_hi"):
        add("dxy" + end, len(DELTA), *cell)
        add("dxz" + end, len(DELTA), 2, *cell)
    add("dz_s", len(DELTA), 2 * EDGE, *cell)
    add("dyz", len(DELTA), 2, EDGE, *cell)
    add("vals", slots, levels, 8 * rows, cols)
    add("fallen", levels, FMAX + 1, 8 * rows, cols)
    add("fall_s", 3, FMAX, *cell)
    add("fall_r", 3, FMAX, *cell)
    for end in ("_ss", "_rs"):
        for tag in FULL:
            spaces["f" + tag + end] = pltpu.SemaphoreType.DMA((14,))
        for tag in THIN:
            spaces["t" + tag + end] = pltpu.SemaphoreType.DMA((6,))
        for tag in DELTA:
            spaces["d" + tag + end] = pltpu.SemaphoreType.DMA((18,))
        spaces["fall" + end] = pltpu.SemaphoreType.DMA((3,))
        spaces["max" + end] = pltpu.SemaphoreType.DMA((len(groups), widest))
    spaces["local_sem"] = pltpu.SemaphoreType.DMA((10,))
    vmem = pl.BlockSpec(memory_space=pltpu.VMEM)
    anywhere = pl.BlockSpec(memory_space=pltpu.HBM)
    results = pl.pallas_call(
        functools.partial(kernel, (tuple(spaces), levels, rows, cols, slots)),
        out_shape=(
            jax.ShapeDtypeStruct(fields.shape, f32),
            jax.ShapeDtypeStruct((3, levels, rows, cols), f32),
        ),
        in_specs=[anywhere] * 6,
        out_specs=(vmem, vmem),
        scratch_shapes=list(spaces.values()),
        compiler_params=pltpu.CompilerParams(
            collective_id=0, has_side_effects=True,
            vmem_limit_bytes=KERNEL_BYTES,
        ),
        name="slab_step",
    )(*(
        pltpu.with_memory_space_constraint(x, pltpu.HBM)
        for x in (fall_depth.transpose(0, 2, 3, 1), fields, radius, weight, column, counts)
    ))
    return pl.pallas_call(
        write_out,
        out_shape=tuple(jax.ShapeDtypeStruct(r.shape, f32) for r in results),
        in_specs=[vmem] * 2,
        out_specs=(anywhere,) * 2,
        scratch_shapes=[pltpu.SemaphoreType.DMA((sum(r.shape[0] for r in results),))],
        compiler_params=pltpu.CompilerParams(vmem_limit_bytes=1024 * 1024),
        name="write_out",
    )(*results)


def solution(mesh):
    in_specs = (
        P(None, "gz", "gy", "gx"),
        P(None, "gz", "gy", "gx"),
        P(None, "gz", "gy", "gx"),
        P(None, "gz", "gy", "gx"),
        P("gz", "gy", "gx"),
        P(None, "gz", "gy", "gx"),
    )
    out_specs = (P(None, "gz", "gy", "gx"), P(None, "gz", "gy", "gx"))
    return jax.shard_map(
        per_device, mesh=mesh, in_specs=in_specs, out_specs=out_specs, check_vma=False
    )
```

```python
import functools
import itertools
import jax
import jax.numpy as jnp
from jax import lax
from jax.experimental import pallas as pl
from jax.experimental.pallas import tpu as pltpu
from jax.sharding import PartitionSpec as P

NS = 4
FMAX = 8
CELLS = 8
SLOT = 8
EDGE = 3
CHUNKS = (40, 24, 24, 24, 16)
ONE_SHOT = 32
KERNEL_BYTES = 40 * 1024 * 1024

sound_speed = 10.0
buoyancy = 0.5
courant_goal = 0.6
growth = 0.3

MESH = pl.DeviceIdType.MESH
AXES = ("gy", "gx", "gz")
FULL = {"0": 0, "1": 1, "2": 2}
THIN = {"c": 0, "d": 1}
DELTA = {"a": 0, "b": 1}


class Named(dict):
    __getattr__ = dict.__getitem__


def flux(wind, a, b, c, d, e, f):
    central = 37.0 * (c + d) - 8.0 * (b + e) + (a + f)
    upwind = 10.0 * (d - c) - 5.0 * (e - b) + (f - a)
    return wind * central - jnp.abs(wind) * upwind


def max_groups(count):
    total = 1
    for a in AXES:
        total *= count[a]
    return (("gz", "gy", "gx"),) if total <= ONE_SHOT else tuple((a,) for a in AXES)


def shifts_of(group, count):
    return [s for s in itertools.product(*(range(count[a]) for a in group)) if any(s)]


def greeted(groups, count):
    found = {}
    diagonals = [
        (pair, steps)
        for pair in itertools.combinations(AXES, 2)
        for steps in itertools.product((1, -1), repeat=2)
    ]
    for group, shift in [(g, s) for g in groups for s in shifts_of(g, count)] + diagonals:
        step = {a: s % count[a] for a, s in zip(group, shift) if s % count[a]}
        if step:
            found[tuple(sorted(step.items()))] = step
    return list(found.values())


def kernel(
    sizes, depth_hbm, fields_hbm, radius_hbm, weight_hbm, column_hbm, counts_hbm,
    out_fields, moments, *scratch
):
    names, levels, rows, cols, slots = sizes
    refs = Named(zip(names, scratch))
    radius, weight, column, counts = (refs[n] for n in ("radius", "weight", "column", "counts"))
    depth = refs.depth
    vals, fallen = refs.vals, refs.fallen
    local_sem = refs.local_sem
    shape = (rows, cols)
    lane = lax.broadcasted_iota(jnp.int32, shape, 1)
    row = lax.broadcasted_iota(jnp.int32, shape, 0)
    slot_lane = lane % SLOT
    place = {a: lax.axis_index(a) for a in AXES}
    count = {a: lax.axis_size(a) for a in AXES}
    groups = max_groups(count)
    has_low = place["gz"] > 0
    has_high = place["gz"] < count["gz"] - 1
    zero = jnp.zeros(shape, jnp.float32)

    def lanes_by(x, shift):
        return pltpu.roll(x, shift % cols, 1)

    def rows_by(x, shift):
        return pltpu.roll(x, shift % rows, 0)

    def loop(n, body, carry, unroll=True):
        return lax.fori_loop(0, n, body, carry, unroll=unroll)

    first_copies = []
    for n, dst in enumerate(
        (refs.C0.at[pl.ds(3, levels)], refs.P0.at[pl.ds(3, levels)],
         refs.U0, refs.V0, refs.W0.at[pl.ds(1, levels)])
    ):
        first_copies.append(pltpu.make_async_copy(fields_hbm.at[n], dst, local_sem.at[n]))
    later_copies = []
    for n, (src, dst) in enumerate(
        ((counts_hbm, counts), (weight_hbm, weight), (radius_hbm, radius),
         (column_hbm, column), (depth_hbm, depth))
    ):
        later_copies.append(pltpu.make_async_copy(src, dst, local_sem.at[5 + n]))
    for copy in first_copies:
        copy.start()

    def away(group, shift):
        return {a: lax.rem(place[a] + s, count[a]) for a, s in zip(group, shift) if s}

    barrier = pltpu.get_barrier_semaphore()
    peers = 0
    for step in sorted(greeted(groups, count), key=lambda step: step.get("gz", count["gz"])):
        pl.semaphore_signal(
            barrier, inc=1, device_id=away(tuple(step), tuple(step.values())),
            device_id_type=MESH,
        )
        peers += 1

    for copy in later_copies:
        copy.start()
    for copy in first_copies:
        copy.wait()

    @pl.when(jnp.logical_not(has_high))
    def _():
        refs.W0[levels] = zero
        for tag in ("0", "1", "2"):
            for t in range(EDGE):
                refs["C" + tag][3 + levels + t] = zero
        for tag in "012abcd":
            for t in range(EDGE if tag in FULL else 1):
                refs["P" + tag][3 + levels + t] = zero

    @pl.when(jnp.logical_not(has_low))
    def _():
        refs.W0[0] = zero
        for tag in ("0", "1", "2"):
            for t in range(EDGE):
                refs["C" + tag][t] = zero
        for tag in "012abcd":
            for t in range(3 - (EDGE if tag in FULL else 1), 3):
                refs["P" + tag][t] = zero

    def fastest(k, top):
        speed = jnp.abs(refs.U0[k]) + jnp.abs(refs.V0[k]) + jnp.abs(refs.W0[k + 1])
        return jnp.maximum(top, speed)

    top = loop(levels, fastest, zero)
    top = jnp.max(top, axis=(0, 1), keepdims=True)
    top = jnp.broadcast_to(top, (1, cols))
    pl.semaphore_wait(barrier, peers)

    def max_start(g, value):
        refs.max_send[g] = value
        copies = []
        for n, shift in reversed(list(enumerate(shifts_of(groups[g], count)))):
            copy = pltpu.make_async_remote_copy(
                src_ref=refs.max_send.at[g],
                dst_ref=refs.max_recv.at[g, n],
                send_sem=refs.max_ss.at[g, n],
                recv_sem=refs.max_rs.at[g, n],
                device_id=away(groups[g], shift), device_id_type=MESH,
            )
            copy.start()
            copies.append(copy)
        return copies

    def max_end(g, value, copies):
        wait(copies)
        for n in range(len(copies)):
            value = jnp.maximum(value, refs.max_recv[g, n])
        return value

    def neighbour(*steps):
        return {
            a: lax.rem(place[a] + count[a] + step, count[a])
            for a, step in zip(steps[::2], steps[1::2])
        }

    def remote(src, dst, sems, n, *steps):
        return pltpu.make_async_remote_copy(
            src_ref=src, dst_ref=dst, send_sem=refs[sems + "_ss"].at[n],
            recv_sem=refs[sems + "_rs"].at[n],
            device_id=neighbour(*steps), device_id_type=MESH,
        )

    def y_copies(name, tag, sems, at):
        source = refs[name + tag]
        if tag in FULL:
            w, low, high, dst = EDGE, rows - EDGE, 0, refs["HY" + name + tag]
        else:
            w, low, high, dst = 1, 0, rows - 1, refs["HYT" + tag]
        own = pl.ds(3, levels)
        return (
            remote(source.at[own, pl.ds(rows - w, w), :], dst.at[:, pl.ds(low, w), :],
                   sems, at, "gy", 1),
            remote(source.at[own, pl.ds(0, w), :], dst.at[:, pl.ds(high, w), :],
                   sems, at + 1, "gy", -1),
        )

    def z_copies(name, tag, sems, at):
        w = EDGE if tag in FULL else 1
        q = refs[name + tag]
        return (
            remote(q.at[pl.ds(3 + levels - w, w)], q.at[pl.ds(3 - w, w)], sems, at, "gz", 1),
            remote(q.at[pl.ds(3, w)], q.at[pl.ds(3 + levels, w)], sems, at + 1, "gz", -1),
        )

    def x_copies(kind, e, sems, at):
        return (
            remote(refs[kind + "_s"].at[e], refs[kind + "_lo"].at[e], sems, at, "gx", 1),
            remote(refs[kind + "_s"].at[e], refs[kind + "_hi"].at[e], sems, at + 1, "gx", -1),
        )

    def start(copies):
        for copy in copies:
            copy.start()

    def wait(copies):
        for copy in copies:
            copy.wait()

    def z_start(up, down):
        @pl.when(has_high)
        def _():
            start(up)

        @pl.when(has_low)
        def _():
            start(down)

    def z_wait(up, down):
        @pl.when(has_high)
        def _():
            for copy in up:
                copy.wait_send()
            for copy in down:
                copy.wait_recv()

        @pl.when(has_low)
        def _():
            for copy in down:
                copy.wait_send()
            for copy in up:
                copy.wait_recv()

    def wind_copies():
        own = refs.V0.at[:, pl.ds(rows - 1, 1), :]
        return (
            remote(own, refs.HYV0.at[:, pl.ds(0, 1), :], "f0", 12, "gy", 1),
            remote(refs.W0.at[levels], refs.W0.at[0], "f0", 13, "gz", 1),
        )

    def pack(value, packed=None):
        for k in range(levels):
            edge = lanes_by(value(k), SLOT * k + EDGE)
            packed = edge if packed is None else jnp.where(lane // SLOT == k, edge, packed)
        return packed

    def pairs(low, high):
        return jnp.where(slot_lane == EDGE, lanes_by(low, 1), lanes_by(high, -1))

    def to_level(packed, k):
        return lanes_by(packed, -(SLOT * k + EDGE))

    def send_full(name, tag):
        sems, e = "f" + tag, FULL[tag]
        at = 0 if name == "P" else 6
        z = z_copies(name, tag, sems, at + 4)
        if name == "P":
            start(y_copies(name, tag, sems, at + 2))
            if tag == "0":
                start(wind_copies()[:1])
                z_start((z[0], wind_copies()[1]), (z[1],))
            else:
                z_start((z[0],), (z[1],))
        packed = pack(lambda k: refs[name + tag][k + 3])
        if tag == "0" and name == "P":
            for k in range(levels):
                wind = lanes_by(refs.U0[k], SLOT * k + 7)
                packed = jnp.where((lane // SLOT == k) & (slot_lane == 6), wind, packed)
        refs["x" + name + "_s"][e] = packed
        if name == "P":
            start(x_copies("x" + name, e, sems, at))
        else:
            z_start((z[0],), (z[1],))
            start(x_copies("x" + name, e, sems, at))
            start(y_copies(name, tag, sems, at + 2))

    def receive_x(name, tag, fix=None):
        sems, e = "f" + tag, FULL[tag]
        wait(x_copies("x" + name, e, sems, 0 if name == "P" else 6))
        if fix is not None:
            receive_z(name, tag)
            receive_y(name, tag)
            fix = fix()
        low, high = refs["x" + name + "_lo"][e], refs["x" + name + "_hi"][e]
        both = jnp.where(slot_lane < EDGE, low, high)
        if fix is not None:
            both = both + fix
        for k in range(levels):
            refs["HX" + name + tag][k] = to_level(both, k)
        if tag == "0" and name == "P":
            for k in range(levels):
                refs.HXU0[k] = lanes_by(low, -(SLOT * k + 6))

    def receive_z(name, tag):
        z = z_copies(name, tag, "f" + tag, 4 if name == "P" else 10)
        if tag == "0" and name == "P":
            z_wait((z[0], wind_copies()[1]), (z[1],))
        else:
            z_wait((z[0],), (z[1],))

    def receive_y(name, tag):
        wait(y_copies(name, tag, "f" + tag, 2 if name == "P" else 8))
        if tag == "0" and name == "P":
            wait(wind_copies()[:1])

    def first_edges():
        for k in range(levels):
            x, y = refs.HXP0[k], refs.HYP0[k]
            refs.HXT0[k] = jnp.where(lane == 0, lanes_by(x, 1), lanes_by(x, -1))
            refs.HYT0[k] = jnp.where(row == 0, rows_by(y, 1), rows_by(y, -1))

    def send_thin(tag):
        sems, e = "t" + tag, THIN[tag]
        z = z_copies("P", tag, sems, 4)
        start(y_copies("P", tag, sems, 2))
        z_start((z[0],), (z[1],))
        refs.tx_s[e] = pack(lambda k: refs["P" + tag][k + 3])
        start(x_copies("tx", e, sems, 0))

    def receive_thin(tag, fix=None):
        sems, e = "t" + tag, THIN[tag]
        z = z_copies("P", tag, sems, 4)
        wait(x_copies("tx", e, sems, 0))
        low, high = refs.tx_lo[e], refs.tx_hi[e]
        if fix is not None:
            z_wait((z[0],), (z[1],))
            wait(y_copies("P", tag, sems, 2))
            fix = fix()
            low, high = low + fix, high + fix
        both = pairs(low, high)
        for k in range(levels):
            refs["HXT" + tag][k] = to_level(both, k)
        if fix is None:
            z_wait((z[0],), (z[1],))
            wait(y_copies("P", tag, sems, 2))

    def change(tag, k):
        return refs["P" + tag][k + 3] - refs.P0[k + 3]

    top_rows, low_rows = pl.ds(rows - EDGE, EDGE), pl.ds(0, EDGE)
    top_levels, low_levels = pl.ds(EDGE, EDGE), pl.ds(0, EDGE)

    def delta_copies(tag):
        e, sems = DELTA[tag], "d" + tag
        s, dz = refs.d_s.at[e], refs.dz_s.at[e]
        flat = list(x_copies("d", e, sems, 0)) + list(y_copies("P", tag, sems, 2))
        for n, (end, sx) in enumerate((("lo", 1), ("hi", -1))):
            dst = refs["dxy_" + end].at[e]
            for m, (part, sy) in enumerate(((top_rows, 1), (low_rows, -1))):
                flat.append(remote(s.at[part, :], dst.at[part, :], sems, 6 + 2 * n + m,
                                   "gx", sx, "gy", sy))
        z = z_copies("P", tag, sems, 4)
        ups, downs = [z[0]], [z[1]]
        for t, (found, sz, part) in enumerate(((ups, 1, top_levels), (downs, -1, low_levels))):
            for n, (end, sx) in enumerate((("lo", 1), ("hi", -1))):
                found.append(remote(s, refs["dxz_" + end].at[e, t], sems, 10 + 2 * t + n,
                                    "gx", sx, "gz", sz))
            for n, (part_y, sy) in enumerate(((top_rows, 1), (low_rows, -1))):
                found.append(remote(dz.at[part, part_y, :], refs.dyz.at[e, t, :, part_y, :],
                                    sems, 14 + 2 * t + n, "gy", sy, "gz", sz))
        return flat, ups, downs

    def send_delta(tag):
        e = DELTA[tag]
        for t in range(EDGE):
            refs.dz_s[e, t] = change(tag, t)
            refs.dz_s[e, EDGE + t] = change(tag, levels - EDGE + t)
        refs.d_s[e] = pack(lambda k: change(tag, k))
        flat, ups, downs = delta_copies(tag)
        z_start(ups[1:] + ups[:1], downs[1:] + downs[:1])
        start(flat[4:] + flat[:4])

    def receive_delta(tag):
        flat, ups, downs = delta_copies(tag)
        wait(flat)
        z_wait(ups, downs)

    edge_lane = (lane == 0) | (lane == cols - 1)
    edge_row = (row == 0) | (row == rows - 1)

    def nearer(x):
        return jnp.where(row == 0, rows_by(x, 1), rows_by(x, -1))

    def packed_fix(tag):
        e = DELTA[tag]
        d = refs.d_s[e]
        across = jnp.where(slot_lane < EDGE, refs.dxy_lo[e], refs.dxy_hi[e])
        below = jnp.where(slot_lane < EDGE, refs.dxz_lo[e, 0], refs.dxz_hi[e, 0])
        above = jnp.where(slot_lane < EDGE, refs.dxz_lo[e, 1], refs.dxz_hi[e, 1])
        last = SLOT * (levels - 1)
        fix = jnp.where(
            slot_lane == EDGE - 1, lanes_by(d, -1),
            jnp.where(slot_lane == EDGE, lanes_by(d, 1), 0.0),
        )
        fix = fix + jnp.where(edge_row, nearer(across), 0.0)
        fix = fix + jnp.where((lane < SLOT) & has_low, lanes_by(below, -last), 0.0)
        return fix + jnp.where((lane // SLOT == levels - 1) & has_high, lanes_by(above, last), 0.0)

    def mend(tag, p_tag, w_tag, push):
        e, gain = DELTA[tag], push * push
        P, U, V, W, HXU, HYV = (refs[n] for n in (
            "P" + p_tag, "U" + w_tag, "V" + w_tag, "W" + w_tag, "HXU" + w_tag, "HYV" + w_tag,
        ))
        full = p_tag in FULL
        face = pairs(refs.d_lo[e], refs.d_hi[e])
        corner = pairs(refs.dxy_lo[e], refs.dxy_hi[e])
        low = refs["P" + tag][2] - refs.P0[2]
        high = refs["P" + tag][3 + levels] - refs.P0[3 + levels]
        W[0] = W[0] + push * low
        W[levels] = W[levels] - push * high

        def layers(t, there, wanted, nearest, source, level, at):
            sides_of = pairs(refs.dxz_lo[e, t], refs.dxz_hi[e, t])
            for n in wanted:
                part = jnp.where(edge_lane, to_level(sides_of, level + n), 0.0)
                part = part + jnp.where(edge_row, nearer(refs.dyz[e, t, n]), 0.0)
                if n == nearest:
                    part = part + change(tag, source)
                P[at + n] = P[at + n] + jnp.where(there, gain * part, 0.0)

        layers(0, has_low, range(EDGE) if full else (EDGE - 1,), EDGE - 1, 0, levels - EDGE, 0)
        layers(1, has_high, range(EDGE) if full else (0,), 0, levels - 1, 0, 3 + levels)
        for k in range(levels):
            own = change(tag, k)
            dx = jnp.where(edge_lane, to_level(face, k), 0.0)
            dy = jnp.where(edge_row, refs["HYT" + tag][k] - refs.HYT0[k], 0.0)
            total = dx + dy
            if k == 0:
                total = total + low
            if k == levels - 1:
                total = total + high
            P[k + 3] = P[k + 3] + gain * total
            U[k] = U[k] - push * jnp.where(lane == cols - 1, dx, 0.0)
            V[k] = V[k] - push * jnp.where(row == rows - 1, dy, 0.0)
            HXU[k] = HXU[k] + push * dx
            HYV[k] = HYV[k] + push * dy
            beside = jnp.where(edge_row, jnp.where(row == 0, rows_by(own, 1), rows_by(own, -1)), 0.0)
            beside = beside + jnp.where(edge_lane, to_level(corner, k), 0.0)
            if k == 0:
                beside = beside + jnp.where(has_low, refs.dyz[e, 0, EDGE - 1], 0.0)
            if k == levels - 1:
                beside = beside + jnp.where(has_high, refs.dyz[e, 1, 0], 0.0)
            if full:
                refs["HYP" + p_tag][k] = refs["HYP" + p_tag][k] + gain * beside
            else:
                refs["HYT" + p_tag][k] = refs["HYT" + p_tag][k] + gain * nearer(beside)

    def sides(q, halo, by, index, extent):
        low = [by(jnp.where(index >= extent - n, halo, q), n) for n in (3, 2, 1)]
        high = [by(jnp.where(index < n, halo, q), -n) for n in (1, 2, 3)]
        return (*low, q, *high)

    def advect_xz(name, tag, rate):
        Q, HX = refs[name + tag], refs["HX" + name + tag]

        def level(k, below):
            u = refs["U" + tag][k]
            u_low = jnp.where(lane == 0, refs["HXU" + tag][k], lanes_by(u, 1))
            xs = sides(Q[k + 3], HX[k], lanes_by, lane, cols)
            above = flux(refs["W" + tag][k + 1], *(Q[k + n] for n in range(1, 7)))
            total = flux(u, *xs[1:]) - flux(u_low, *xs[:6])
            refs[rate][k] = total + (above - below)
            return above

        loop(levels, level, flux(refs["W" + tag][0], *(Q[n] for n in range(6))))

    def advect_y(name, tag, rate):
        Q, HY = refs[name + tag], refs["HY" + name + tag]

        def level(k, carry):
            v = refs["V" + tag][k]
            v_low = jnp.where(row == 0, refs["HYV" + tag][k], rows_by(v, 1))
            ys = sides(Q[k + 3], HY[k], rows_by, row, rows)
            total = refs[rate][k] + (flux(v, *ys[1:]) - flux(v_low, *ys[:6]))
            refs[rate][k] = total * (-1.0 / 60.0)
            return carry

        loop(levels, level, 0)

    def lift_of(tag):
        C = refs["C" + tag]
        lid_low = jnp.where(has_low, 1.0, 0.0)
        lid_high = jnp.where(has_high, 1.0, 0.0)
        for k in range(levels + 1):
            lift = (buoyancy * 0.5) * (C[k + 2] + C[k + 3])
            if k == 0:
                lift = lift * lid_low
            if k == levels:
                lift = lift * lid_high
            refs.lift[k] = lift

    def substep(sp, hp, sw, dp, dw, sub_step):
        SP, HP, HXT, HYT = refs["P" + sp], refs["P" + hp], refs["HXT" + hp], refs["HYT" + hp]
        SU, SV, SW, HXU, HYV = (refs[n + sw] for n in ("U", "V", "W", "HXU", "HYV"))
        push = sub_step * sound_speed
        lid_low = jnp.where(has_low, 1.0, 0.0)
        lid_high = jnp.where(has_high, 1.0, 0.0)
        last = dp is None

        def vertical(k):
            above = (HP if k == levels else SP)[k + 3]
            below = (HP if k == 0 else SP)[k + 2]
            return SW[k] + sub_step * (refs.lift[k] - sound_speed * (above - below))

        w_low = vertical(0) * lid_low
        if not last:
            refs["W" + dw][0] = w_low
        for k in range(levels):
            p, u, v = SP[k + 3], SU[k], SV[k]
            hx, hy = HXT[k], HYT[k]
            w = vertical(k + 1)
            if k == levels - 1:
                w = w * lid_high
            hu, hv = HXU[k], HYV[k]
            u_new = u - push * (jnp.where(lane == cols - 1, hx, lanes_by(p, -1)) - p)
            v_new = v - push * (jnp.where(row == rows - 1, hy, rows_by(p, -1)) - p)
            u_halo = u_low = jnp.where(lane == 0, hu, lanes_by(u, 1)) - push * (
                p - jnp.where(lane == 0, hx, lanes_by(p, 1))
            )
            v_halo = v_low = jnp.where(row == 0, hv, rows_by(v, 1)) - push * (
                p - jnp.where(row == 0, hy, rows_by(p, 1))
            )
            if last:
                div = (u_new - u_low) + (v_new - v_low) + (w - w_low)
                p_new = p + sub_step * (refs.rate_p[k] - sound_speed * div)
            w_low = w
            if last:
                for n, part in enumerate((p_new, u_new, v_new, w)):
                    out_fields[n + 1, k] = part
            else:
                refs["U" + dw][k] = u_new
                refs["V" + dw][k] = v_new
                refs["W" + dw][k + 1] = w
                refs["HXU" + dw][k] = u_halo
                refs["HYV" + dw][k] = v_halo

    def spread_of(p, hx, hy):
        east = jnp.where(lane == cols - 1, hx, lanes_by(p, -1))
        west = jnp.where(lane == 0, hx, lanes_by(p, 1))
        north = jnp.where(row == rows - 1, hy, rows_by(p, -1))
        south = jnp.where(row == 0, hy, rows_by(p, 1))
        return ((east - p) + (west - p)) + ((north - p) + (south - p))

    def lids():
        return jnp.where(has_low, 1.0, 0.0), jnp.where(has_high, 1.0, 0.0)

    def first_parts():
        P, U, V, W = (refs[n + "0"] for n in "PUVW")
        lid_low, lid_high = lids()
        low = (P[3] - P[2]) * lid_low
        for k in range(levels):
            p, u, v = P[k + 3], U[k], V[k]
            high = P[k + 4] - p
            if k == levels - 1:
                high = high * lid_high
            u_low = jnp.where(lane == 0, refs.HXU0[k], lanes_by(u, 1))
            v_low = jnp.where(row == 0, refs.HYV0[k], rows_by(v, 1))
            refs.div[k] = (u - u_low) + (v - v_low) + (W[k + 1] - W[k])
            refs.bend[k] = spread_of(p, refs.HXT0[k], refs.HYT0[k]) + (high - low)
            low = high

    def press_first(dp, sub_step):
        push = sub_step * sound_speed
        for k in range(levels):
            rate = refs.rate_p[k] - sound_speed * refs.div[k]
            lift = sound_speed * refs.bend[k] - (refs.lift[k + 1] - refs.lift[k])
            refs["P" + dp][k + 3] = refs.P0[k + 3] + sub_step * (rate + push * lift)

    def press(sp, hp, pp, dp, sub_step):
        SP, HP, PP, DP = (refs["P" + t] for t in (sp, hp, pp, dp))
        push = sub_step * sound_speed
        lid_low, lid_high = lids()

        def rise(k):
            above = (HP if k == levels else SP)[k + 3]
            below = (HP if k == 0 else SP)[k + 2]
            return refs.lift[k] - sound_speed * (above - below)

        low = rise(0) * lid_low
        for k in range(levels):
            p = SP[k + 3]
            high = rise(k + 1)
            if k == levels - 1:
                high = high * lid_high
            spread = spread_of(p, refs["HXT" + hp][k], refs["HYT" + hp][k])
            gain = (push * sub_step) * (sound_speed * spread - (high - low))
            DP[k + 3] = (p + (p - PP[k + 3])) + gain
            low = high

    def winds(sp, hp, sw, dw, sub_step):
        substep(sp, hp, sw, "", dw, sub_step)

    def tracer(tag, scale):
        for k in range(levels):
            value = refs.C0[k + 3] + scale * refs.rate_c[k]
            if tag is None:
                out_fields[0, k] = value
                swell = jnp.exp(growth * value)
                refs.swell[0, k] = swell
                refs.swell[1, k] = swell * jnp.sqrt(swell)
            else:
                refs["C" + tag][k + 3] = value

    def droplet_terms():
        for copy in later_copies:
            copy.wait()

        def cell(k, carry):
            live = counts[k]
            for s in range(slots):
                r = jnp.abs(radius[s, k])
                number = jnp.where(live > s, weight[s, k], 0.0)
                area = number * (r * r)
                mass = area * r
                for m, term in enumerate((number, area, mass)):
                    high = term.astype(jnp.bfloat16).astype(jnp.float32)
                    vals[s, k, m * rows:(m + 1) * rows, :] = high
                    vals[s, k, (m + 3) * rows:(m + 4) * rows, :] = term - high
                vals[s, k, 6 * rows:, :] = jnp.zeros((2 * rows, cols), jnp.float32)
            return carry

        loop(levels, cell, 0, 2)

    def deposit(begin, cells):
        narrow, thin_type = jnp.bfloat16, jnp.float8_e4m3fn
        ids = lax.broadcasted_iota(jnp.int32, (cols, cols), 0).astype(jnp.float32).astype(narrow)
        one = jnp.ones((cols, cols), narrow)
        none = jnp.zeros((cols, cols), narrow)
        tile = (2 * rows, cols)
        blank = jnp.zeros(tile, narrow)
        half = (lax.broadcasted_iota(jnp.int32, tile, 0) // rows).astype(jnp.float32)
        stairs = [(half + 2.0 * q).astype(narrow) for q in range(FMAX // 2 + 1)]

        def cell(n, carry):
            k, j = (begin + n) // rows, (begin + n) % rows
            total = None
            for s in range(0, slots, 2):
                left, hots = [], []
                for t in (s, s + 1):
                    v = vals[t, k, pl.ds(j, 8, stride=rows), :]
                    base = jnp.concatenate([v, v], axis=0).astype(narrow)
                    fall = jnp.full(tile, depth[t, j, 0, k], jnp.int32)
                    fall = fall.astype(jnp.float32).astype(narrow)
                    left.append(jnp.concatenate(
                        [jnp.where(stair == fall, base, blank) for stair in stairs], axis=0
                    ))
                    c = column[t, k, pl.ds(j, 1), :].astype(jnp.float32).astype(narrow)
                    hot = jnp.where(ids == jnp.broadcast_to(c, (cols, cols)), one, none)
                    hots.append(hot.astype(thin_type))
                got = lax.dot_general(
                    jnp.concatenate(left, axis=1), jnp.concatenate(hots, axis=1),
                    (((1,), (1,)), ((), ())), preferred_element_type=jnp.float32,
                )
                total = got if total is None else total + got
            at = pl.ds(pl.multiple_of(j * 8, 8), 8)
            for d in range(FMAX + 1):
                fallen[k, d, at, :] = total[8 * d:8 * (d + 1)]
            return carry

        lax.fori_loop(0, cells, cell, 0, unroll=min(CELLS, cells))

    def landed(m, l):
        total = None
        for d in range(FMAX + 1):
            k = l + d
            if not 0 <= k < levels:
                continue
            part = (
                fallen[k, d, pl.ds(m, rows, stride=8), :]
                + fallen[k, d, pl.ds(m + 3, rows, stride=8), :]
            )
            if m:
                part = part * refs.swell[m - 1, k]
            total = part if total is None else total + part
        return total

    def fall_copy(m):
        return remote(refs.fall_s.at[m], refs.fall_r.at[m], "fall", m, "gz", -1)

    def fall_send(m):
        for l in range(FMAX):
            refs.fall_s[m, l] = landed(m, l - FMAX)

        @pl.when(has_low)
        def _():
            fall_copy(m).start()

    def fall_home(m):
        for l in range(levels):
            moments[m, l] = landed(m, l)

    begins = [sum(CHUNKS[:n]) for n in range(len(CHUNKS))]
    cells = levels * rows

    def chunk(n):
        begin = min(begins[n], cells)
        end = cells if n == len(CHUNKS) - 1 else min(begins[n] + CHUNKS[n], cells)
        if end > begin:
            deposit(begin, end - begin)

    def advect(name, tag, rate):
        advect_xz(name, tag, rate)
        receive_y(name, tag)
        advect_y(name, tag, rate)

    def tracer_section(tag):
        receive_x("C", tag)
        advect("C", tag, "rate_c")

    copies = max_start(0, top)
    send_full("P", "0")
    send_full("C", "0")
    droplet_terms()
    chunk(0)
    for g in range(1, len(groups)):
        top = max_end(g - 1, top, copies)
        copies = max_start(g, top)
    receive_x("P", "0")
    receive_z("P", "0")
    advect("P", "0", "rate_p")
    first_edges()
    first_parts()
    receive_z("C", "0")
    lift_of("0")
    top = max_end(len(groups) - 1, top, copies)
    time_step = jnp.broadcast_to(courant_goal / (1.0 + top), shape)

    third = time_step * (1.0 / 3.0)
    press_first("1", third)
    send_full("P", "1")
    winds("0", "0", "0", "1", third)
    tracer_section("0")
    tracer("1", third)
    send_full("C", "1")
    chunk(1)

    receive_x("P", "1")
    receive_z("P", "1")
    advect("P", "1", "rate_p")
    receive_z("C", "1")
    lift_of("1")
    half = time_step * 0.5
    part = half / (NS // 2)
    press_first("a", part)
    send_delta("a")
    press("a", "0", "0", "2", part)
    send_full("P", "2")
    winds("0", "0", "0", "a", part)
    winds("a", "0", "a", "2", part)
    tracer_section("1")
    tracer("2", half)
    send_full("C", "2")
    chunk(2)
    fall_send(0)

    push = part * sound_speed
    receive_delta("a")
    receive_x("P", "2", lambda: push * push * packed_fix("a"))
    mend("a", "2", "2", push)
    advect_xz("P", "2", "rate_p")
    advect_y("P", "2", "rate_p")
    receive_z("C", "2")
    lift_of("2")
    part = time_step / NS
    press_first("b", part)
    send_delta("b")
    press("b", "0", "0", "c", part)
    send_thin("c")
    winds("0", "0", "0", "b", part)
    winds("b", "0", "b", "c", part)
    tracer_section("2")
    tracer(None, time_step)
    fall_send(1)
    fall_send(2)
    chunk(3)

    receive_delta("b")
    push = part * sound_speed
    receive_thin("c", lambda: push * push * packed_fix("b"))
    mend("b", "c", "c", push)
    press("c", "c", "b", "d", part)
    send_thin("d")
    winds("c", "c", "c", "c", part)
    chunk(4)
    for m in range(3):
        fall_home(m)
    receive_thin("d")
    substep("d", "d", "c", None, None, part)

    @pl.when(has_low)
    def _():
        for m in range(3):
            fall_copy(m).wait_send()

    @pl.when(has_high)
    def _():
        for m in range(3):
            fall_copy(m).wait_recv()
            for l in range(FMAX):
                at = levels - FMAX + l
                moments[m, at] = moments[m, at] + refs.fall_r[m, l]


def write_out(fields, moments, out_fields, out_moments, sem):
    copies = []
    for source, out in ((fields, out_fields), (moments, out_moments)):
        for n in range(source.shape[0]):
            copies.append(pltpu.make_async_copy(source.at[n], out.at[n], sem.at[len(copies)]))
    for copy in copies:
        copy.start()
    for copy in copies:
        copy.wait()


def per_device(fields, radius, weight, column, counts, fall_depth):
    levels, rows, cols = fields.shape[1:]
    slots = radius.shape[0]
    assert slots % 4 == 0 and levels * SLOT <= cols and rows == 8 and max(FMAX, 2 * EDGE) <= levels
    f32 = jnp.float32
    cell = (rows, cols)
    count = {a: lax.axis_size(a) for a in AXES}
    groups = max_groups(count)
    widest = max(len(shifts_of(g, count)) for g in groups)
    spaces = {}

    def add(name, *shape, dtype=f32):
        spaces[name] = pltpu.VMEM(shape, dtype)

    add("radius", *radius.shape)
    add("weight", *weight.shape)
    add("column", *column.shape, dtype=jnp.int32)
    add("counts", *counts.shape, dtype=jnp.int32)
    spaces["depth"] = pltpu.SMEM((slots, rows, 1, levels), jnp.int32)
    for tag in "012":
        add("C" + tag, levels + 6, *cell)
        for name in ("HXC", "HXP", "HYC", "HYP"):
            add(name + tag, levels, *cell)
    for tag in "012abcd":
        add("P" + tag, levels + 6, *cell)
    for tag in "0cd":
        add("HXT" + tag, levels, *cell)
    for tag in "0abcd":
        add("HYT" + tag, levels, *cell)
    for tag in "012abc":
        for name in ("U", "V", "HXU", "HYV"):
            add(name + tag, levels, *cell)
        add("W" + tag, levels + 1, *cell)
    add("rate_c", levels, *cell)
    add("rate_p", levels, *cell)
    add("lift", levels + 1, *cell)
    add("swell", 2, levels, *cell)
    add("div", levels, *cell)
    add("bend", levels, *cell)
    add("max_send", len(groups), 1, cols)
    add("max_recv", len(groups), widest, 1, cols)
    for end in ("_s", "_lo", "_hi"):
        add("xP" + end, len(FULL), *cell)
        add("xC" + end, len(FULL), *cell)
        add("tx" + end, len(THIN), *cell)
        add("d" + end, len(DELTA), *cell)
    for end in ("_lo", "_hi"):
        add("dxy" + end, len(DELTA), *cell)
        add("dxz" + end, len(DELTA), 2, *cell)
    add("dz_s", len(DELTA), 2 * EDGE, *cell)
    add("dyz", len(DELTA), 2, EDGE, *cell)
    add("vals", slots, levels, 8 * rows, cols)
    add("fallen", levels, FMAX + 1, 8 * rows, cols)
    add("fall_s", 3, FMAX, *cell)
    add("fall_r", 3, FMAX, *cell)
    for end in ("_ss", "_rs"):
        for tag in FULL:
            spaces["f" + tag + end] = pltpu.SemaphoreType.DMA((14,))
        for tag in THIN:
            spaces["t" + tag + end] = pltpu.SemaphoreType.DMA((6,))
        for tag in DELTA:
            spaces["d" + tag + end] = pltpu.SemaphoreType.DMA((18,))
        spaces["fall" + end] = pltpu.SemaphoreType.DMA((3,))
        spaces["max" + end] = pltpu.SemaphoreType.DMA((len(groups), widest))
    spaces["local_sem"] = pltpu.SemaphoreType.DMA((10,))
    vmem = pl.BlockSpec(memory_space=pltpu.VMEM)
    anywhere = pl.BlockSpec(memory_space=pltpu.HBM)
    results = pl.pallas_call(
        functools.partial(kernel, (tuple(spaces), levels, rows, cols, slots)),
        out_shape=(
            jax.ShapeDtypeStruct(fields.shape, f32),
            jax.ShapeDtypeStruct((3, levels, rows, cols), f32),
        ),
        in_specs=[anywhere] * 6,
        out_specs=(vmem, vmem),
        scratch_shapes=list(spaces.values()),
        compiler_params=pltpu.CompilerParams(
            collective_id=0, has_side_effects=True,
            vmem_limit_bytes=KERNEL_BYTES,
        ),
        name="slab_step",
    )(*(
        pltpu.with_memory_space_constraint(x, pltpu.HBM)
        for x in (fall_depth.transpose(0, 2, 3, 1), fields, radius, weight, column, counts)
    ))
    return pl.pallas_call(
        write_out,
        out_shape=tuple(jax.ShapeDtypeStruct(r.shape, f32) for r in results),
        in_specs=[vmem] * 2,
        out_specs=(anywhere,) * 2,
        scratch_shapes=[pltpu.SemaphoreType.DMA((sum(r.shape[0] for r in results),))],
        compiler_params=pltpu.CompilerParams(vmem_limit_bytes=1024 * 1024),
        name="write_out",
    )(*results)


def solution(mesh):
    in_specs = (
        P(None, "gz", "gy", "gx"),
        P(None, "gz", "gy", "gx"),
        P(None, "gz", "gy", "gx"),
        P(None, "gz", "gy", "gx"),
        P("gz", "gy", "gx"),
        P(None, "gz", "gy", "gx"),
    )
    out_specs = (P(None, "gz", "gy", "gx"), P(None, "gz", "gy", "gx"))
    return jax.shard_map(
        per_device, mesh=mesh, in_specs=in_specs, out_specs=out_specs, check_vma=False
    )
```
